8 devices in a mesh: dp: 1 (over z), fsdp: 8 (over y, x, core).
Axes of the slice: x: 2, y: 2, z: 1, core: 2. Of those that a mesh axis runs over, the one named last changes fastest.
Arguments:
- hidden: bfloat16 [8192, 512], P(('dp', 'fsdp'))
- targets: int32 [8192], P(('dp', 'fsdp'))
- weight: bfloat16 [32128, 512], P('fsdp')
Outputs:
- output 1: float32 [1], P('dp')
- output 2: float32 [8192, 512], P(('dp', 'fsdp'))
- output 3: float32 [32128, 512], P(('dp', 'fsdp'))
All inputs are finite; a program needn't handle non-finite values.
Results may differ from the reference program's by a relative error of at most 0.001.
Values are sent between devices in bfloat16 or wider.
A program may use at most 1 GiB of HBM per device.

```python
import jax
import jax.numpy as jnp
from jax import lax

TOKENS = 8192
VOCAB = 32128
WIDTH = 512
BLOCKS = 8

BLOCK_ROWS = VOCAB // BLOCKS


def setup_inputs(seed: int = 0, part: int = 0) -> dict:
    base_key = jax.random.key(seed)
    key_hid, key_tgt, key_wgt = jax.random.split(base_key, 3)
    key_hid = jax.random.fold_in(key_hid, part)
    key_tgt = jax.random.fold_in(key_tgt, part)
    hidden = jax.random.normal(key_hid, (TOKENS, WIDTH), jnp.float32).astype(jnp.bfloat16)
    targets = jax.random.randint(key_tgt, (TOKENS,), 0, VOCAB, dtype=jnp.int32)
    weight = (jax.random.normal(key_wgt, (VOCAB, WIDTH), jnp.float32) * WIDTH ** -0.5).astype(jnp.bfloat16)
    return {"hidden": hidden, "targets": targets, "weight": weight}


def reference(hidden, targets, weight):
    w_blocks = weight.reshape(BLOCKS, BLOCK_ROWS, WIDTH)
    blk_starts = jnp.arange(BLOCKS, dtype=jnp.int32) * BLOCK_ROWS
    col_ids = jnp.arange(BLOCK_ROWS, dtype=jnp.int32)

    def block_logits(w_blk, blk_start):
        logits = jnp.dot(hidden, w_blk.T, preferred_element_type=jnp.float32)
        is_target = (targets - blk_start)[:, None] == col_ids[None, :]
        return logits, is_target

    def fwd_step(fwd_state, blk_pair):
        run_max, run_sum, tgt_logit = fwd_state
        logits, is_target = block_logits(blk_pair[0], blk_pair[1])
        new_max = jnp.maximum(run_max, jnp.max(logits, axis=1))
        run_sum = run_sum * jnp.exp(run_max - new_max) + jnp.sum(jnp.exp(logits - new_max[:, None]), axis=1)
        tgt_logit = tgt_logit + jnp.sum(jnp.where(is_target, logits, 0.0), axis=1)
        return (new_max, run_sum, tgt_logit), None

    init_state = (jnp.full((TOKENS,), -jnp.inf, jnp.float32), jnp.zeros((TOKENS,), jnp.float32), jnp.zeros((TOKENS,), jnp.float32))
    run_max, run_sum, tgt_logit = lax.scan(fwd_step, init_state, (w_blocks, blk_starts))[0]
    log_norm = run_max + jnp.log(run_sum)
    loss_val = (jnp.sum(log_norm - tgt_logit) / TOKENS).reshape(1)

    def bwd_step(dh_acc, blk_pair):
        logits, is_target = block_logits(blk_pair[0], blk_pair[1])
        dlogits = ((jnp.exp(logits - log_norm[:, None]) - is_target.astype(jnp.float32)) / TOKENS).astype(jnp.bfloat16)
        dh_acc = dh_acc + jnp.dot(dlogits, blk_pair[0], preferred_element_type=jnp.float32)
        dw_blk = jnp.dot(dlogits.T, hidden, preferred_element_type=jnp.float32)
        return dh_acc, dw_blk

    grad_hidden, dw_blocks = lax.scan(bwd_step, jnp.zeros((TOKENS, WIDTH), jnp.float32), (w_blocks, blk_starts))
    return loss_val, grad_hidden, dw_blocks.reshape(VOCAB, WIDTH)
```

```python
import jax
import jax.numpy as jnp
from jax import lax
from jax.sharding import PartitionSpec as P


def solution(mesh):
    groups = mesh.shape["fsdp"]
    tok_spec = P(("dp", "fsdp"), None)

    def local_head(hidden, targets, weight):
        tok_loc = hidden.shape[0]
        shard_rows = weight.shape[0]
        tokens = tok_loc * groups
        rank_id = lax.axis_index("fsdp")
        hid = lax.all_gather(hidden, "fsdp", tiled=True)
        tgt = lax.all_gather(targets, "fsdp", tiled=True)
        row_ids = jnp.arange(shard_rows, dtype=jnp.int32)
        is_target = row_ids[:, None] == (tgt - rank_id * shard_rows)[None, :]
        logits = lax.dot_general(weight, hid, (((1,), (1,)), ((), ())), preferred_element_type=jnp.float32)
        loc_max = jnp.max(logits, axis=0)
        glob_max = lax.pmax(loc_max, "fsdp")
        exps = jnp.exp(logits - glob_max[None, :])
        loc_sum = jnp.sum(exps, axis=0)
        loc_tgt = jnp.sum(jnp.where(is_target, logits, 0.0), axis=0)
        glob_sum, glob_tgt = lax.psum((loc_sum, loc_tgt), "fsdp")
        log_norm = glob_max + jnp.log(glob_sum)
        loss_val = (jnp.sum(log_norm - glob_tgt) / tokens).reshape(1)
        dz = ((jnp.exp(logits - log_norm[None, :]) - is_target.astype(jnp.float32)) / tokens).astype(jnp.bfloat16)
        dw = jnp.dot(dz, hid, preferred_element_type=jnp.float32)
        dh = lax.dot_general(dz, weight, (((0,), (0,)), ((), ())), preferred_element_type=jnp.float32)
        dh = lax.psum_scatter(dh, "fsdp", scatter_dimension=0, tiled=True)
        return loss_val, dh, dw

    return jax.shard_map(local_head, mesh=mesh, in_specs=(tok_spec, P(("dp", "fsdp")), P("fsdp", None)), out_specs=(P("dp"), tok_spec, tok_spec), check_vma=False)
```

```python
import functools

import jax
import jax.numpy as jnp
from jax import lax
from jax.experimental import pallas as pl
from jax.experimental.pallas import tpu as pltpu
from jax.sharding import PartitionSpec as P

PIECE = 128
CHIPS = 4
STEP_TOK = PIECE * CHIPS
CHUNK = 512
F32 = jnp.float32


def head_kernel(hid, tgt, w, loss_out, dh_out, dw_out, wt, probs, dw_acc, hbuf, tbuf, zbuf_a, zbuf_b, dz_a, dz_b, dh_acc,
                runmax, factor, tgt_sum, lse_sum, st_send, st_recv, tt_send, tt_recv, pair_buf, s1_buf, r1_buf, s2_buf, r2_buf,
                own_buf, out_stage, h_sem, h_send, fw_send, t_sem, t_send, st_rsem, st_ssem, tt_sem, pair_sem, s1_sem, s2_sem,
                out_sem, out_send, dw_sem):
    tok_loc, width = hid.shape
    vocab = w.shape[0]
    steps = 2 * tok_loc // PIECE
    tokens = tok_loc * 2 * CHIPS
    half = width // 2
    n_chunks = -(-vocab // CHUNK)
    last_rows = vocab - (n_chunks - 1) * CHUNK
    inv_tokens = 1.0 / tokens
    zbufs, dzs = (zbuf_a, zbuf_b), (dz_a, dz_b)

    me = lax.axis_index("fsdp")
    core, chip = me % 2, me // 2
    x, y = chip % 2, chip // 2
    partner = chip * 2 + 1 - core
    chip_x, chip_y, chip_d = y * 2 + (1 - x), (1 - y) * 2 + x, (1 - y) * 2 + (1 - x)
    chip_1 = (1 - core) * chip_x + core * chip_y
    chip_2 = (1 - core) * chip_y + core * chip_x

    def remote(src, dst, send, recv, dev):
        return pltpu.make_async_remote_copy(src_ref=src, dst_ref=dst, send_sem=send, recv_sem=recv, device_id={"fsdp": dev},
                                            device_id_type=pl.DeviceIdType.MESH)

    def wait_bytes(ref, sem):
        pltpu.make_async_copy(ref, ref, sem).wait()

    def chunk_rows(c):
        return CHUNK if c < n_chunks - 1 else last_rows

    def h_sends(q):
        s = 2 * q + core
        rows = pl.ds(pl.multiple_of(q * PIECE, PIECE), PIECE)
        cols = pl.ds(pl.multiple_of(chip * PIECE, PIECE), PIECE)
        return [remote(hid.at[rows], hbuf.at[s, cols], h_send.at[i, q], h_sem.at[s], peer * 2 + core)
                for i, peer in enumerate((chip_x, chip_y, chip_d))]

    def h_forward(s):
        return remote(hbuf.at[s], hbuf.at[s], fw_send.at[s // 2], h_sem.at[s], partner)

    def stats_sends(s):
        return [remote(st_send.at[s], st_recv.at[s, me], st_ssem.at[s], st_rsem.at[s], (me + i) % (2 * CHIPS)) for i in range(1, 2 * CHIPS)]

    def pair_copy(s):
        rows = pl.ds(pl.multiple_of((1 - core) * half, half), half)
        return remote(dh_acc.at[s % 2, rows], pair_buf.at[s % 2], pair_sem.at[0, s % 2], pair_sem.at[1, s % 2], partner)

    def s1_copies(s):
        sl = s % 2
        return [remote(s1_buf.at[sl, block], r1_buf.at[sl, i], s1_sem.at[0, sl], s1_sem.at[1, sl], chip_1 * 2 + core)
                for i, block in enumerate((chip_1, chip_d))]

    def s2_copy(s):
        return remote(s2_buf.at[s % 2], r2_buf.at[s % 2], s2_sem.at[0, s % 2], s2_sem.at[1, s % 2], chip_2 * 2 + core)

    def out_dst(s):
        return dh_out.at[pl.ds(pl.multiple_of(s // 2 * PIECE, PIECE), PIECE), pl.ds(pl.multiple_of(core * half, half), half)]

    def out_remote(s):
        return remote(out_stage.at[s], out_dst(s), out_send.at[s // 2], out_sem, partner)

    def reduce_stages(u):
        @pl.when((u >= 6) & (u < steps + 6))
        def _():
            s = u - 6
            wait_bytes(r2_buf.at[s % 2], s2_sem.at[1, s % 2])
            out_stage[s] = (own_buf[s % 2] + r2_buf[s % 2]).T

            @pl.when(s % 2 == core)
            def _():
                pltpu.make_async_copy(out_stage.at[s], out_dst(s), out_sem).start()

            @pl.when(s % 2 != core)
            def _():
                out_remote(s).start()

        @pl.when((u >= 5) & (u < steps + 5))
        def _():
            s = u - 5
            sl = s % 2
            wait_bytes(r1_buf.at[sl], s1_sem.at[1, sl])

            @pl.when(s >= 2)
            def _():
                wait_bytes(s2_buf.at[sl], s2_sem.at[0, sl])

            s2_buf[sl] = s1_buf[sl, chip_2] + r1_buf[sl, 1]
            own_buf[sl] = s1_buf[sl, chip] + r1_buf[sl, 0]
            s2_copy(s).start()

        @pl.when((u >= 4) & (u < steps + 4))
        def _():
            s = u - 4
            sl = s % 2
            wait_bytes(pair_buf.at[sl], pair_sem.at[1, sl])
            wait_bytes(pair_buf.at[sl], pair_sem.at[0, sl])

            @pl.when(s >= 2)
            def _():
                wait_bytes(r1_buf.at[sl], s1_sem.at[0, sl])

            rows = pl.ds(pl.multiple_of(core * half, half), half)
            for j in range(CHIPS):
                cols = pl.ds(j * PIECE, PIECE)
                s1_buf[sl, j] = dh_acc[sl, rows, cols] + pair_buf[sl, :, cols]
            for copy in s1_copies(s):
                copy.start()

        @pl.when((u >= 3) & (u < steps + 3))
        def _():
            pair_copy(u - 3).start()

    def h_stages(u):
        @pl.when((u + 4 < steps) & (u % 2 == core))
        def _():
            for copy in h_sends((u + 4) // 2):
                copy.start()

        @pl.when((u + 1 < steps) & ((u + 1) % 2 == core))
        def _():
            wait_bytes(hbuf.at[u + 1], h_sem.at[u + 1])
            h_forward(u + 1).start()

        @pl.when((u < steps) & (u % 2 != core))
        def _():
            wait_bytes(hbuf.at[u], h_sem.at[u])

    def target_row(s):
        row = jnp.concatenate([tbuf[2 * j + s % 2, pl.ds(s // 2, 1), :] for j in range(CHIPS)], axis=1)
        return row - me * vocab

    def finish_stats(s):
        wait_bytes(st_recv.at[s], st_rsem.at[s])
        stats = st_recv[s]
        m, e = stats[:, :CHIPS], stats[:, CHIPS:]
        top = jnp.max(m, axis=0)
        lse = top + jnp.log(jnp.sum(e * jnp.exp(m - top[None]), axis=0))
        lse_sum[...] += lse
        lse_row = jnp.concatenate([lse[j:j + 1] for j in range(CHIPS)], axis=1)
        factor[...] = jnp.exp(runmax[s % 2] - lse_row) * inv_tokens

    def chunks(u, fwd, bwd):
        par = u % 2
        if fwd:
            h_f = hbuf.at[u]
            t_f = target_row(u)
        if bwd:
            s = u - 2
            h_b = hbuf.at[s]
            t_b = target_row(s)
        run_m = run_s = tacc = None
        for c in range(n_chunks + 1):
            if c < n_chunks:
                lo, n = c * CHUNK, chunk_rows(c)
                if bwd:
                    dz_ref = dzs[c % 2]
                    ids = lax.broadcasted_iota(jnp.int32, (n, STEP_TOK), 0) + lo
                    hot = jnp.where(ids == t_b, inv_tokens, 0.0)
                    dz_ref[:n] = (probs[par, lo:lo + n] * factor[c:c + 1] - hot).astype(jnp.bfloat16)
                    if n < CHUNK:
                        dz_ref[n:] = jnp.zeros((CHUNK - n, STEP_TOK), jnp.bfloat16)
                if fwd:
                    zbufs[c % 2][:n] = lax.dot_general(w[lo:lo + n], h_f[...], (((1,), (1,)), ((), ())), preferred_element_type=F32)
            if c > 0:
                p = c - 1
                lo, n = p * CHUNK, chunk_rows(p)
                if bwd:
                    dz_ref = dzs[p % 2]
                    part = jnp.dot(wt[:, lo:lo + CHUNK], dz_ref[...], preferred_element_type=F32)
                    if p == 0:
                        dh_acc[par] = part
                    else:
                        dh_acc[par] += part
                    dw_acc[lo:lo + n] += jnp.dot(dz_ref[:n], h_b[...], preferred_element_type=F32)
                if fwd:
                    z = zbufs[p % 2][:n]
                    new_m = jnp.max(z, axis=0, keepdims=True)
                    if p > 0:
                        new_m = jnp.maximum(new_m, run_m)
                    e = jnp.exp(z - new_m)
                    probs[par, lo:lo + n] = e
                    part = jnp.sum(e, axis=0, keepdims=True)
                    ids = lax.broadcasted_iota(jnp.int32, (n, STEP_TOK), 0) + lo
                    hit = jnp.sum(jnp.where(ids == t_f, z, 0.0), axis=0, keepdims=True)
                    if p > 0:
                        part = run_s * jnp.exp(run_m - new_m) + part
                        hit = tacc + hit
                    run_m, run_s, tacc = new_m, part, hit
                    runmax[par, p:p + 1] = new_m
        if fwd:
            for j in range(CHIPS):
                cols = slice(j * PIECE, (j + 1) * PIECE)
                st_send[u, j:j + 1] = run_m[:, cols]
                st_send[u, CHIPS + j:CHIPS + j + 1] = run_s[:, cols]
            tgt_sum[...] += tacc
            pltpu.make_async_copy(st_send.at[u], st_recv.at[u, me], st_rsem.at[u]).start()
            for copy in stats_sends(u):
                copy.start()

    def prepare(u):
        reduce_stages(u)
        h_stages(u)

    barrier = pltpu.get_barrier_semaphore()
    for i in range(1, 2 * CHIPS):
        pl.semaphore_signal(barrier, inc=1, device_id={"fsdp": (me + i) % (2 * CHIPS)}, device_id_type=pl.DeviceIdType.MESH)
    pl.semaphore_wait(barrier, 2 * CHIPS - 1)

    def own_piece(q, _):
        s = 2 * q + core
        pltpu.make_async_copy(hid.at[pl.ds(pl.multiple_of(q * PIECE, PIECE), PIECE)],
                              hbuf.at[s, pl.ds(pl.multiple_of(chip * PIECE, PIECE), PIECE)], h_sem.at[s]).start()
        return 0

    lax.fori_loop(0, steps // 2, own_piece, 0)
    for copy in h_sends(0):
        copy.start()
    pltpu.make_async_copy(tgt, tbuf.at[me], t_sem).start()
    t_copies = [remote(tgt, tbuf.at[me], t_send, t_sem, (me + i) % (2 * CHIPS)) for i in range(1, 2 * CHIPS)]
    for copy in t_copies:
        copy.start()
    for copy in h_sends(1):
        copy.start()

    for c in range(n_chunks):
        n = chunk_rows(c)
        wt[:, c * CHUNK:c * CHUNK + n] = w[c * CHUNK:c * CHUNK + n].T
    if last_rows < CHUNK:
        wt[:, vocab:] = jnp.zeros((width, n_chunks * CHUNK - vocab), jnp.bfloat16)
    dw_acc[...] = jnp.zeros_like(dw_acc)
    tgt_sum[...] = jnp.zeros_like(tgt_sum)
    lse_sum[...] = jnp.zeros_like(lse_sum)

    @pl.when(core == 0)
    def _():
        wait_bytes(hbuf.at[0], h_sem.at[0])
        h_forward(0).start()

    wait_bytes(tbuf, t_sem)

    def fwd_step(u, _):
        prepare(u)
        chunks(u, True, False)
        return 0

    def both_step(u, _):
        prepare(u)
        finish_stats(u - 2)
        chunks(u, True, True)
        return 0

    def bwd_step(u, _):
        prepare(u)
        finish_stats(u - 2)
        chunks(u, False, True)
        return 0

    def tail_step(u, _):
        reduce_stages(u)
        return 0

    lax.fori_loop(0, 2, fwd_step, 0)
    lax.fori_loop(2, steps, both_step, 0)
    row = tgt_sum[...]
    tile = jnp.concatenate([row[:, j * PIECE:(j + 1) * PIECE] for j in range(CHIPS)] + [jnp.zeros((8 - CHIPS, PIECE), F32)], axis=0)
    tt_send[...] = tile
    pltpu.make_async_copy(tt_send, tt_recv.at[me], tt_sem.at[1]).start()
    for i in range(1, 2 * CHIPS):
        remote(tt_send, tt_recv.at[me], tt_sem.at[0], tt_sem.at[1], (me + i) % (2 * CHIPS)).start()
    lax.fori_loop(steps, steps + 2, bwd_step, 0)
    dw_copy = pltpu.make_async_copy(dw_acc, dw_out, dw_sem)
    dw_copy.start()
    wait_bytes(tt_recv, tt_sem.at[1])
    loss_out[0] = (jnp.sum(lse_sum[...]) - jnp.sum(tt_recv[...])) * inv_tokens
    lax.fori_loop(steps + 2, steps + 6, tail_step, 0)

    wait_bytes(dh_out, out_sem)
    dw_copy.wait()
    peers = 2 * CHIPS - 1
    wait_bytes(tbuf.at[:peers], t_send)
    wait_bytes(tt_recv.at[:peers], tt_sem.at[0])

    def drain_pieces(q, _):
        for copy in h_sends(q):
            copy.wait_send()
        wait_bytes(hbuf.at[2 * q + core], fw_send.at[q])
        wait_bytes(out_stage.at[2 * q], out_send.at[q])
        return 0

    def drain_stats(s, _):
        wait_bytes(st_recv.at[s, :peers], st_ssem.at[s])
        return 0

    lax.fori_loop(0, steps // 2, drain_pieces, 0)
    lax.fori_loop(0, steps, drain_stats, 0)
    for sl in range(2):
        wait_bytes(r1_buf.at[sl], s1_sem.at[0, sl])
        wait_bytes(s2_buf.at[sl], s2_sem.at[0, sl])


def solution(mesh):
    groups = mesh.shape["fsdp"]
    tok_spec = P(("dp", "fsdp"), None)

    def local_head(hidden, targets, weight):
        tok_loc, width = hidden.shape
        vocab = weight.shape[0]
        steps = 2 * tok_loc // PIECE
        padded = -(-vocab // CHUNK) * CHUNK
        half = width // 2
        dma, bf16 = pltpu.SemaphoreType.DMA, jnp.bfloat16
        vmem = pl.BlockSpec(memory_space=pltpu.VMEM)
        anyspace = pl.BlockSpec(memory_space=pl.ANY)
        scratch = [
            pltpu.VMEM((width, padded), bf16),
            pltpu.VMEM((2, padded, STEP_TOK), F32),
            pltpu.VMEM((vocab, width), F32),
            pltpu.VMEM((steps, STEP_TOK, width), bf16),
            pltpu.VMEM((groups, tok_loc // PIECE, PIECE), jnp.int32),
            pltpu.VMEM((CHUNK, STEP_TOK), F32), pltpu.VMEM((CHUNK, STEP_TOK), F32),
            pltpu.VMEM((CHUNK, STEP_TOK), bf16), pltpu.VMEM((CHUNK, STEP_TOK), bf16),
            pltpu.VMEM((2, width, STEP_TOK), F32),
            pltpu.VMEM((2, padded // CHUNK, STEP_TOK), F32),
            pltpu.VMEM((padded // CHUNK, STEP_TOK), F32),
            pltpu.VMEM((1, STEP_TOK), F32),
            pltpu.VMEM((CHIPS, PIECE), F32),
            pltpu.VMEM((steps, 8, PIECE), F32),
            pltpu.VMEM((steps, groups, 8, PIECE), F32),
            pltpu.VMEM((8, PIECE), F32),
            pltpu.VMEM((groups, 8, PIECE), F32),
            pltpu.VMEM((2, half, STEP_TOK), F32),
            pltpu.VMEM((2, CHIPS, half, PIECE), F32),
            pltpu.VMEM((2, 2, half, PIECE), F32),
            pltpu.VMEM((2, half, PIECE), F32),
            pltpu.VMEM((2, half, PIECE), F32),
            pltpu.VMEM((2, half, PIECE), F32),
            pltpu.VMEM((steps, PIECE, half), F32),
            dma((steps,)), dma((3, steps // 2)), dma((steps // 2,)),
            dma(()), dma(()),
            dma((steps,)), dma((steps,)),
            dma((2,)), dma((2, 2)), dma((2, 2)), dma((2, 2)),
            dma(()), dma((steps // 2,)), dma(()),
        ]
        flops = 6 * tok_loc * groups * vocab * width
        return pl.pallas_call(
            head_kernel,
            out_shape=(jax.ShapeDtypeStruct((1,), F32), jax.ShapeDtypeStruct((tok_loc, width), F32), jax.ShapeDtypeStruct((vocab, width), F32)),
            in_specs=[vmem, vmem, vmem],
            out_specs=(pl.BlockSpec(memory_space=pltpu.SMEM), anyspace, anyspace),
            scratch_shapes=scratch,
            compiler_params=pltpu.CompilerParams(collective_id=0, has_side_effects=True, vmem_limit_bytes=67_043_328),
            cost_estimate=pl.CostEstimate(flops=flops, bytes_accessed=20_000_000, transcendentals=tok_loc * groups * vocab),
        )(hidden, targets.reshape(tok_loc // PIECE, PIECE), weight)

    return jax.shard_map(local_head, mesh=mesh, in_specs=(tok_spec, P(("dp", "fsdp")), P("fsdp", None)), out_specs=(P("dp"), tok_spec, tok_spec), check_vma=False)
```

```python
import functools

import jax
import jax.numpy as jnp
from jax import lax
from jax.experimental import pallas as pl
from jax.experimental.pallas import tpu as pltpu
from jax.sharding import PartitionSpec as P

PIECE = 128
CHIPS = 4
STEP_TOK = PIECE * CHIPS
DIRECT = 4
CHUNK = 512
F32 = jnp.float32


def head_kernel(hid, tgt, w_in, loss_out, dh_out, dw_out, w, wt, probs, hbuf, tbuf, zbuf_a, zbuf_b, dz_a, dz_b, dh_acc,
                runmax, factor, tgt_sum, lse_sum, st_send, st_recv, tt_send, tt_recv, pair_buf, s1_buf, r1_buf, s2_buf, r2_buf,
                own_buf, out_stage, w_sem, h_own, h_recv, h_fwd, h_send, fw_send, t_sem, t_send, st_rsem, st_ssem, tt_sem, pair_sem,
                s1_sem, s2_sem, out_sem, out_send):
    tok_loc, width = hid.shape
    vocab = w.shape[0]
    steps = 2 * tok_loc // PIECE
    tokens = tok_loc * 2 * CHIPS
    half = width // 2
    n_chunks = -(-vocab // CHUNK)
    last_rows = vocab - (n_chunks - 1) * CHUNK
    inv_tokens = 1.0 / tokens
    dw_acc = dw_out
    zbufs, dzs = (zbuf_a, zbuf_b), (dz_a, dz_b)

    me = lax.axis_index("fsdp")
    core, chip = me % 2, me // 2
    x, y = chip % 2, chip // 2
    partner = chip * 2 + 1 - core
    chip_x, chip_y, chip_d = y * 2 + (1 - x), (1 - y) * 2 + x, (1 - y) * 2 + (1 - x)
    chip_1 = (1 - core) * chip_x + core * chip_y
    chip_2 = (1 - core) * chip_y + core * chip_x

    def remote(src, dst, send, recv, dev):
        return pltpu.make_async_remote_copy(src_ref=src, dst_ref=dst, send_sem=send, recv_sem=recv, device_id={"fsdp": dev},
                                            device_id_type=pl.DeviceIdType.MESH)

    def wait_bytes(ref, sem):
        pltpu.make_async_copy(ref, ref, sem).wait()

    def chunk_rows(c):
        return CHUNK if c < n_chunks - 1 else last_rows

    def piece(s, of_chip, lo=0, n=PIECE):
        return hbuf.at[s, pl.ds(pl.multiple_of(of_chip * PIECE + lo, n), n)]

    def h_sends(q, direct):
        s = 2 * q + core
        peers = (chip_x, chip_y, chip_d)[:3 if direct else 2]
        return [remote(piece(s, chip), piece(s, chip), h_send.at[i, q], h_recv.at[i, q], peer * 2 + core) for i, peer in enumerate(peers)]

    def h_relays(s):
        q = s // 2
        return [remote(piece(s, src, lo, PIECE // 2), piece(s, src, lo, PIECE // 2), h_send.at[3 + i, q], h_recv.at[2, q], dst * 2 + core)
                for i, (src, dst, lo) in enumerate(((chip_x, chip_y, 0), (chip_y, chip_x, PIECE // 2)))]

    def h_forward(s):
        return remote(hbuf.at[s], hbuf.at[s], fw_send.at[s // 2], h_fwd.at[s // 2], partner)

    def stats_sends(s):
        return [remote(st_send.at[s], st_recv.at[s, me], st_ssem.at[s], st_rsem.at[s], (me + i) % (2 * CHIPS)) for i in range(1, 2 * CHIPS)]

    def pair_copy(s):
        rows = pl.ds(pl.multiple_of((1 - core) * half, half), half)
        return remote(dh_acc.at[s % 2, rows], pair_buf.at[s % 2], pair_sem.at[0, s % 2], pair_sem.at[1, s % 2], partner)

    def s1_copies(s):
        sl = s % 2
        return [remote(s1_buf.at[sl, block], r1_buf.at[sl, i], s1_sem.at[0, sl], s1_sem.at[1, sl], chip_1 * 2 + core)
                for i, block in enumerate((chip_1, chip_d))]

    def s2_copy(s):
        return remote(s2_buf.at[s % 2], r2_buf.at[s % 2], s2_sem.at[0, s % 2], s2_sem.at[1, s % 2], chip_2 * 2 + core)

    def out_dst(s):
        return dh_out.at[pl.ds(pl.multiple_of(s // 2 * PIECE, PIECE), PIECE), pl.ds(pl.multiple_of(core * half, half), half)]

    def out_remote(s):
        return remote(out_stage.at[s], out_dst(s), out_send.at[s // 2], out_sem, partner)

    def reduce_stages(u):
        @pl.when((u >= 6) & (u < steps + 6))
        def _():
            s = u - 6
            wait_bytes(r2_buf.at[s % 2], s2_sem.at[1, s % 2])
            out_stage[s] = (own_buf[s % 2] + r2_buf[s % 2]).T

            @pl.when(s % 2 == core)
            def _():
                pltpu.make_async_copy(out_stage.at[s], out_dst(s), out_sem).start()

            @pl.when(s % 2 != core)
            def _():
                out_remote(s).start()

        @pl.when((u >= 5) & (u < steps + 5))
        def _():
            s = u - 5
            sl = s % 2
            wait_bytes(r1_buf.at[sl], s1_sem.at[1, sl])

            @pl.when(s >= 2)
            def _():
                wait_bytes(s2_buf.at[sl], s2_sem.at[0, sl])

            s2_buf[sl] = s1_buf[sl, chip_2] + r1_buf[sl, 1]
            own_buf[sl] = s1_buf[sl, chip] + r1_buf[sl, 0]
            s2_copy(s).start()

        @pl.when((u >= 4) & (u < steps + 4))
        def _():
            s = u - 4
            sl = s % 2
            wait_bytes(pair_buf.at[sl], pair_sem.at[1, sl])
            wait_bytes(pair_buf.at[sl], pair_sem.at[0, sl])

            @pl.when(s >= 2)
            def _():
                wait_bytes(r1_buf.at[sl], s1_sem.at[0, sl])

            rows = pl.ds(pl.multiple_of(core * half, half), half)
            for j in range(CHIPS):
                cols = pl.ds(j * PIECE, PIECE)
                s1_buf[sl, j] = dh_acc[sl, rows, cols] + pair_buf[sl, :, cols]
            for copy in s1_copies(s):
                copy.start()

        @pl.when((u >= 3) & (u < steps + 3))
        def _():
            pair_copy(u - 3).start()

    def first_set(u):
        return jnp.minimum(DIRECT + u + 2 * jnp.clip(u - 2, 0, 2), steps)

    def h_ready(s, lo):
        for i in range(lo, 3):
            wait_bytes(hbuf.at[s, pl.ds(0, PIECE)], h_recv.at[i, s // 2])

    def h_stages(u):
        for i in range(3):
            @pl.when((first_set(u) + i < first_set(u + 1)) & ((first_set(u) + i) % 2 == core))
            def _():
                for copy in h_sends((first_set(u) + i) // 2, False):
                    copy.start()

        @pl.when((u + 2 >= DIRECT) & (u + 2 < steps) & (u % 2 == core))
        def _():
            for i in range(2):
                wait_bytes(hbuf.at[u + 2, pl.ds(0, PIECE)], h_recv.at[i, (u + 2) // 2])
            for copy in h_relays(u + 2):
                copy.start()

        @pl.when((u + 1 < DIRECT) & ((u + 1) % 2 == core))
        def _():
            h_ready(u + 1, 0)
            h_forward(u + 1).start()

        @pl.when((u + 1 >= DIRECT) & (u + 1 < steps) & ((u + 1) % 2 == core))
        def _():
            h_ready(u + 1, 2)
            h_forward(u + 1).start()

        @pl.when((u < steps) & (u % 2 != core))
        def _():
            wait_bytes(hbuf.at[u], h_fwd.at[u // 2])

    def target_row(s):
        row = jnp.concatenate([tbuf[2 * j + s % 2, pl.ds(s // 2, 1), :] for j in range(CHIPS)], axis=1)
        return row - me * vocab

    def finish_stats(s):
        wait_bytes(st_recv.at[s], st_rsem.at[s])
        stats = st_recv[s]
        m, e = stats[:, :CHIPS], stats[:, CHIPS:]
        top = jnp.max(m, axis=0)
        lse = top + jnp.log(jnp.sum(e * jnp.exp(m - top[None]), axis=0))
        lse_sum[...] += lse
        lse_row = jnp.concatenate([lse[j:j + 1] for j in range(CHIPS)], axis=1)
        factor[...] = jnp.exp(runmax[s % 2] - lse_row) * inv_tokens

    def chunks(u, fwd, bwd, late_dw=False):
        par = u % 2
        if fwd:
            h_f = hbuf.at[u]
            t_f = target_row(u)
        if bwd:
            s = u - 2
            h_b = hbuf.at[s]
            t_b = target_row(s)
        run_m = run_s = tacc = None
        for c in range(n_chunks + 1):
            if c < n_chunks:
                lo, n = c * CHUNK, chunk_rows(c)
                if bwd:
                    dz_ref = dzs[c % 2]
                    ids = lax.broadcasted_iota(jnp.int32, (n, STEP_TOK), 0) + lo
                    hot = jnp.where(ids == t_b, inv_tokens, 0.0)
                    dz = (probs[par, lo:lo + n] * factor[c:c + 1] - hot).astype(jnp.bfloat16)
                    dz_ref[:n] = dz
                    if late_dw:
                        probs[par, lo:lo + n] = dz.astype(F32)
                    if n < CHUNK:
                        dz_ref[n:] = jnp.zeros((CHUNK - n, STEP_TOK), jnp.bfloat16)
                if fwd:
                    zbufs[c % 2][:n] = lax.dot_general(w[lo:lo + n], h_f[...], (((1,), (1,)), ((), ())), preferred_element_type=F32)
            if c > 0:
                p = c - 1
                lo, n = p * CHUNK, chunk_rows(p)
                if bwd:
                    dz_ref = dzs[p % 2]
                    part = jnp.dot(wt[:, lo:lo + CHUNK], dz_ref[...], preferred_element_type=F32)
                    if p == 0:
                        dh_acc[par] = part
                    else:
                        dh_acc[par] += part
                    if not late_dw:
                        dw_acc[lo:lo + n] += jnp.dot(dz_ref[:n], h_b[...], preferred_element_type=F32)
                if fwd:
                    z = zbufs[p % 2][:n]
                    new_m = jnp.max(z, axis=0, keepdims=True)
                    if p > 0:
                        new_m = jnp.maximum(new_m, run_m)
                    e = jnp.exp(z - new_m)
                    probs[par, lo:lo + n] = e
                    part = jnp.sum(e, axis=0, keepdims=True)
                    ids = lax.broadcasted_iota(jnp.int32, (n, STEP_TOK), 0) + lo
                    hit = jnp.sum(jnp.where(ids == t_f, z, 0.0), axis=0, keepdims=True)
                    if p > 0:
                        part = run_s * jnp.exp(run_m - new_m) + part
                        hit = tacc + hit
                    run_m, run_s, tacc = new_m, part, hit
                    runmax[par, p:p + 1] = new_m
        if fwd:
            for j in range(CHIPS):
                cols = slice(j * PIECE, (j + 1) * PIECE)
                st_send[u, j:j + 1] = run_m[:, cols]
                st_send[u, CHIPS + j:CHIPS + j + 1] = run_s[:, cols]
            tgt_sum[...] += tacc
            pltpu.make_async_copy(st_send.at[u], st_recv.at[u, me], st_rsem.at[u]).start()
            for copy in stats_sends(u):
                copy.start()

    def late_chunks(s):
        for c in range(n_chunks):
            lo, n = c * CHUNK, chunk_rows(c)
            dw_acc[lo:lo + n] += jnp.dot(probs[s % 2, lo:lo + n].astype(jnp.bfloat16), hbuf[s], preferred_element_type=F32)

    def prepare(u):
        reduce_stages(u)
        h_stages(u)

    def own_piece(q):
        return pltpu.make_async_copy(hid.at[pl.ds(pl.multiple_of(q * PIECE, PIECE), PIECE)], piece(2 * q + core, chip), h_own.at[q])

    def start_piece(q, _):
        own_piece(q).start()
        return 0

    def wait_piece(q, _):
        own_piece(q).wait()
        return 0

    lax.fori_loop(0, steps // 2, start_piece, 0)
    w_copy = pltpu.make_async_copy(w_in, w, w_sem)
    w_copy.start()
    barrier = pltpu.get_barrier_semaphore()
    for i in range(1, 2 * CHIPS):
        pl.semaphore_signal(barrier, inc=1, device_id={"fsdp": (me + i) % (2 * CHIPS)}, device_id_type=pl.DeviceIdType.MESH)
    lax.fori_loop(0, steps // 2, wait_piece, 0)
    pl.semaphore_wait(barrier, 2 * CHIPS - 1)
    for copy in h_sends(0, True):
        copy.start()
    pltpu.make_async_copy(tgt, tbuf.at[me], t_sem).start()
    t_copies = [remote(tgt, tbuf.at[me], t_send, t_sem, (me + i) % (2 * CHIPS)) for i in range(1, 2 * CHIPS)]
    for copy in t_copies:
        copy.start()
    for copy in h_sends(1, True):
        copy.start()

    dw_acc[...] = jnp.zeros_like(dw_acc)
    tgt_sum[...] = jnp.zeros_like(tgt_sum)
    lse_sum[...] = jnp.zeros_like(lse_sum)
    w_copy.wait()
    for c in range(n_chunks):
        n = chunk_rows(c)
        wt[:, c * CHUNK:c * CHUNK + n] = w[c * CHUNK:c * CHUNK + n].T
    if last_rows < CHUNK:
        wt[:, vocab:] = jnp.zeros((width, n_chunks * CHUNK - vocab), jnp.bfloat16)

    @pl.when(core == 0)
    def _():
        h_ready(0, 0)
        h_forward(0).start()

    wait_bytes(tbuf, t_sem)

    def fwd_step(u, _):
        prepare(u)
        chunks(u, True, False)
        return 0

    def both_step(u, _):
        prepare(u)
        finish_stats(u - 2)
        chunks(u, True, True)
        return 0

    def bwd_step(u, _):
        prepare(u)
        finish_stats(u - 2)
        chunks(u, False, True, late_dw=True)
        return 0

    def late_step(u, _):
        reduce_stages(u)
        late_chunks(u - 4)
        return 0

    def tail_step(u, _):
        reduce_stages(u)
        return 0

    lax.fori_loop(0, 2, fwd_step, 0)
    lax.fori_loop(2, steps, both_step, 0)
    row = tgt_sum[...]
    tile = jnp.concatenate([row[:, j * PIECE:(j + 1) * PIECE] for j in range(CHIPS)] + [jnp.zeros((8 - CHIPS, PIECE), F32)], axis=0)
    tt_send[...] = tile
    pltpu.make_async_copy(tt_send, tt_recv.at[me], tt_sem.at[1]).start()
    for i in range(1, 2 * CHIPS):
        remote(tt_send, tt_recv.at[me], tt_sem.at[0], tt_sem.at[1], (me + i) % (2 * CHIPS)).start()
    lax.fori_loop(steps, steps + 2, bwd_step, 0)
    lax.fori_loop(steps + 2, steps + 4, late_step, 0)
    wait_bytes(tt_recv, tt_sem.at[1])
    loss_out[0] = (jnp.sum(lse_sum[...]) - jnp.sum(tt_recv[...])) * inv_tokens
    lax.fori_loop(steps + 4, steps + 6, tail_step, 0)

    wait_bytes(dh_out, out_sem)
    peers = 2 * CHIPS - 1
    wait_bytes(tbuf.at[:peers], t_send)
    wait_bytes(tt_recv.at[:peers], tt_sem.at[0])

    def drain_pieces(q, _):
        for i in range(2):
            wait_bytes(hbuf.at[0, pl.ds(0, PIECE)], h_send.at[i, q])

        @pl.when(2 * q < DIRECT)
        def _():
            wait_bytes(hbuf.at[0, pl.ds(0, PIECE)], h_send.at[2, q])

        @pl.when(2 * q >= DIRECT)
        def _():
            for i in range(2):
                wait_bytes(hbuf.at[0, pl.ds(0, PIECE // 2)], h_send.at[3 + i, q])

        wait_bytes(hbuf.at[0], fw_send.at[q])
        wait_bytes(out_stage.at[2 * q], out_send.at[q])
        return 0

    def drain_stats(s, _):
        wait_bytes(st_recv.at[s, :peers], st_ssem.at[s])
        return 0

    lax.fori_loop(0, steps // 2, drain_pieces, 0)
    lax.fori_loop(0, steps, drain_stats, 0)
    for sl in range(2):
        wait_bytes(r1_buf.at[sl], s1_sem.at[0, sl])
        wait_bytes(s2_buf.at[sl], s2_sem.at[0, sl])


def solution(mesh):
    groups = mesh.shape["fsdp"]
    tok_spec = P(("dp", "fsdp"), None)

    def local_head(hidden, targets, weight):
        tok_loc, width = hidden.shape
        vocab = weight.shape[0]
        steps = 2 * tok_loc // PIECE
        padded = -(-vocab // CHUNK) * CHUNK
        half = width // 2
        dma, bf16 = pltpu.SemaphoreType.DMA, jnp.bfloat16
        vmem = pl.BlockSpec(memory_space=pltpu.VMEM)
        hbm = pl.BlockSpec(memory_space=pltpu.HBM)
        scratch = [
            pltpu.VMEM((vocab, width), bf16),
            pltpu.VMEM((width, padded), bf16),
            pltpu.VMEM((2, vocab, STEP_TOK), F32),
            pltpu.VMEM((steps, STEP_TOK, width), bf16),
            pltpu.VMEM((groups, tok_loc // PIECE, PIECE), jnp.int32),
            pltpu.VMEM((CHUNK, STEP_TOK), F32), pltpu.VMEM((CHUNK, STEP_TOK), F32),
            pltpu.VMEM((CHUNK, STEP_TOK), bf16), pltpu.VMEM((CHUNK, STEP_TOK), bf16),
            pltpu.VMEM((2, width, STEP_TOK), F32),
            pltpu.VMEM((2, padded // CHUNK, STEP_TOK), F32),
            pltpu.VMEM((padded // CHUNK, STEP_TOK), F32),
            pltpu.VMEM((1, STEP_TOK), F32),
            pltpu.VMEM((CHIPS, PIECE), F32),
            pltpu.VMEM((steps, 8, PIECE), F32),
            pltpu.VMEM((steps, groups, 8, PIECE), F32),
            pltpu.VMEM((8, PIECE), F32),
            pltpu.VMEM((groups, 8, PIECE), F32),
            pltpu.VMEM((2, half, STEP_TOK), F32),
            pltpu.VMEM((2, CHIPS, half, PIECE), F32),
            pltpu.VMEM((2, 2, half, PIECE), F32),
            pltpu.VMEM((2, half, PIECE), F32),
            pltpu.VMEM((2, half, PIECE), F32),
            pltpu.VMEM((2, half, PIECE), F32),
            pltpu.VMEM((steps, PIECE, half), F32),
            dma(()), dma((steps // 2,)), dma((3, steps // 2)), dma((steps // 2,)),
            dma((5, steps // 2)), dma((steps // 2,)),
            dma(()), dma(()),
            dma((steps,)), dma((steps,)),
            dma((2,)), dma((2, 2)), dma((2, 2)), dma((2, 2)),
            dma(()), dma((steps // 2,)),
        ]
        flops = 6 * tok_loc * groups * vocab * width
        return pl.pallas_call(
            head_kernel,
            out_shape=(jax.ShapeDtypeStruct((1,), F32), pltpu.VMEM((tok_loc, width), F32), pltpu.VMEM((vocab, width), F32)),
            in_specs=[hbm, vmem, hbm],
            out_specs=(pl.BlockSpec(memory_space=pltpu.SMEM), vmem, vmem),
            scratch_shapes=scratch,
            compiler_params=pltpu.CompilerParams(collective_id=0, has_side_effects=True, vmem_limit_bytes=53_000_000),
            cost_estimate=pl.CostEstimate(flops=flops, bytes_accessed=20_000_000, transcendentals=tok_loc * groups * vocab),
        )(hidden, targets.reshape(tok_loc // PIECE, PIECE), weight)

    return jax.shard_map(local_head, mesh=mesh, in_specs=(tok_spec, P(("dp", "fsdp")), P("fsdp", None)), out_specs=(P("dp"), tok_spec, tok_spec), check_vma=False)
```

```python
import functools

import jax
import jax.numpy as jnp
from jax import lax
from jax.experimental import pallas as pl
from jax.experimental.pallas import tpu as pltpu
from jax.sharding import PartitionSpec as P

PIECE = 128
CHIPS = 4
STEP_TOK = PIECE * CHIPS
TILE = 64
SLOTS = 4
DIRECT = 4
CHUNK = 512
F32 = jnp.float32


def head_kernel(hid, tgt, w_in, loss_out, dh_out, dw_out, w, wt, probs, hbuf, tbuf, zbuf_a, zbuf_b, dz_a, dz_b, dh_acc,
                runmax, factor, tgt_sum, lse_sum, st_send, st_recv, tt_send, tt_recv, pair_buf, s1_buf, r1_buf, s2_buf, r2_buf,
                own_buf, out_stage, w_sem, h_own, h_recv, h_fwd, h_send, fw_send, t_sem, t_send, st_rsem, st_ssem, tt_sem, pair_sem,
                s1_sem, s2_sem, out_sem, out_send):
    tok_loc, width = hid.shape
    vocab = w.shape[0]
    steps = 2 * tok_loc // PIECE
    tokens = tok_loc * 2 * CHIPS
    half = width // 2
    n_chunks = -(-vocab // CHUNK)
    last_rows = vocab - (n_chunks - 1) * CHUNK
    inv_tokens = 1.0 / tokens
    dw_acc = dw_out
    zbufs, dzs = (zbuf_a, zbuf_b), (dz_a, dz_b)

    me = lax.axis_index("fsdp")
    core, chip = me % 2, me // 2
    x, y = chip % 2, chip // 2
    partner = chip * 2 + 1 - core
    chip_x, chip_y, chip_d = y * 2 + (1 - x), (1 - y) * 2 + x, (1 - y) * 2 + (1 - x)
    chip_1 = (1 - core) * chip_x + core * chip_y
    chip_2 = (1 - core) * chip_y + core * chip_x

    def remote(src, dst, send, recv, dev):
        return pltpu.make_async_remote_copy(src_ref=src, dst_ref=dst, send_sem=send, recv_sem=recv, device_id={"fsdp": dev},
                                            device_id_type=pl.DeviceIdType.MESH)

    def wait_bytes(ref, sem):
        pltpu.make_async_copy(ref, ref, sem).wait()

    def chunk_rows(c):
        return CHUNK if c < n_chunks - 1 else last_rows

    def piece(s, of_chip, lo=0, n=PIECE):
        return hbuf.at[s, pl.ds(pl.multiple_of(of_chip * PIECE + lo, n), n)]

    def h_sends(q, direct):
        s = 2 * q + core
        peers = (chip_x, chip_y, chip_d)[:3 if direct else 2]
        return [remote(piece(s, chip), piece(s, chip), h_send.at[i, q], h_recv.at[i, q], peer * 2 + core) for i, peer in enumerate(peers)]

    def h_relays(s):
        q = s // 2
        return [remote(piece(s, src, lo, PIECE // 2), piece(s, src, lo, PIECE // 2), h_send.at[3 + i, q], h_recv.at[2, q], dst * 2 + core)
                for i, (src, dst, lo) in enumerate(((chip_x, chip_y, 0), (chip_y, chip_x, PIECE // 2)))]

    def h_forward(s):
        return remote(hbuf.at[s], hbuf.at[s], fw_send.at[s // 2], h_fwd.at[s // 2], partner)

    def stats_sends(s):
        return [remote(st_send.at[s], st_recv.at[s, me], st_ssem.at[s], st_rsem.at[s], (me + i) % (2 * CHIPS)) for i in range(1, 2 * CHIPS)]

    def pair_copy(s):
        rows = pl.ds(pl.multiple_of((1 - core) * half, half), half)
        return remote(dh_acc.at[s % 2, rows], pair_buf.at[s % 2], pair_sem.at[0, s % 2], pair_sem.at[1, s % 2], partner)

    def s1_copies(s):
        sl = s % SLOTS
        return [remote(s1_buf.at[sl, block], r1_buf.at[sl, i], s1_sem.at[0, sl], s1_sem.at[1, sl], chip_1 * 2 + core)
                for i, block in enumerate((chip_1, chip_d))]

    def s2_copy(s):
        return remote(s2_buf.at[s % SLOTS], r2_buf.at[s % SLOTS], s2_sem.at[0, s % SLOTS], s2_sem.at[1, s % SLOTS], chip_2 * 2 + core)

    def out_dst(s):
        return dh_out.at[pl.ds(pl.multiple_of(s // 2 * PIECE, PIECE), PIECE), pl.ds(pl.multiple_of(core * half, half), half)]

    def out_remote(s):
        return remote(out_stage.at[s], out_dst(s), out_send.at[s // 2], out_sem, partner)

    def reduce_stages(u):
        @pl.when((u >= 8) & (u < steps + 8))
        def _():
            s = u - 8
            sl = s % SLOTS
            wait_bytes(r2_buf.at[sl], s2_sem.at[1, sl])
            out_stage[s] = (own_buf[sl] + r2_buf[sl]).T

            @pl.when(s % 2 == core)
            def _():
                pltpu.make_async_copy(out_stage.at[s], out_dst(s), out_sem).start()

            @pl.when(s % 2 != core)
            def _():
                out_remote(s).start()

        @pl.when((u >= 6) & (u < steps + 6))
        def _():
            s = u - 6
            sl = s % SLOTS
            wait_bytes(r1_buf.at[sl], s1_sem.at[1, sl])

            @pl.when(s >= SLOTS)
            def _():
                wait_bytes(s2_buf.at[sl], s2_sem.at[0, sl])

            s2_buf[sl] = s1_buf[sl, chip_2] + r1_buf[sl, 1]
            own_buf[sl] = s1_buf[sl, chip] + r1_buf[sl, 0]
            s2_copy(s).start()

        @pl.when((u >= 4) & (u < steps + 4))
        def _():
            s = u - 4
            sl = s % 2
            sl1 = s % SLOTS
            wait_bytes(pair_buf.at[sl], pair_sem.at[1, sl])
            wait_bytes(pair_buf.at[sl], pair_sem.at[0, sl])

            @pl.when(s >= SLOTS)
            def _():
                wait_bytes(r1_buf.at[sl1], s1_sem.at[0, sl1])

            rows = pl.ds(pl.multiple_of(core * half, half), half)
            for j in range(CHIPS):
                cols = pl.ds(j * PIECE, PIECE)
                s1_buf[sl1, j] = dh_acc[sl, rows, cols] + pair_buf[sl, :, cols]
            for copy in s1_copies(s):
                copy.start()

        @pl.when((u >= 3) & (u < steps + 3))
        def _():
            pair_copy(u - 3).start()

    def first_set(u):
        return jnp.minimum(DIRECT + u + 2 * jnp.clip(u - 2, 0, 2), steps)

    def h_ready(s, lo):
        for i in range(lo, 3):
            wait_bytes(hbuf.at[s, pl.ds(0, PIECE)], h_recv.at[i, s // 2])

    def h_stages(u):
        for i in range(3):
            @pl.when((first_set(u) + i < first_set(u + 1)) & ((first_set(u) + i) % 2 == core))
            def _():
                for copy in h_sends((first_set(u) + i) // 2, False):
                    copy.start()

        @pl.when((u + 2 >= DIRECT) & (u + 2 < steps) & (u % 2 == core))
        def _():
            for i in range(2):
                wait_bytes(hbuf.at[u + 2, pl.ds(0, PIECE)], h_recv.at[i, (u + 2) // 2])
            for copy in h_relays(u + 2):
                copy.start()

        @pl.when((u + 1 < DIRECT) & ((u + 1) % 2 == core))
        def _():
            h_ready(u + 1, 0)
            h_forward(u + 1).start()

        @pl.when((u + 1 >= DIRECT) & (u + 1 < steps) & ((u + 1) % 2 == core))
        def _():
            h_ready(u + 1, 2)
            h_forward(u + 1).start()

        @pl.when((u < steps) & (u % 2 != core))
        def _():
            wait_bytes(hbuf.at[u], h_fwd.at[u // 2])

    def row_ids(lo, n):
        return jnp.concatenate([lax.broadcasted_iota(jnp.int32, (n, PIECE), 0) + lo] * CHIPS, axis=1)

    def target_row(s):
        row = jnp.concatenate([tbuf[2 * j + s % 2, pl.ds(s // 2, 1), :] for j in range(CHIPS)], axis=1)
        return row - me * vocab

    def finish_stats(s):
        wait_bytes(st_recv.at[s], st_rsem.at[s])
        stats = st_recv[s]
        m, e = stats[:, :CHIPS], stats[:, CHIPS:]
        top = jnp.max(m, axis=0)
        lse = top + jnp.log(jnp.sum(e * jnp.exp(m - top[None]), axis=0))
        lse_sum[...] += lse
        lse_row = jnp.concatenate([lse[j:j + 1] for j in range(CHIPS)], axis=1)
        factor[...] = jnp.exp(runmax[s % 2] - lse_row) * inv_tokens

    def chunks(u, fwd, bwd, late_dw=False):
        par = u % 2
        if fwd:
            h_f = hbuf.at[u]
            t_f = target_row(u)
        if bwd:
            s = u - 2
            h_b = hbuf.at[s]
            t_b = target_row(s)
        run_m = run_s = tacc = new_m = None
        for c in range(n_chunks + 1):
            if c > 0 and fwd:
                p, m = c - 1, new_m
            if c < n_chunks:
                lo, n = c * CHUNK, chunk_rows(c)
                if bwd:
                    dz_ref = dzs[c % 2]
                    for r in range(0, n, TILE):
                        k = min(TILE, n - r)
                        hot = jnp.where(row_ids(lo + r, k) == t_b, inv_tokens, 0.0)
                        dz = (probs[par, lo + r:lo + r + k] * factor[c:c + 1] - hot).astype(jnp.bfloat16)
                        dz_ref[r:r + k] = dz
                        if late_dw:
                            probs[par, lo + r:lo + r + k] = dz.astype(F32)
                    if n < CHUNK:
                        dz_ref[n:] = jnp.zeros((CHUNK - n, STEP_TOK), jnp.bfloat16)
                if fwd:
                    z = lax.dot_general(w[lo:lo + n], h_f[...], (((1,), (1,)), ((), ())), preferred_element_type=F32)
                    zbufs[c % 2][:n] = z
                    new_m = jnp.max(z, axis=0, keepdims=True)
                    if c > 0:
                        new_m = jnp.maximum(new_m, m)
                    runmax[par, c:c + 1] = new_m
            if c > 0:
                p = c - 1
                lo, n = p * CHUNK, chunk_rows(p)
                if bwd:
                    dz_ref = dzs[p % 2]
                    part = jnp.dot(wt[:, lo:lo + CHUNK], dz_ref[...], preferred_element_type=F32)
                    if p == 0:
                        dh_acc[par] = part
                    else:
                        dh_acc[par] += part
                    if not late_dw:
                        dw_acc[lo:lo + n] += jnp.dot(dz_ref[:n], h_b[...], preferred_element_type=F32)
                if fwd:
                    part = hit = None
                    for r in range(0, n, TILE):
                        k = min(TILE, n - r)
                        z = zbufs[p % 2][r:r + k]
                        e = jnp.exp(z - m)
                        probs[par, lo + r:lo + r + k] = e
                        e = jnp.sum(e.reshape(k // 8, 8, STEP_TOK), axis=0)
                        t = jnp.sum(jnp.where(row_ids(lo + r, k) == t_f, z, 0.0).reshape(k // 8, 8, STEP_TOK), axis=0)
                        part, hit = (e, t) if part is None else (part + e, hit + t)
                    if p > 0:
                        part = run_s * jnp.exp(run_m - m) + part
                        hit = tacc + hit
                    run_m, run_s, tacc = m, part, hit
        if fwd:
            run_s = jnp.sum(run_s, axis=0, keepdims=True)
            tacc = jnp.sum(tacc, axis=0, keepdims=True)
        if fwd:
            for j in range(CHIPS):
                cols = slice(j * PIECE, (j + 1) * PIECE)
                st_send[u, j:j + 1] = run_m[:, cols]
                st_send[u, CHIPS + j:CHIPS + j + 1] = run_s[:, cols]
            tgt_sum[...] += tacc
            pltpu.make_async_copy(st_send.at[u], st_recv.at[u, me], st_rsem.at[u]).start()
            for copy in stats_sends(u):
                copy.start()

    def late_chunks(s):
        for c in range(n_chunks):
            lo, n = c * CHUNK, chunk_rows(c)
            dw_acc[lo:lo + n] += jnp.dot(probs[s % 2, lo:lo + n].astype(jnp.bfloat16), hbuf[s], preferred_element_type=F32)

    def prepare(u):
        reduce_stages(u)
        h_stages(u)

    def own_piece(q):
        return pltpu.make_async_copy(hid.at[pl.ds(pl.multiple_of(q * PIECE, PIECE), PIECE)], piece(2 * q + core, chip), h_own.at[q])

    def start_piece(q, _):
        own_piece(q).start()
        return 0

    def wait_piece(q, _):
        own_piece(q).wait()
        return 0

    lax.fori_loop(0, steps // 2, start_piece, 0)
    w_copy = pltpu.make_async_copy(w_in, w, w_sem)
    w_copy.start()
    barrier = pltpu.get_barrier_semaphore()
    for i in range(1, 2 * CHIPS):
        pl.semaphore_signal(barrier, inc=1, device_id={"fsdp": (me + i) % (2 * CHIPS)}, device_id_type=pl.DeviceIdType.MESH)
    lax.fori_loop(0, steps // 2, wait_piece, 0)
    pl.semaphore_wait(barrier, 2 * CHIPS - 1)
    for copy in h_sends(0, True):
        copy.start()
    pltpu.make_async_copy(tgt, tbuf.at[me], t_sem).start()
    t_copies = [remote(tgt, tbuf.at[me], t_send, t_sem, (me + i) % (2 * CHIPS)) for i in range(1, 2 * CHIPS)]
    for copy in t_copies:
        copy.start()
    for copy in h_sends(1, True):
        copy.start()

    dw_acc[...] = jnp.zeros_like(dw_acc)
    tgt_sum[...] = jnp.zeros_like(tgt_sum)
    lse_sum[...] = jnp.zeros_like(lse_sum)
    w_copy.wait()
    for c in range(n_chunks):
        n = chunk_rows(c)
        wt[:, c * CHUNK:c * CHUNK + n] = w[c * CHUNK:c * CHUNK + n].T
    if last_rows < CHUNK:
        wt[:, vocab:] = jnp.zeros((width, n_chunks * CHUNK - vocab), jnp.bfloat16)

    @pl.when(core == 0)
    def _():
        h_ready(0, 0)
        h_forward(0).start()

    wait_bytes(tbuf, t_sem)

    def fwd_step(u, _):
        prepare(u)
        chunks(u, True, False)
        return 0

    def both_step(u, _):
        prepare(u)
        finish_stats(u - 2)
        chunks(u, True, True)
        return 0

    def bwd_step(u, _):
        prepare(u)
        finish_stats(u - 2)
        chunks(u, False, True, late_dw=True)
        return 0

    def late_step(u, _):
        reduce_stages(u)
        late_chunks(u - 4)
        return 0

    def tail_step(u, _):
        reduce_stages(u)
        return 0

    lax.fori_loop(0, 2, fwd_step, 0)
    lax.fori_loop(2, steps, both_step, 0)
    row = tgt_sum[...]
    tile = jnp.concatenate([row[:, j * PIECE:(j + 1) * PIECE] for j in range(CHIPS)] + [jnp.zeros((8 - CHIPS, PIECE), F32)], axis=0)
    tt_send[...] = tile
    pltpu.make_async_copy(tt_send, tt_recv.at[me], tt_sem.at[1]).start()
    for i in range(1, 2 * CHIPS):
        remote(tt_send, tt_recv.at[me], tt_sem.at[0], tt_sem.at[1], (me + i) % (2 * CHIPS)).start()
    lax.fori_loop(steps, steps + 2, bwd_step, 0)
    lax.fori_loop(steps + 2, steps + 4, late_step, 0)
    wait_bytes(tt_recv, tt_sem.at[1])
    loss_out[0] = (jnp.sum(lse_sum[...]) - jnp.sum(tt_recv[...])) * inv_tokens
    lax.fori_loop(steps + 4, steps + 8, tail_step, 0)

    wait_bytes(dh_out, out_sem)
    peers = 2 * CHIPS - 1
    wait_bytes(tbuf.at[:peers], t_send)
    wait_bytes(tt_recv.at[:peers], tt_sem.at[0])

    def drain_pieces(q, _):
        for i in range(2):
            wait_bytes(hbuf.at[0, pl.ds(0, PIECE)], h_send.at[i, q])

        @pl.when(2 * q < DIRECT)
        def _():
            wait_bytes(hbuf.at[0, pl.ds(0, PIECE)], h_send.at[2, q])

        @pl.when(2 * q >= DIRECT)
        def _():
            for i in range(2):
                wait_bytes(hbuf.at[0, pl.ds(0, PIECE // 2)], h_send.at[3 + i, q])

        wait_bytes(hbuf.at[0], fw_send.at[q])
        wait_bytes(out_stage.at[2 * q], out_send.at[q])
        return 0

    def drain_stats(s, _):
        wait_bytes(st_recv.at[s, :peers], st_ssem.at[s])
        return 0

    lax.fori_loop(0, steps // 2, drain_pieces, 0)
    lax.fori_loop(0, steps, drain_stats, 0)
    for sl in range(SLOTS):
        wait_bytes(r1_buf.at[sl], s1_sem.at[0, sl])
        wait_bytes(s2_buf.at[sl], s2_sem.at[0, sl])


def solution(mesh):
    groups = mesh.shape["fsdp"]
    tok_spec = P(("dp", "fsdp"), None)

    def local_head(hidden, targets, weight):
        tok_loc, width = hidden.shape
        vocab = weight.shape[0]
        steps = 2 * tok_loc // PIECE
        padded = -(-vocab // CHUNK) * CHUNK
        half = width // 2
        dma, bf16 = pltpu.SemaphoreType.DMA, jnp.bfloat16
        vmem = pl.BlockSpec(memory_space=pltpu.VMEM)
        hbm = pl.BlockSpec(memory_space=pltpu.HBM)
        scratch = [
            pltpu.VMEM((vocab, width), bf16),
            pltpu.VMEM((width, padded), bf16),
            pltpu.VMEM((2, vocab, STEP_TOK), F32),
            pltpu.VMEM((steps, STEP_TOK, width), bf16),
            pltpu.VMEM((groups, tok_loc // PIECE, PIECE), jnp.int32),
            pltpu.VMEM((CHUNK, STEP_TOK), F32), pltpu.VMEM((CHUNK, STEP_TOK), F32),
            pltpu.VMEM((CHUNK, STEP_TOK), bf16), pltpu.VMEM((CHUNK, STEP_TOK), bf16),
            pltpu.VMEM((2, width, STEP_TOK), F32),
            pltpu.VMEM((2, padded // CHUNK, STEP_TOK), F32),
            pltpu.VMEM((padded // CHUNK, STEP_TOK), F32),
            pltpu.VMEM((1, STEP_TOK), F32),
            pltpu.VMEM((CHIPS, PIECE), F32),
            pltpu.VMEM((steps, 8, PIECE), F32),
            pltpu.VMEM((steps, groups, 8, PIECE), F32),
            pltpu.VMEM((8, PIECE), F32),
            pltpu.VMEM((groups, 8, PIECE), F32),
            pltpu.VMEM((2, half, STEP_TOK), F32),
            pltpu.VMEM((SLOTS, CHIPS, half, PIECE), F32),
            pltpu.VMEM((SLOTS, 2, half, PIECE), F32),
            pltpu.VMEM((SLOTS, half, PIECE), F32),
            pltpu.VMEM((SLOTS, half, PIECE), F32),
            pltpu.VMEM((SLOTS, half, PIECE), F32),
            pltpu.VMEM((steps, PIECE, half), F32),
            dma(()), dma((steps // 2,)), dma((3, steps // 2)), dma((steps // 2,)),
            dma((5, steps // 2)), dma((steps // 2,)),
            dma(()), dma(()),
            dma((steps,)), dma((steps,)),
            dma((2,)), dma((2, 2)), dma((2, SLOTS)), dma((2, SLOTS)),
            dma(()), dma((steps // 2,)),
        ]
        flops = 6 * tok_loc * groups * vocab * width
        return pl.pallas_call(
            head_kernel,
            out_shape=(jax.ShapeDtypeStruct((1,), F32), pltpu.VMEM((tok_loc, width), F32), pltpu.VMEM((vocab, width), F32)),
            in_specs=[hbm, vmem, hbm],
            out_specs=(pl.BlockSpec(memory_space=pltpu.SMEM), vmem, vmem),
            scratch_shapes=scratch,
            compiler_params=pltpu.CompilerParams(collective_id=0, has_side_effects=True, vmem_limit_bytes=56_000_000),
            cost_estimate=pl.CostEstimate(flops=flops, bytes_accessed=20_000_000, transcendentals=tok_loc * groups * vocab),
        )(hidden, targets.reshape(tok_loc // PIECE, PIECE), weight)

    return jax.shard_map(local_head, mesh=mesh, in_specs=(tok_spec, P(("dp", "fsdp")), P("fsdp", None)), out_specs=(P("dp"), tok_spec, tok_spec), check_vma=False)
```

```python
import functools

import jax
import jax.numpy as jnp
from jax import lax
from jax.experimental import pallas as pl
from jax.experimental.pallas import tpu as pltpu
from jax.sharding import PartitionSpec as P

PIECE = 128
CHIPS = 4
STEP_TOK = PIECE * CHIPS
GROUP = 1
TILE = 64
SLOTS = 4
DIRECT = 6
CHUNK = 512
F32 = jnp.float32


def head_kernel(hid, tgt, w_in, loss_out, dh_out, dw_out, w, wt, probs, hbuf, tbuf, zbuf_a, zbuf_b, dz_a, dz_b, dh_acc,
                runmax, factor, tgt_sum, lse_sum, st_send, st_recv, tt_send, tt_recv, pair_buf, s1_buf, r1_buf, s2_buf, r2_buf,
                own_buf, out_stage, w_sem, h_own, h_recv, h_fwd, h_send, fw_send, t_sem, t_send, st_rsem, st_ssem, tt_sem, pair_sem,
                s1_sem, s2_sem, out_sem, out_send):
    tok_loc, width = hid.shape
    vocab = w.shape[0]
    steps = 2 * tok_loc // PIECE
    tokens = tok_loc * 2 * CHIPS
    half = width // 2
    n_chunks = -(-vocab // CHUNK)
    last_rows = vocab - (n_chunks - 1) * CHUNK
    inv_tokens = 1.0 / tokens
    dw_acc = dw_out
    zbufs, dzs = (zbuf_a, zbuf_b), (dz_a, dz_b)

    me = lax.axis_index("fsdp")
    core, chip = me % 2, me // 2
    x, y = chip % 2, chip // 2
    partner = chip * 2 + 1 - core
    chip_x, chip_y, chip_d = y * 2 + (1 - x), (1 - y) * 2 + x, (1 - y) * 2 + (1 - x)
    chip_1 = (1 - core) * chip_x + core * chip_y
    chip_2 = (1 - core) * chip_y + core * chip_x

    def remote(src, dst, send, recv, dev):
        return pltpu.make_async_remote_copy(src_ref=src, dst_ref=dst, send_sem=send, recv_sem=recv, device_id={"fsdp": dev},
                                            device_id_type=pl.DeviceIdType.MESH)

    def wait_bytes(ref, sem):
        pltpu.make_async_copy(ref, ref, sem).wait()

    def chunk_rows(c):
        return CHUNK if c < n_chunks - 1 else last_rows

    def piece(s, of_chip, lo=0, n=PIECE):
        return hbuf.at[s, pl.ds(pl.multiple_of(of_chip * PIECE + lo, n), n)]

    def h_sends(q, direct):
        s = 2 * q + core
        peers = (chip_x, chip_y, chip_d)[:3 if direct else 2]
        return [remote(piece(s, chip), piece(s, chip), h_send.at[i, q], h_recv.at[i, q], peer * 2 + core) for i, peer in enumerate(peers)]

    def h_relays(s):
        q = s // 2
        return [remote(piece(s, src, lo, PIECE // 2), piece(s, src, lo, PIECE // 2), h_send.at[3 + i, q], h_recv.at[2, q], dst * 2 + core)
                for i, (src, dst, lo) in enumerate(((chip_x, chip_y, 0), (chip_y, chip_x, PIECE // 2)))]

    def h_forward(s):
        return remote(hbuf.at[s], hbuf.at[s], fw_send.at[s // 2], h_fwd.at[s // 2], partner)

    def stats_sends(s):
        return [remote(st_send.at[s], st_recv.at[s, me], st_ssem.at[s], st_rsem.at[s], (me + i) % (2 * CHIPS)) for i in range(1, 2 * CHIPS)]

    def pair_copy(s):
        rows = pl.ds(pl.multiple_of((1 - core) * half, half), half)
        return remote(dh_acc.at[s % 2, rows], pair_buf.at[s % 2], pair_sem.at[0, s % 2], pair_sem.at[1, s % 2], partner)

    def s1_copies(s):
        sl = s % SLOTS
        return [remote(s1_buf.at[sl, block], r1_buf.at[sl, i], s1_sem.at[0, sl], s1_sem.at[1, sl], chip_1 * 2 + core)
                for i, block in enumerate((chip_1, chip_d))]

    def s2_copy(s):
        return remote(s2_buf.at[s % SLOTS], r2_buf.at[s % SLOTS], s2_sem.at[0, s % SLOTS], s2_sem.at[1, s % SLOTS], chip_2 * 2 + core)

    def out_dst(s):
        return dh_out.at[pl.ds(pl.multiple_of(s // 2 * PIECE, PIECE), PIECE), pl.ds(pl.multiple_of(core * half, half), half)]

    def out_remote(s):
        return remote(out_stage.at[s], out_dst(s), out_send.at[s // 2], out_sem, partner)

    def reduce_stages(u):
        @pl.when((u >= 8) & (u < steps + 8))
        def _():
            s = u - 8
            sl = s % SLOTS
            wait_bytes(r2_buf.at[sl], s2_sem.at[1, sl])
            out_stage[s] = (own_buf[sl] + r2_buf[sl]).T

            @pl.when(s % 2 == core)
            def _():
                pltpu.make_async_copy(out_stage.at[s], out_dst(s), out_sem).start()

            @pl.when(s % 2 != core)
            def _():
                out_remote(s).start()

        @pl.when((u >= 6) & (u < steps + 6))
        def _():
            s = u - 6
            sl = s % SLOTS
            wait_bytes(r1_buf.at[sl], s1_sem.at[1, sl])

            @pl.when(s >= SLOTS)
            def _():
                wait_bytes(s2_buf.at[sl], s2_sem.at[0, sl])

            s2_buf[sl] = s1_buf[sl, chip_2] + r1_buf[sl, 1]
            own_buf[sl] = s1_buf[sl, chip] + r1_buf[sl, 0]
            s2_copy(s).start()

        @pl.when((u >= 4) & (u < steps + 4))
        def _():
            s = u - 4
            sl = s % 2
            sl1 = s % SLOTS
            wait_bytes(pair_buf.at[sl], pair_sem.at[1, sl])
            wait_bytes(pair_buf.at[sl], pair_sem.at[0, sl])

            @pl.when(s >= SLOTS)
            def _():
                wait_bytes(r1_buf.at[sl1], s1_sem.at[0, sl1])

            rows = pl.ds(pl.multiple_of(core * half, half), half)
            for j in range(CHIPS):
                cols = pl.ds(j * PIECE, PIECE)
                s1_buf[sl1, j] = dh_acc[sl, rows, cols] + pair_buf[sl, :, cols]
            for copy in s1_copies(s):
                copy.start()

        @pl.when((u >= 3) & (u < steps + 3))
        def _():
            pair_copy(u - 3).start()

    def first_set(u):
        return jnp.minimum(4 + u + 2 * jnp.clip(u - 2, 0, 2), steps)

    def h_ready(s, lo):
        for i in range(lo, 3):
            wait_bytes(hbuf.at[s, pl.ds(0, PIECE)], h_recv.at[i, s // 2])

    def h_stages(u):
        for i in range(3):
            @pl.when((first_set(u) + i < first_set(u + 1)) & ((first_set(u) + i) % 2 == core))
            def _():
                for j, copy in enumerate(h_sends((first_set(u) + i) // 2, True)):
                    if j < 2:
                        copy.start()
                    else:
                        pl.when(u < 2)(lambda copy=copy: copy.start())

        @pl.when((u + 3 >= DIRECT) & (u + 3 < steps) & ((u + 3) % 2 == core))
        def _():
            for i in range(2):
                wait_bytes(hbuf.at[u + 3, pl.ds(0, PIECE)], h_recv.at[i, (u + 3) // 2])
            for copy in h_relays(u + 3):
                copy.start()

        @pl.when((u + 1 < DIRECT) & ((u + 1) % 2 == core))
        def _():
            h_ready(u + 1, 0)
            h_forward(u + 1).start()

        @pl.when((u + 1 >= DIRECT) & (u + 1 < steps) & ((u + 1) % 2 == core))
        def _():
            h_ready(u + 1, 2)
            h_forward(u + 1).start()

        @pl.when((u < steps) & (u % 2 != core))
        def _():
            wait_bytes(hbuf.at[u], h_fwd.at[u // 2])

    def row_ids(lo, n):
        return jnp.concatenate([lax.broadcasted_iota(jnp.int32, (n, PIECE), 0) + lo] * CHIPS, axis=1)

    def target_row(s):
        row = jnp.concatenate([tbuf[2 * j + s % 2, pl.ds(s // 2, 1), :] for j in range(CHIPS)], axis=1)
        return row - me * vocab

    def finish_stats(s):
        wait_bytes(st_recv.at[s], st_rsem.at[s])
        stats = st_recv[s]
        m, e = stats[:, :CHIPS], stats[:, CHIPS:]
        top = jnp.max(m, axis=0)
        lse = top + jnp.log(jnp.sum(e * jnp.exp(m - top[None]), axis=0))
        lse_sum[...] += lse
        lse_row = jnp.concatenate([lse[j:j + 1] for j in range(CHIPS)], axis=1)
        factor[...] = jnp.exp(runmax[s % 2] - lse_row) * inv_tokens

    def chunks(u, fwd, bwd, late_dw=False):
        par = u % 2
        if fwd:
            h_f = hbuf.at[u]
            t_f = target_row(u)
        if bwd:
            s = u - 2
            h_b = hbuf.at[s]
            t_b = target_row(s)
        run_m = run_s = new_m = m = None
        tacc = jnp.zeros((8, STEP_TOK), F32)
        for c in range(n_chunks + 1):
            m = new_m
            if c < n_chunks and bwd:
                lo, n = c * CHUNK, chunk_rows(c)
                dz_ref, at = dzs[c // GROUP % 2], c % GROUP * CHUNK
                for r in range(0, n, TILE):
                    k = min(TILE, n - r)
                    hot = jnp.where(row_ids(lo + r, k) == t_b, inv_tokens, 0.0)
                    dz = probs[par, lo + r:lo + r + k] * factor[c:c + 1] - hot
                    dz_ref[at + r:at + r + k] = dz.astype(jnp.bfloat16)
                    if late_dw:
                        probs[par, lo + r:lo + r + k] = dz
                if n < CHUNK:
                    dz_ref[at + n:at + CHUNK] = jnp.zeros((CHUNK - n, STEP_TOK), jnp.bfloat16)
            if c < n_chunks and fwd:
                lo, n = c * CHUNK, chunk_rows(c)
                z = lax.dot_general(w[lo:lo + n], h_f[...], (((1,), (1,)), ((), ())), preferred_element_type=F32)
                zbufs[c % 2][:n] = z
                new_m = jnp.max(z, axis=0, keepdims=True)
                if c > 0:
                    new_m = jnp.maximum(new_m, m)
                runmax[par, c:c + 1] = new_m
            if c > 0 and bwd and (c % GROUP == 0 or c == n_chunks):
                g = (c - 1) // GROUP
                lo = g * GROUP * CHUNK
                n = min(GROUP * CHUNK, vocab - lo)
                k = -(-n // CHUNK) * CHUNK
                dz_ref = dzs[g % 2]
                part = jnp.dot(wt[:, lo:lo + k], dz_ref[:k], preferred_element_type=F32)
                if g == 0:
                    dh_acc[par] = part
                else:
                    dh_acc[par] += part
                if not late_dw:
                    dw_acc[lo:lo + n] += jnp.dot(dz_ref[:n], h_b[...], preferred_element_type=F32)
            if c > 0 and fwd:
                p = c - 1
                lo, n = p * CHUNK, chunk_rows(p)
                part = None
                for r in range(0, n, TILE):
                    k = min(TILE, n - r)
                    z = zbufs[p % 2][r:r + k]
                    e = jnp.exp(z - m)
                    probs[par, lo + r:lo + r + k] = e
                    e = jnp.sum(e.reshape(k // 8, 8, STEP_TOK), axis=0)
                    part = e if part is None else part + e
                    for i in range(0, k, 8):
                        tacc = jnp.where(row_ids(lo + r + i, 8) == t_f, z[i:i + 8], tacc)
                if p > 0:
                    part = run_s * jnp.exp(run_m - m) + part
                run_m, run_s = m, part
        if fwd:
            run_s = jnp.sum(run_s, axis=0, keepdims=True)
            tacc = jnp.sum(tacc, axis=0, keepdims=True)
        if fwd:
            for j in range(CHIPS):
                cols = slice(j * PIECE, (j + 1) * PIECE)
                st_send[u, j:j + 1] = run_m[:, cols]
                st_send[u, CHIPS + j:CHIPS + j + 1] = run_s[:, cols]
            tgt_sum[...] += tacc
            pltpu.make_async_copy(st_send.at[u], st_recv.at[u, me], st_rsem.at[u]).start()
            for copy in stats_sends(u):
                copy.start()

    def late_chunks(s):
        for c in range(n_chunks):
            lo, n = c * CHUNK, chunk_rows(c)
            dw_acc[lo:lo + n] += jnp.dot(probs[s % 2, lo:lo + n].astype(jnp.bfloat16), hbuf[s], preferred_element_type=F32)

    def prepare(u):
        reduce_stages(u)
        h_stages(u)

    def own_piece(q):
        return pltpu.make_async_copy(hid.at[pl.ds(pl.multiple_of(q * PIECE, PIECE), PIECE)], piece(2 * q + core, chip), h_own.at[q])

    def start_piece(q, _):
        own_piece(q).start()
        return 0

    def wait_piece(q, _):
        own_piece(q).wait()
        return 0

    lax.fori_loop(0, steps // 2, start_piece, 0)
    w_copy = pltpu.make_async_copy(w_in, w, w_sem)
    w_copy.start()
    barrier = pltpu.get_barrier_semaphore()
    for i in range(1, 2 * CHIPS):
        pl.semaphore_signal(barrier, inc=1, device_id={"fsdp": (me + i) % (2 * CHIPS)}, device_id_type=pl.DeviceIdType.MESH)
    lax.fori_loop(0, steps // 2, wait_piece, 0)
    pl.semaphore_wait(barrier, 2 * CHIPS - 1)
    for copy in h_sends(0, True):
        copy.start()
    pltpu.make_async_copy(tgt, tbuf.at[me], t_sem).start()
    t_copies = [remote(tgt, tbuf.at[me], t_send, t_sem, (me + i) % (2 * CHIPS)) for i in range(1, 2 * CHIPS)]
    for copy in t_copies:
        copy.start()
    for copy in h_sends(1, True):
        copy.start()

    dw_acc[...] = jnp.zeros_like(dw_acc)
    tgt_sum[...] = jnp.zeros_like(tgt_sum)
    lse_sum[...] = jnp.zeros_like(lse_sum)
    w_copy.wait()
    for c in range(n_chunks):
        n = chunk_rows(c)
        wt[:, c * CHUNK:c * CHUNK + n] = w[c * CHUNK:c * CHUNK + n].T
    if last_rows < CHUNK:
        wt[:, vocab:] = jnp.zeros((width, n_chunks * CHUNK - vocab), jnp.bfloat16)

    @pl.when(core == 0)
    def _():
        h_ready(0, 0)
        h_forward(0).start()

    wait_bytes(tbuf, t_sem)

    def fwd_step(u, _):
        prepare(u)
        chunks(u, True, False)
        return 0

    def both_step(u, _):
        prepare(u)
        finish_stats(u - 2)
        chunks(u, True, True)
        return 0

    def bwd_step(u, _):
        prepare(u)
        finish_stats(u - 2)
        chunks(u, False, True, late_dw=True)
        return 0

    def late_step(u, _):
        reduce_stages(u)
        late_chunks(u - 4)
        return 0

    def tail_step(u, _):
        reduce_stages(u)
        return 0

    lax.fori_loop(0, 2, fwd_step, 0)
    lax.fori_loop(2, steps, both_step, 0)
    row = tgt_sum[...]
    tile = jnp.concatenate([row[:, j * PIECE:(j + 1) * PIECE] for j in range(CHIPS)] + [jnp.zeros((8 - CHIPS, PIECE), F32)], axis=0)
    tt_send[...] = tile
    pltpu.make_async_copy(tt_send, tt_recv.at[me], tt_sem.at[1]).start()
    for i in range(1, 2 * CHIPS):
        remote(tt_send, tt_recv.at[me], tt_sem.at[0], tt_sem.at[1], (me + i) % (2 * CHIPS)).start()
    lax.fori_loop(steps, steps + 2, bwd_step, 0)
    lax.fori_loop(steps + 2, steps + 4, late_step, 0)
    wait_bytes(tt_recv, tt_sem.at[1])
    loss_out[0] = (jnp.sum(lse_sum[...]) - jnp.sum(tt_recv[...])) * inv_tokens
    lax.fori_loop(steps + 4, steps + 8, tail_step, 0)

    wait_bytes(dh_out, out_sem)
    peers = 2 * CHIPS - 1
    wait_bytes(tbuf.at[:peers], t_send)
    wait_bytes(tt_recv.at[:peers], tt_sem.at[0])

    def drain_pieces(q, _):
        for i in range(2):
            wait_bytes(hbuf.at[0, pl.ds(0, PIECE)], h_send.at[i, q])

        @pl.when(2 * q < DIRECT)
        def _():
            wait_bytes(hbuf.at[0, pl.ds(0, PIECE)], h_send.at[2, q])

        @pl.when(2 * q >= DIRECT)
        def _():
            for i in range(2):
                wait_bytes(hbuf.at[0, pl.ds(0, PIECE // 2)], h_send.at[3 + i, q])

        wait_bytes(hbuf.at[0], fw_send.at[q])
        wait_bytes(out_stage.at[2 * q], out_send.at[q])
        return 0

    def drain_stats(s, _):
        wait_bytes(st_recv.at[s, :peers], st_ssem.at[s])
        return 0

    lax.fori_loop(0, steps // 2, drain_pieces, 0)
    lax.fori_loop(0, steps, drain_stats, 0)
    for sl in range(SLOTS):
        wait_bytes(r1_buf.at[sl], s1_sem.at[0, sl])
        wait_bytes(s2_buf.at[sl], s2_sem.at[0, sl])


def solution(mesh):
    groups = mesh.shape["fsdp"]
    tok_spec = P(("dp", "fsdp"), None)

    def local_head(hidden, targets, weight):
        tok_loc, width = hidden.shape
        vocab = weight.shape[0]
        steps = 2 * tok_loc // PIECE
        padded = -(-vocab // CHUNK) * CHUNK
        half = width // 2
        dma, bf16 = pltpu.SemaphoreType.DMA, jnp.bfloat16
        vmem = pl.BlockSpec(memory_space=pltpu.VMEM)
        hbm = pl.BlockSpec(memory_space=pltpu.HBM)
        scratch = [
            pltpu.VMEM((vocab, width), bf16),
            pltpu.VMEM((width, padded), bf16),
            pltpu.VMEM((2, vocab, STEP_TOK), F32),
            pltpu.VMEM((steps, STEP_TOK, width), bf16),
            pltpu.VMEM((groups, tok_loc // PIECE, PIECE), jnp.int32),
            pltpu.VMEM((CHUNK, STEP_TOK), F32), pltpu.VMEM((CHUNK, STEP_TOK), F32),
            pltpu.VMEM((GROUP * CHUNK, STEP_TOK), bf16), pltpu.VMEM((GROUP * CHUNK, STEP_TOK), bf16),
            pltpu.VMEM((2, width, STEP_TOK), F32),
            pltpu.VMEM((2, padded // CHUNK, STEP_TOK), F32),
            pltpu.VMEM((padded // CHUNK, STEP_TOK), F32),
            pltpu.VMEM((1, STEP_TOK), F32),
            pltpu.VMEM((CHIPS, PIECE), F32),
            pltpu.VMEM((steps, 8, PIECE), F32),
            pltpu.VMEM((steps, groups, 8, PIECE), F32),
            pltpu.VMEM((8, PIECE), F32),
            pltpu.VMEM((groups, 8, PIECE), F32),
            pltpu.VMEM((2, half, STEP_TOK), F32),
            pltpu.VMEM((SLOTS, CHIPS, half, PIECE), F32),
            pltpu.VMEM((SLOTS, 2, half, PIECE), F32),
            pltpu.VMEM((SLOTS, half, PIECE), F32),
            pltpu.VMEM((SLOTS, half, PIECE), F32),
            pltpu.VMEM((SLOTS, half, PIECE), F32),
            pltpu.VMEM((steps, PIECE, half), F32),
            dma(()), dma((steps // 2,)), dma((3, steps // 2)), dma((steps // 2,)),
            dma((5, steps // 2)), dma((steps // 2,)),
            dma(()), dma(()),
            dma((steps,)), dma((steps,)),
            dma((2,)), dma((2, 2)), dma((2, SLOTS)), dma((2, SLOTS)),
            dma(()), dma((steps // 2,)),
        ]
        flops = 6 * tok_loc * groups * vocab * width
        return pl.pallas_call(
            head_kernel,
            out_shape=(jax.ShapeDtypeStruct((1,), F32), pltpu.VMEM((tok_loc, width), F32), pltpu.VMEM((vocab, width), F32)),
            in_specs=[hbm, vmem, hbm],
            out_specs=(pl.BlockSpec(memory_space=pltpu.SMEM), vmem, vmem),
            scratch_shapes=scratch,
            compiler_params=pltpu.CompilerParams(collective_id=0, has_side_effects=True, vmem_limit_bytes=56_000_000),
            cost_estimate=pl.CostEstimate(flops=flops, bytes_accessed=20_000_000, transcendentals=tok_loc * groups * vocab),
        )(hidden, targets.reshape(tok_loc // PIECE, PIECE), weight)

    return jax.shard_map(local_head, mesh=mesh, in_specs=(tok_spec, P(("dp", "fsdp")), P("fsdp", None)), out_specs=(P("dp"), tok_spec, tok_spec), check_vma=False)
```

```python
import functools

import jax
import jax.numpy as jnp
from jax import lax
from jax.experimental import pallas as pl
from jax.experimental.pallas import tpu as pltpu
from jax.sharding import PartitionSpec as P

PIECE = 128
CHIPS = 4
STEP_TOK = PIECE * CHIPS
GROUP = 1
TILE = 64
SLOTS = 4
DIRECT = 4
CHUNK = 512
F32 = jnp.float32


def head_kernel(hid, tgt, w_in, loss_out, dh_out, dw_out, w, wt, probs, hbuf, tbuf, zbuf_a, zbuf_b, dz_a, dz_b, dh_acc,
                runmax, factor, tgt_sum, lse_sum, st_send, st_recv, tt_send, tt_recv, pair_buf, s1_buf, r1_buf, s2_buf, r2_buf,
                own_buf, out_stage, w_sem, h_own, h_recv, h_fwd, h_send, fw_send, t_sem, t_send, st_rsem, st_ssem, tt_sem, pair_sem,
                s1_sem, s2_sem, out_sem, out_send):
    tok_loc, width = hid.shape
    vocab = w.shape[0]
    steps = 2 * tok_loc // PIECE
    tokens = tok_loc * 2 * CHIPS
    half = width // 2
    n_chunks = -(-vocab // CHUNK)
    last_rows = vocab - (n_chunks - 1) * CHUNK
    inv_tokens = 1.0 / tokens
    dw_acc = dw_out
    zbufs, dzs = (zbuf_a, zbuf_b), (dz_a, dz_b)

    me = lax.axis_index("fsdp")
    core, chip = me % 2, me // 2
    x, y = chip % 2, chip // 2
    partner = chip * 2 + 1 - core
    chip_x, chip_y, chip_d = y * 2 + (1 - x), (1 - y) * 2 + x, (1 - y) * 2 + (1 - x)
    chip_1 = (1 - core) * chip_x + core * chip_y
    chip_2 = (1 - core) * chip_y + core * chip_x

    def remote(src, dst, send, recv, dev):
        return pltpu.make_async_remote_copy(src_ref=src, dst_ref=dst, send_sem=send, recv_sem=recv, device_id={"fsdp": dev},
                                            device_id_type=pl.DeviceIdType.MESH)

    def wait_bytes(ref, sem):
        pltpu.make_async_copy(ref, ref, sem).wait()

    def chunk_rows(c):
        return CHUNK if c < n_chunks - 1 else last_rows

    def piece(s, of_chip, lo=0, n=PIECE):
        return hbuf.at[s, pl.ds(pl.multiple_of(of_chip * PIECE + lo, n), n)]

    def h_sends(q, direct):
        s = 2 * q + core
        peers = (chip_x, chip_y, chip_d)[:3 if direct else 2]
        return [remote(piece(s, chip), piece(s, chip), h_send.at[i, q], h_recv.at[i, q], peer * 2 + core) for i, peer in enumerate(peers)]

    def h_relays(s):
        q = s // 2
        return [remote(piece(s, src, lo, PIECE // 2), piece(s, src, lo, PIECE // 2), h_send.at[3 + i, q], h_recv.at[2, q], dst * 2 + core)
                for i, (src, dst, lo) in enumerate(((chip_x, chip_y, 0), (chip_y, chip_x, PIECE // 2)))]

    def h_forward(s):
        return remote(hbuf.at[s], hbuf.at[s], fw_send.at[s // 2], h_fwd.at[s // 2], partner)

    def stats_sends(s):
        return [remote(st_send.at[s], st_recv.at[s, me], st_ssem.at[s], st_rsem.at[s], (me + i) % (2 * CHIPS)) for i in range(1, 2 * CHIPS)]

    def pair_copy(s):
        rows = pl.ds(pl.multiple_of((1 - core) * half, half), half)
        return remote(dh_acc.at[s % 2, rows], pair_buf.at[s % 2], pair_sem.at[0, s % 2], pair_sem.at[1, s % 2], partner)

    def s1_copies(s):
        sl = s % SLOTS
        return [remote(s1_buf.at[sl, block], r1_buf.at[sl, i], s1_sem.at[0, sl], s1_sem.at[1, sl], chip_1 * 2 + core)
                for i, block in enumerate((chip_1, chip_d))]

    def s2_copy(s):
        return remote(s2_buf.at[s % SLOTS], r2_buf.at[s % SLOTS], s2_sem.at[0, s % SLOTS], s2_sem.at[1, s % SLOTS], chip_2 * 2 + core)

    def out_dst(s):
        return dh_out.at[pl.ds(pl.multiple_of(s // 2 * PIECE, PIECE), PIECE), pl.ds(pl.multiple_of(core * half, half), half)]

    def out_remote(s):
        return remote(out_stage.at[s], out_dst(s), out_send.at[s // 2], out_sem, partner)

    def reduce_stages(u):
        @pl.when((u >= 8) & (u < steps + 8))
        def _():
            s = u - 8
            sl = s % SLOTS
            wait_bytes(r2_buf.at[sl], s2_sem.at[1, sl])
            out_stage[s] = (own_buf[sl] + r2_buf[sl]).T

            @pl.when(s % 2 == core)
            def _():
                pltpu.make_async_copy(out_stage.at[s], out_dst(s), out_sem).start()

            @pl.when(s % 2 != core)
            def _():
                out_remote(s).start()

        @pl.when((u >= 6) & (u < steps + 6))
        def _():
            s = u - 6
            sl = s % SLOTS
            wait_bytes(r1_buf.at[sl], s1_sem.at[1, sl])

            @pl.when(s >= SLOTS)
            def _():
                wait_bytes(s2_buf.at[sl], s2_sem.at[0, sl])

            s2_buf[sl] = s1_buf[sl, chip_2] + r1_buf[sl, 1]
            own_buf[sl] = s1_buf[sl, chip] + r1_buf[sl, 0]
            s2_copy(s).start()

        @pl.when((u >= 4) & (u < steps + 4))
        def _():
            s = u - 4
            sl = s % 2
            sl1 = s % SLOTS
            wait_bytes(pair_buf.at[sl], pair_sem.at[1, sl])
            wait_bytes(pair_buf.at[sl], pair_sem.at[0, sl])

            @pl.when(s >= SLOTS)
            def _():
                wait_bytes(r1_buf.at[sl1], s1_sem.at[0, sl1])

            rows = pl.ds(pl.multiple_of(core * half, half), half)
            for j in range(CHIPS):
                cols = pl.ds(j * PIECE, PIECE)
                s1_buf[sl1, j] = dh_acc[sl, rows, cols] + pair_buf[sl, :, cols]
            for copy in s1_copies(s):
                copy.start()

        @pl.when((u >= 3) & (u < steps + 3))
        def _():
            pair_copy(u - 3).start()

    def first_set(u):
        return jnp.minimum(DIRECT + u + 2 * jnp.clip(u - 2, 0, 2), steps)

    def h_ready(s, lo):
        for i in range(lo, 3):
            wait_bytes(hbuf.at[s, pl.ds(0, PIECE)], h_recv.at[i, s // 2])

    def h_stages(u):
        for i in range(3):
            @pl.when((first_set(u) + i < first_set(u + 1)) & ((first_set(u) + i) % 2 == core))
            def _():
                for copy in h_sends((first_set(u) + i) // 2, False):
                    copy.start()

        @pl.when((u + 2 >= DIRECT) & (u + 2 < steps) & (u % 2 == core))
        def _():
            for i in range(2):
                wait_bytes(hbuf.at[u + 2, pl.ds(0, PIECE)], h_recv.at[i, (u + 2) // 2])
            for copy in h_relays(u + 2):
                copy.start()

        @pl.when((u + 1 < DIRECT) & ((u + 1) % 2 == core))
        def _():
            h_ready(u + 1, 0)
            h_forward(u + 1).start()

        @pl.when((u + 1 >= DIRECT) & (u + 1 < steps) & ((u + 1) % 2 == core))
        def _():
            h_ready(u + 1, 2)
            h_forward(u + 1).start()

        @pl.when((u < steps) & (u % 2 != core))
        def _():
            wait_bytes(hbuf.at[u], h_fwd.at[u // 2])

    def row_ids(lo, n):
        return jnp.concatenate([lax.broadcasted_iota(jnp.int32, (n, PIECE), 0) + lo] * CHIPS, axis=1)

    def target_row(s):
        row = jnp.concatenate([tbuf[2 * j + s % 2, pl.ds(s // 2, 1), :] for j in range(CHIPS)], axis=1)
        return row - me * vocab

    def finish_stats(s):
        wait_bytes(st_recv.at[s], st_rsem.at[s])
        stats = st_recv[s]
        m, e = stats[:, :CHIPS], stats[:, CHIPS:]
        top = jnp.max(m, axis=0)
        lse = top + jnp.log(jnp.sum(e * jnp.exp(m - top[None]), axis=0))
        lse_sum[...] += lse
        lse_row = jnp.concatenate([lse[j:j + 1] for j in range(CHIPS)], axis=1)
        factor[...] = jnp.exp(runmax[s % 2] - lse_row) * inv_tokens

    def chunks(u, fwd, bwd, late_dw=False):
        par = u % 2
        if fwd:
            h_f = hbuf.at[u]
            t_f = target_row(u)
        if bwd:
            s = u - 2
            h_b = hbuf.at[s]
            t_b = target_row(s)
        run_m = run_s = new_m = m = None
        tacc = jnp.zeros((8, STEP_TOK), F32)
        for c in range(n_chunks + 1):
            m = new_m
            if c < n_chunks and bwd:
                lo, n = c * CHUNK, chunk_rows(c)
                dz_ref, at = dzs[c // GROUP % 2], c % GROUP * CHUNK
                for r in range(0, n, TILE):
                    k = min(TILE, n - r)
                    hot = jnp.where(row_ids(lo + r, k) == t_b, inv_tokens, 0.0)
                    dz = probs[par, lo + r:lo + r + k] * factor[c:c + 1] - hot
                    dz_ref[at + r:at + r + k] = dz.astype(jnp.bfloat16)
                    if late_dw:
                        probs[par, lo + r:lo + r + k] = dz
                if n < CHUNK:
                    dz_ref[at + n:at + CHUNK] = jnp.zeros((CHUNK - n, STEP_TOK), jnp.bfloat16)
            if c < n_chunks and fwd:
                lo, n = c * CHUNK, chunk_rows(c)
                z = lax.dot_general(w[lo:lo + n], h_f[...], (((1,), (1,)), ((), ())), preferred_element_type=F32)
                zbufs[c % 2][:n] = z
                new_m = jnp.max(z, axis=0, keepdims=True)
                if c > 0:
                    new_m = jnp.maximum(new_m, m)
                runmax[par, c:c + 1] = new_m
            if c > 0 and bwd and (c % GROUP == 0 or c == n_chunks):
                g = (c - 1) // GROUP
                lo = g * GROUP * CHUNK
                n = min(GROUP * CHUNK, vocab - lo)
                k = -(-n // CHUNK) * CHUNK
                dz_ref = dzs[g % 2]
                part = jnp.dot(wt[:, lo:lo + k], dz_ref[:k], preferred_element_type=F32)
                if g == 0:
                    dh_acc[par] = part
                else:
                    dh_acc[par] += part
                if not late_dw:
                    dw_acc[lo:lo + n] += jnp.dot(dz_ref[:n], h_b[...], preferred_element_type=F32)
            if c > 0 and fwd:
                p = c - 1
                lo, n = p * CHUNK, chunk_rows(p)
                part = None
                for r in range(0, n, TILE):
                    k = min(TILE, n - r)
                    z = zbufs[p % 2][r:r + k]
                    e = jnp.exp(z - m)
                    probs[par, lo + r:lo + r + k] = e
                    e = jnp.sum(e.reshape(k // 8, 8, STEP_TOK), axis=0)
                    part = e if part is None else part + e
                    for i in range(0, k, 8):
                        tacc = jnp.where(row_ids(lo + r + i, 8) == t_f, z[i:i + 8], tacc)
                if p > 0:
                    part = run_s * jnp.exp(run_m - m) + part
                run_m, run_s = m, part
        if fwd:
            run_s = jnp.sum(run_s, axis=0, keepdims=True)
            tacc = jnp.sum(tacc, axis=0, keepdims=True)
        if fwd:
            for j in range(CHIPS):
                cols = slice(j * PIECE, (j + 1) * PIECE)
                st_send[u, j:j + 1] = run_m[:, cols]
                st_send[u, CHIPS + j:CHIPS + j + 1] = run_s[:, cols]
            tgt_sum[...] += tacc
            pltpu.make_async_copy(st_send.at[u], st_recv.at[u, me], st_rsem.at[u]).start()
            for copy in stats_sends(u):
                copy.start()

    def late_chunks(s):
        for c in range(n_chunks):
            lo, n = c * CHUNK, chunk_rows(c)
            dw_acc[lo:lo + n] += jnp.dot(probs[s % 2, lo:lo + n].astype(jnp.bfloat16), hbuf[s], preferred_element_type=F32)

    def prepare(u):
        reduce_stages(u)
        h_stages(u)

    def own_piece(q):
        return pltpu.make_async_copy(hid.at[pl.ds(pl.multiple_of(q * PIECE, PIECE), PIECE)], piece(2 * q + core, chip), h_own.at[q])

    def start_piece(q, _):
        own_piece(q).start()
        return 0

    def wait_piece(q, _):
        own_piece(q).wait()
        return 0

    lax.fori_loop(0, steps // 2, start_piece, 0)
    w_copy = pltpu.make_async_copy(w_in, w, w_sem)
    w_copy.start()
    barrier = pltpu.get_barrier_semaphore()
    for i in range(1, 2 * CHIPS):
        pl.semaphore_signal(barrier, inc=1, device_id={"fsdp": (me + i) % (2 * CHIPS)}, device_id_type=pl.DeviceIdType.MESH)
    lax.fori_loop(0, steps // 2, wait_piece, 0)
    pl.semaphore_wait(barrier, 2 * CHIPS - 1)
    for copy in h_sends(0, True):
        copy.start()
    pltpu.make_async_copy(tgt, tbuf.at[me], t_sem).start()
    t_copies = [remote(tgt, tbuf.at[me], t_send, t_sem, (me + i) % (2 * CHIPS)) for i in range(1, 2 * CHIPS)]
    for copy in t_copies:
        copy.start()
    for copy in h_sends(1, True):
        copy.start()

    dw_acc[...] = jnp.zeros_like(dw_acc)
    tgt_sum[...] = jnp.zeros_like(tgt_sum)
    lse_sum[...] = jnp.zeros_like(lse_sum)
    w_copy.wait()
    for c in range(n_chunks):
        n = chunk_rows(c)
        wt[:, c * CHUNK:c * CHUNK + n] = w[c * CHUNK:c * CHUNK + n].T
    if last_rows < CHUNK:
        wt[:, vocab:] = jnp.zeros((width, n_chunks * CHUNK - vocab), jnp.bfloat16)

    @pl.when(core == 0)
    def _():
        h_ready(0, 0)
        h_forward(0).start()

    wait_bytes(tbuf, t_sem)

    def fwd_step(u, _):
        prepare(u)
        chunks(u, True, False)
        return 0

    def both_step(u, _):
        prepare(u)
        finish_stats(u - 2)
        chunks(u, True, True)
        return 0

    def bwd_step(u, _):
        prepare(u)
        finish_stats(u - 2)
        chunks(u, False, True, late_dw=True)
        return 0

    def late_step(u, _):
        reduce_stages(u)
        late_chunks(u - 4)
        return 0

    def tail_step(u, _):
        reduce_stages(u)
        return 0

    lax.fori_loop(0, 2, fwd_step, 0)
    lax.fori_loop(2, steps, both_step, 0)
    row = tgt_sum[...]
    tile = jnp.concatenate([row[:, j * PIECE:(j + 1) * PIECE] for j in range(CHIPS)] + [jnp.zeros((8 - CHIPS, PIECE), F32)], axis=0)
    tt_send[...] = tile
    pltpu.make_async_copy(tt_send, tt_recv.at[me], tt_sem.at[1]).start()
    for i in range(1, 2 * CHIPS):
        remote(tt_send, tt_recv.at[me], tt_sem.at[0], tt_sem.at[1], (me + i) % (2 * CHIPS)).start()
    lax.fori_loop(steps, steps + 2, bwd_step, 0)
    lax.fori_loop(steps + 2, steps + 4, late_step, 0)
    wait_bytes(tt_recv, tt_sem.at[1])
    loss_out[0] = (jnp.sum(lse_sum[...]) - jnp.sum(tt_recv[...])) * inv_tokens
    lax.fori_loop(steps + 4, steps + 8, tail_step, 0)

    wait_bytes(dh_out, out_sem)
    peers = 2 * CHIPS - 1
    wait_bytes(tbuf.at[:peers], t_send)
    wait_bytes(tt_recv.at[:peers], tt_sem.at[0])

    def drain_pieces(q, _):
        for i in range(2):
            wait_bytes(hbuf.at[0, pl.ds(0, PIECE)], h_send.at[i, q])

        @pl.when(2 * q < DIRECT)
        def _():
            wait_bytes(hbuf.at[0, pl.ds(0, PIECE)], h_send.at[2, q])

        @pl.when(2 * q >= DIRECT)
        def _():
            for i in range(2):
                wait_bytes(hbuf.at[0, pl.ds(0, PIECE // 2)], h_send.at[3 + i, q])

        wait_bytes(hbuf.at[0], fw_send.at[q])
        wait_bytes(out_stage.at[2 * q], out_send.at[q])
        return 0

    def drain_stats(s, _):
        wait_bytes(st_recv.at[s, :peers], st_ssem.at[s])
        return 0

    lax.fori_loop(0, steps // 2, drain_pieces, 0)
    lax.fori_loop(0, steps, drain_stats, 0)
    for sl in range(SLOTS):
        wait_bytes(r1_buf.at[sl], s1_sem.at[0, sl])
        wait_bytes(s2_buf.at[sl], s2_sem.at[0, sl])


def solution(mesh):
    groups = mesh.shape["fsdp"]
    tok_spec = P(("dp", "fsdp"), None)

    def local_head(hidden, targets, weight):
        tok_loc, width = hidden.shape
        vocab = weight.shape[0]
        steps = 2 * tok_loc // PIECE
        padded = -(-vocab // CHUNK) * CHUNK
        half = width // 2
        dma, bf16 = pltpu.SemaphoreType.DMA, jnp.bfloat16
        vmem = pl.BlockSpec(memory_space=pltpu.VMEM)
        hbm = pl.BlockSpec(memory_space=pltpu.HBM)
        scratch = [
            pltpu.VMEM((vocab, width), bf16),
            pltpu.VMEM((width, padded), bf16),
            pltpu.VMEM((2, vocab, STEP_TOK), F32),
            pltpu.VMEM((steps, STEP_TOK, width), bf16),
            pltpu.VMEM((groups, tok_loc // PIECE, PIECE), jnp.int32),
            pltpu.VMEM((CHUNK, STEP_TOK), F32), pltpu.VMEM((CHUNK, STEP_TOK), F32),
            pltpu.VMEM((GROUP * CHUNK, STEP_TOK), bf16), pltpu.VMEM((GROUP * CHUNK, STEP_TOK), bf16),
            pltpu.VMEM((2, width, STEP_TOK), F32),
            pltpu.VMEM((2, padded // CHUNK, STEP_TOK), F32),
            pltpu.VMEM((padded // CHUNK, STEP_TOK), F32),
            pltpu.VMEM((1, STEP_TOK), F32),
            pltpu.VMEM((CHIPS, PIECE), F32),
            pltpu.VMEM((steps, 8, PIECE), F32),
            pltpu.VMEM((steps, groups, 8, PIECE), F32),
            pltpu.VMEM((8, PIECE), F32),
            pltpu.VMEM((groups, 8, PIECE), F32),
            pltpu.VMEM((2, half, STEP_TOK), F32),
            pltpu.VMEM((SLOTS, CHIPS, half, PIECE), F32),
            pltpu.VMEM((SLOTS, 2, half, PIECE), F32),
            pltpu.VMEM((SLOTS, half, PIECE), F32),
            pltpu.VMEM((SLOTS, half, PIECE), F32),
            pltpu.VMEM((SLOTS, half, PIECE), F32),
            pltpu.VMEM((steps, PIECE, half), F32),
            dma(()), dma((steps // 2,)), dma((3, steps // 2)), dma((steps // 2,)),
            dma((5, steps // 2)), dma((steps // 2,)),
            dma(()), dma(()),
            dma((steps,)), dma((steps,)),
            dma((2,)), dma((2, 2)), dma((2, SLOTS)), dma((2, SLOTS)),
            dma(()), dma((steps // 2,)),
        ]
        flops = 6 * tok_loc * groups * vocab * width
        return pl.pallas_call(
            head_kernel,
            out_shape=(jax.ShapeDtypeStruct((1,), F32), pltpu.VMEM((tok_loc, width), F32), pltpu.VMEM((vocab, width), F32)),
            in_specs=[hbm, vmem, hbm],
            out_specs=(pl.BlockSpec(memory_space=pltpu.SMEM), vmem, vmem),
            scratch_shapes=scratch,
            compiler_params=pltpu.CompilerParams(collective_id=0, has_side_effects=True, vmem_limit_bytes=56_000_000),
            cost_estimate=pl.CostEstimate(flops=flops, bytes_accessed=20_000_000, transcendentals=tok_loc * groups * vocab),
        )(hidden, targets.reshape(tok_loc // PIECE, PIECE), weight)

    return jax.shard_map(local_head, mesh=mesh, in_specs=(tok_spec, P(("dp", "fsdp")), P("fsdp", None)), out_specs=(P("dp"), tok_spec, tok_spec), check_vma=False)
```

```python
import functools

import jax
import jax.numpy as jnp
from jax import lax
from jax.experimental import pallas as pl
from jax.experimental.pallas import tpu as pltpu
from jax.sharding import PartitionSpec as P

PIECE = 128
CHIPS = 4
STEP_TOK = PIECE * CHIPS
GROUP = 1
TILE = 64
SLOTS = 4
DIRECT = 4
CHUNK = 512
F32 = jnp.float32


def head_kernel(hid, tgt, w_in, loss_out, dh_out, dw_out, w, wt, probs, hbuf, tbuf, zbuf_a, zbuf_b, dz_a, dz_b, dh_acc,
                runmax, factor, tgt_sum, lse_sum, st_send, st_recv, tt_send, tt_recv, pair_buf, s1_buf, r1_buf, s2_buf, r2_buf,
                own_buf, out_stage, w_sem, h_own, h_recv, h_fwd, h_send, fw_send, t_sem, t_send, st_rsem, st_ssem, tt_sem, pair_sem,
                s1_sem, s2_sem, out_sem, out_send):
    tok_loc, width = hid.shape
    vocab = w.shape[0]
    steps = 2 * tok_loc // PIECE
    tokens = tok_loc * 2 * CHIPS
    half = width // 2
    n_chunks = -(-vocab // CHUNK)
    last_rows = vocab - (n_chunks - 1) * CHUNK
    inv_tokens = 1.0 / tokens
    dw_acc = dw_out
    zbufs, dzs = (zbuf_a, zbuf_b), (dz_a, dz_b)

    me = lax.axis_index("fsdp")
    core, chip = me % 2, me // 2
    x, y = chip % 2, chip // 2
    partner = chip * 2 + 1 - core
    chip_x, chip_y, chip_d = y * 2 + (1 - x), (1 - y) * 2 + x, (1 - y) * 2 + (1 - x)
    chip_1 = (1 - core) * chip_x + core * chip_y
    chip_2 = (1 - core) * chip_y + core * chip_x

    def remote(src, dst, send, recv, dev):
        return pltpu.make_async_remote_copy(src_ref=src, dst_ref=dst, send_sem=send, recv_sem=recv, device_id={"fsdp": dev},
                                            device_id_type=pl.DeviceIdType.MESH)

    def wait_bytes(ref, sem):
        pltpu.make_async_copy(ref, ref, sem).wait()

    def chunk_rows(c):
        return CHUNK if c < n_chunks - 1 else last_rows

    def piece(s, of_chip, lo=0, n=PIECE):
        return hbuf.at[s, pl.ds(pl.multiple_of(of_chip * PIECE + lo, n), n)]

    def h_sends(q, direct):
        s = 2 * q + core
        peers = (chip_x, chip_y, chip_d)[:3 if direct else 2]
        return [remote(piece(s, chip), piece(s, chip), h_send.at[i, q], h_recv.at[i, q], peer * 2 + core) for i, peer in enumerate(peers)]

    def h_relays(s):
        q = s // 2
        return [remote(piece(s, src, lo, PIECE // 2), piece(s, src, lo, PIECE // 2), h_send.at[3 + i, q], h_recv.at[2, q], dst * 2 + core)
                for i, (src, dst, lo) in enumerate(((chip_x, chip_y, 0), (chip_y, chip_x, PIECE // 2)))]

    def h_forward(s):
        return remote(hbuf.at[s], hbuf.at[s], fw_send.at[s // 2], h_fwd.at[s // 2], partner)

    def stats_sends(s):
        return [remote(st_send.at[s], st_recv.at[s, me], st_ssem.at[s], st_rsem.at[s], (me + i) % (2 * CHIPS)) for i in range(1, 2 * CHIPS)]

    def pair_copy(s):
        rows = pl.ds(pl.multiple_of((1 - core) * half, half), half)
        return remote(dh_acc.at[s % 2, rows], pair_buf.at[s % 2], pair_sem.at[0, s % 2], pair_sem.at[1, s % 2], partner)

    def s1_copies(s):
        sl = s % SLOTS
        return [remote(s1_buf.at[sl, block], r1_buf.at[sl, i], s1_sem.at[0, sl], s1_sem.at[1, sl], chip_1 * 2 + core)
                for i, block in enumerate((chip_1, chip_d))]

    def s2_copy(s):
        return remote(s2_buf.at[s % SLOTS], r2_buf.at[s % SLOTS], s2_sem.at[0, s % SLOTS], s2_sem.at[1, s % SLOTS], chip_2 * 2 + core)

    def out_dst(s):
        return dh_out.at[pl.ds(pl.multiple_of(s // 2 * PIECE, PIECE), PIECE), pl.ds(pl.multiple_of(core * half, half), half)]

    def out_remote(s):
        return remote(out_stage.at[s], out_dst(s), out_send.at[s // 2], out_sem, partner)

    def finish_block(s):
        sl = s % SLOTS
        wait_bytes(r2_buf.at[sl], s2_sem.at[1, sl])
        out_stage[s] = (own_buf[sl] + r2_buf[sl]).T

        @pl.when(s % 2 == core)
        def _():
            pltpu.make_async_copy(out_stage.at[s], out_dst(s), out_sem).start()

        @pl.when(s % 2 != core)
        def _():
            out_remote(s).start()

    def second_stage(s):
        sl = s % SLOTS
        wait_bytes(r1_buf.at[sl], s1_sem.at[1, sl])

        @pl.when(s >= SLOTS)
        def _():
            wait_bytes(s2_buf.at[sl], s2_sem.at[0, sl])

        s2_buf[sl] = s1_buf[sl, chip_2] + r1_buf[sl, 1]
        own_buf[sl] = s1_buf[sl, chip] + r1_buf[sl, 0]
        s2_copy(s).start()

    def first_stage(s):
        sl, sl1 = s % 2, s % SLOTS
        wait_bytes(pair_buf.at[sl], pair_sem.at[1, sl])
        wait_bytes(pair_buf.at[sl], pair_sem.at[0, sl])

        @pl.when(s >= SLOTS)
        def _():
            wait_bytes(r1_buf.at[sl1], s1_sem.at[0, sl1])

        rows = pl.ds(pl.multiple_of(core * half, half), half)
        for j in range(CHIPS):
            cols = pl.ds(j * PIECE, PIECE)
            s1_buf[sl1, j] = dh_acc[sl, rows, cols] + pair_buf[sl, :, cols]
        for copy in s1_copies(s):
            copy.start()

    def reduce_stages(u):
        pl.when(u >= 8)(lambda: finish_block(u - 8))
        pl.when(u >= 6)(lambda: second_stage(u - 6))
        pl.when(u >= 4)(lambda: first_stage(u - 4))
        pl.when(u >= 3)(lambda: pair_copy(u - 3).start())

    def first_set(u):
        return jnp.minimum(DIRECT + u + 2 * jnp.clip(u - 2, 0, 2), steps)

    def h_ready(s, lo):
        for i in range(lo, 3):
            wait_bytes(hbuf.at[s, pl.ds(0, PIECE)], h_recv.at[i, s // 2])

    def h_stages(u):
        for i in range(3):
            @pl.when((first_set(u) + i < first_set(u + 1)) & ((first_set(u) + i) % 2 == core))
            def _():
                for copy in h_sends((first_set(u) + i) // 2, False):
                    copy.start()

        @pl.when((u + 2 >= DIRECT) & (u + 2 < steps) & (u % 2 == core))
        def _():
            for i in range(2):
                wait_bytes(hbuf.at[u + 2, pl.ds(0, PIECE)], h_recv.at[i, (u + 2) // 2])
            for copy in h_relays(u + 2):
                copy.start()

        @pl.when((u + 1 < DIRECT) & ((u + 1) % 2 == core))
        def _():
            h_ready(u + 1, 0)
            h_forward(u + 1).start()

        @pl.when((u + 1 >= DIRECT) & (u + 1 < steps) & ((u + 1) % 2 == core))
        def _():
            h_ready(u + 1, 2)
            h_forward(u + 1).start()

        @pl.when((u > 0) & (u < steps) & (u % 2 != core))
        def _():
            wait_bytes(hbuf.at[u], h_fwd.at[u // 2])

    def row_ids(lo, n):
        return jnp.concatenate([lax.broadcasted_iota(jnp.int32, (n, PIECE), 0) + lo] * CHIPS, axis=1)

    def target_row(s):
        row = jnp.concatenate([tbuf[2 * j + s % 2, pl.ds(s // 2, 1), :] for j in range(CHIPS)], axis=1)
        return row - me * vocab

    def finish_stats(s):
        wait_bytes(st_recv.at[s], st_rsem.at[s])
        stats = st_recv[s]
        m, e = stats[:, :CHIPS], stats[:, CHIPS:]
        top = jnp.max(m, axis=0)
        lse = top + jnp.log(jnp.sum(e * jnp.exp(m - top[None]), axis=0))
        lse_sum[...] += lse
        lse_row = jnp.concatenate([lse[j:j + 1] for j in range(CHIPS)], axis=1)
        factor[...] = jnp.exp(runmax[s % 2] - lse_row) * inv_tokens

    def chunks(u, fwd, bwd, late_dw=False):
        par = u % 2
        if fwd:
            h_f = hbuf.at[u]
            t_f = target_row(u)
        if bwd:
            s = u - 2
            h_b = hbuf.at[s]
            t_b = target_row(s)
        run_m = run_s = new_m = m = None
        tacc = jnp.zeros((8, STEP_TOK), F32)
        for c in range(n_chunks + 1):
            m = new_m
            if c < n_chunks and bwd:
                lo, n = c * CHUNK, chunk_rows(c)
                dz_ref, at = dzs[c // GROUP % 2], c % GROUP * CHUNK
                for r in range(0, n, TILE):
                    k = min(TILE, n - r)
                    hot = jnp.where(row_ids(lo + r, k) == t_b, inv_tokens, 0.0)
                    dz = probs[par, lo + r:lo + r + k] * factor[c:c + 1] - hot
                    dz_ref[at + r:at + r + k] = dz.astype(jnp.bfloat16)
                    if late_dw:
                        probs[par, lo + r:lo + r + k] = dz
                if n < CHUNK:
                    dz_ref[at + n:at + CHUNK] = jnp.zeros((CHUNK - n, STEP_TOK), jnp.bfloat16)
            if c < n_chunks and fwd:
                lo, n = c * CHUNK, chunk_rows(c)
                z = lax.dot_general(w[lo:lo + n], h_f[...], (((1,), (1,)), ((), ())), preferred_element_type=F32)
                zbufs[c % 2][:n] = z
                new_m = jnp.max(z, axis=0, keepdims=True)
                if c > 0:
                    new_m = jnp.maximum(new_m, m)
                runmax[par, c:c + 1] = new_m
            if c > 0 and bwd and (c % GROUP == 0 or c == n_chunks):
                g = (c - 1) // GROUP
                lo = g * GROUP * CHUNK
                n = min(GROUP * CHUNK, vocab - lo)
                k = -(-n // CHUNK) * CHUNK
                dz_ref = dzs[g % 2]
                part = jnp.dot(wt[:, lo:lo + k], dz_ref[:k], preferred_element_type=F32)
                if g == 0:
                    dh_acc[par] = part
                else:
                    dh_acc[par] += part
                if not late_dw:
                    dw_acc[lo:lo + n] += jnp.dot(dz_ref[:n], h_b[...], preferred_element_type=F32)
            if c > 0 and fwd:
                p = c - 1
                lo, n = p * CHUNK, chunk_rows(p)
                part = None
                for r in range(0, n, TILE):
                    k = min(TILE, n - r)
                    z = zbufs[p % 2][r:r + k]
                    e = jnp.exp(z - m)
                    probs[par, lo + r:lo + r + k] = e
                    e = jnp.sum(e.reshape(k // 8, 8, STEP_TOK), axis=0)
                    part = e if part is None else part + e
                    for i in range(0, k, 8):
                        tacc = jnp.where(row_ids(lo + r + i, 8) == t_f, z[i:i + 8], tacc)
                if p > 0:
                    part = run_s * jnp.exp(run_m - m) + part
                run_m, run_s = m, part
        if fwd:
            run_s = jnp.sum(run_s, axis=0, keepdims=True)
            tacc = jnp.sum(tacc, axis=0, keepdims=True)
        if fwd:
            for j in range(CHIPS):
                cols = slice(j * PIECE, (j + 1) * PIECE)
                st_send[u, j:j + 1] = run_m[:, cols]
                st_send[u, CHIPS + j:CHIPS + j + 1] = run_s[:, cols]
            tgt_sum[...] += tacc
            pltpu.make_async_copy(st_send.at[u], st_recv.at[u, me], st_rsem.at[u]).start()
            for copy in stats_sends(u):
                copy.start()

    def late_chunks(s, which):
        for c in which:
            lo, n = c * CHUNK, chunk_rows(c)
            dw_acc[lo:lo + n] += jnp.dot(probs[s % 2, lo:lo + n].astype(jnp.bfloat16), hbuf[s], preferred_element_type=F32)

    def prepare(u):
        reduce_stages(u)
        h_stages(u)

    def own_piece(q):
        return pltpu.make_async_copy(hid.at[pl.ds(pl.multiple_of(q * PIECE, PIECE), PIECE)], piece(2 * q + core, chip), h_own.at[q])

    def start_piece(q, _):
        own_piece(q).start()
        return 0

    def wait_piece(q, _):
        own_piece(q).wait()
        return 0

    lax.fori_loop(0, steps // 2, start_piece, 0)
    w_copy = pltpu.make_async_copy(w_in, w, w_sem)
    w_copy.start()
    barrier = pltpu.get_barrier_semaphore()
    for i in range(1, 2 * CHIPS):
        pl.semaphore_signal(barrier, inc=1, device_id={"fsdp": (me + i) % (2 * CHIPS)}, device_id_type=pl.DeviceIdType.MESH)
    lax.fori_loop(0, steps // 2, wait_piece, 0)
    pl.semaphore_wait(barrier, 2 * CHIPS - 1)

    def send_set(q, of_core):
        @pl.when(core == of_core)
        def _():
            for copy in h_sends(q, True):
                copy.start()

    send_set(0, 0)
    pltpu.make_async_copy(tgt, tbuf.at[me], t_sem).start()
    t_copies = [remote(tgt, tbuf.at[me], t_send, t_sem, (me + i) % (2 * CHIPS)) for i in range(1, 2 * CHIPS)]
    for copy in t_copies:
        copy.start()

    dw_acc[...] = jnp.zeros_like(dw_acc)
    tgt_sum[...] = jnp.zeros_like(tgt_sum)
    lse_sum[...] = jnp.zeros_like(lse_sum)
    w_copy.wait()
    for c in range(n_chunks):
        n = chunk_rows(c)
        wt[:, c * CHUNK:c * CHUNK + n] = w[c * CHUNK:c * CHUNK + n].T
    if last_rows < CHUNK:
        wt[:, vocab:] = jnp.zeros((width, n_chunks * CHUNK - vocab), jnp.bfloat16)

    send_set(0, 1)

    @pl.when(core == 0)
    def _():
        h_ready(0, 0)
        h_forward(0).start()

    @pl.when(core == 1)
    def _():
        wait_bytes(hbuf.at[0], h_fwd.at[0])

    for copy in h_sends(1, True):
        copy.start()

    wait_bytes(tbuf, t_sem)

    def fwd_step(u, _):
        prepare(u)
        chunks(u, True, False)
        return 0

    def both_step(u, _):
        prepare(u)
        finish_stats(u - 2)
        chunks(u, True, True)
        return 0

    def bwd_step(u, _):
        prepare(u)
        finish_stats(u - 2)
        chunks(u, False, True, late_dw=True)
        return 0

    lax.fori_loop(0, 2, fwd_step, 0)
    lax.fori_loop(2, steps, both_step, 0)
    row = tgt_sum[...]
    tile = jnp.concatenate([row[:, j * PIECE:(j + 1) * PIECE] for j in range(CHIPS)] + [jnp.zeros((8 - CHIPS, PIECE), F32)], axis=0)
    tt_send[...] = tile
    pltpu.make_async_copy(tt_send, tt_recv.at[me], tt_sem.at[1]).start()
    for i in range(1, 2 * CHIPS):
        remote(tt_send, tt_recv.at[me], tt_sem.at[0], tt_sem.at[1], (me + i) % (2 * CHIPS)).start()
    lax.fori_loop(steps, steps + 2, bwd_step, 0)
    mid = n_chunks // 2
    reduce_stages(jnp.int32(steps + 2))
    late_chunks(steps - 2, range(mid))
    finish_block(steps - 5)
    second_stage(steps - 3)
    first_stage(steps - 1)
    late_chunks(steps - 2, range(mid, n_chunks))
    late_chunks(steps - 1, range(mid))
    finish_block(steps - 4)
    second_stage(steps - 2)
    late_chunks(steps - 1, range(mid, n_chunks))
    wait_bytes(tt_recv, tt_sem.at[1])
    loss_out[0] = (jnp.sum(lse_sum[...]) - jnp.sum(tt_recv[...])) * inv_tokens
    finish_block(steps - 3)
    second_stage(steps - 1)
    finish_block(steps - 2)
    finish_block(steps - 1)

    wait_bytes(dh_out, out_sem)
    peers = 2 * CHIPS - 1
    wait_bytes(tbuf.at[:peers], t_send)
    wait_bytes(tt_recv.at[:peers], tt_sem.at[0])

    def drain_pieces(q, _):
        for i in range(2):
            wait_bytes(hbuf.at[0, pl.ds(0, PIECE)], h_send.at[i, q])

        @pl.when(2 * q < DIRECT)
        def _():
            wait_bytes(hbuf.at[0, pl.ds(0, PIECE)], h_send.at[2, q])

        @pl.when(2 * q >= DIRECT)
        def _():
            for i in range(2):
                wait_bytes(hbuf.at[0, pl.ds(0, PIECE // 2)], h_send.at[3 + i, q])

        wait_bytes(hbuf.at[0], fw_send.at[q])
        wait_bytes(out_stage.at[2 * q], out_send.at[q])
        return 0

    def drain_stats(s, _):
        wait_bytes(st_recv.at[s, :peers], st_ssem.at[s])
        return 0

    lax.fori_loop(0, steps // 2, drain_pieces, 0)
    lax.fori_loop(0, steps, drain_stats, 0)
    for sl in range(SLOTS):
        wait_bytes(r1_buf.at[sl], s1_sem.at[0, sl])
        wait_bytes(s2_buf.at[sl], s2_sem.at[0, sl])


def solution(mesh):
    groups = mesh.shape["fsdp"]
    tok_spec = P(("dp", "fsdp"), None)

    def local_head(hidden, targets, weight):
        tok_loc, width = hidden.shape
        vocab = weight.shape[0]
        steps = 2 * tok_loc // PIECE
        padded = -(-vocab // CHUNK) * CHUNK
        half = width // 2
        dma, bf16 = pltpu.SemaphoreType.DMA, jnp.bfloat16
        vmem = pl.BlockSpec(memory_space=pltpu.VMEM)
        hbm = pl.BlockSpec(memory_space=pltpu.HBM)
        scratch = [
            pltpu.VMEM((vocab, width), bf16),
            pltpu.VMEM((width, padded), bf16),
            pltpu.VMEM((2, vocab, STEP_TOK), F32),
            pltpu.VMEM((steps, STEP_TOK, width), bf16),
            pltpu.VMEM((groups, tok_loc // PIECE, PIECE), jnp.int32),
            pltpu.VMEM((CHUNK, STEP_TOK), F32), pltpu.VMEM((CHUNK, STEP_TOK), F32),
            pltpu.VMEM((GROUP * CHUNK, STEP_TOK), bf16), pltpu.VMEM((GROUP * CHUNK, STEP_TOK), bf16),
            pltpu.VMEM((2, width, STEP_TOK), F32),
            pltpu.VMEM((2, padded // CHUNK, STEP_TOK), F32),
            pltpu.VMEM((padded // CHUNK, STEP_TOK), F32),
            pltpu.VMEM((1, STEP_TOK), F32),
            pltpu.VMEM((CHIPS, PIECE), F32),
            pltpu.VMEM((steps, 8, PIECE), F32),
            pltpu.VMEM((steps, groups, 8, PIECE), F32),
            pltpu.VMEM((8, PIECE), F32),
            pltpu.VMEM((groups, 8, PIECE), F32),
            pltpu.VMEM((2, half, STEP_TOK), F32),
            pltpu.VMEM((SLOTS, CHIPS, half, PIECE), F32),
            pltpu.VMEM((SLOTS, 2, half, PIECE), F32),
            pltpu.VMEM((SLOTS, half, PIECE), F32),
            pltpu.VMEM((SLOTS, half, PIECE), F32),
            pltpu.VMEM((SLOTS, half, PIECE), F32),
            pltpu.VMEM((steps, PIECE, half), F32),
            dma(()), dma((steps // 2,)), dma((3, steps // 2)), dma((steps // 2,)),
            dma((5, steps // 2)), dma((steps // 2,)),
            dma(()), dma(()),
            dma((steps,)), dma((steps,)),
            dma((2,)), dma((2, 2)), dma((2, SLOTS)), dma((2, SLOTS)),
            dma(()), dma((steps // 2,)),
        ]
        flops = 6 * tok_loc * groups * vocab * width
        return pl.pallas_call(
            head_kernel,
            out_shape=(jax.ShapeDtypeStruct((1,), F32), pltpu.VMEM((tok_loc, width), F32), pltpu.VMEM((vocab, width), F32)),
            in_specs=[hbm, vmem, hbm],
            out_specs=(pl.BlockSpec(memory_space=pltpu.SMEM), vmem, vmem),
            scratch_shapes=scratch,
            compiler_params=pltpu.CompilerParams(collective_id=0, has_side_effects=True, vmem_limit_bytes=56_000_000),
            cost_estimate=pl.CostEstimate(flops=flops, bytes_accessed=20_000_000, transcendentals=tok_loc * groups * vocab),
        )(hidden, targets.reshape(tok_loc // PIECE, PIECE), weight)

    return jax.shard_map(local_head, mesh=mesh, in_specs=(tok_spec, P(("dp", "fsdp")), P("fsdp", None)), out_specs=(P("dp"), tok_spec, tok_spec), check_vma=False)
```

```python
import functools

import jax
import jax.numpy as jnp
from jax import lax
from jax.experimental import pallas as pl
from jax.experimental.pallas import tpu as pltpu
from jax.sharding import PartitionSpec as P

PIECE = 128
CHIPS = 4
STEP_TOK = PIECE * CHIPS
GROUP = 1
TILE = 64
SLOTS = 4
DIRECT = 4
CHUNK = 512
F32 = jnp.float32


def head_kernel(hid, tgt, w_in, loss_out, dh_out, dw_out, w, wt, probs, hbuf, tbuf, zbuf_a, zbuf_b, dz_a, dz_b, dh_acc,
                runmax, factor, tgt_sum, lse_sum, st_send, st_recv, tt_send, tt_recv, pair_buf, s1_buf, r1_buf, s2_buf, r2_buf,
                own_buf, out_stage, w_sem, h_own, h_recv, h_fwd, h_send, fw_send, t_sem, t_send, st_rsem, st_ssem, tt_sem, pair_sem,
                s1_sem, s2_sem, out_sem, out_send):
    tok_loc, width = hid.shape
    vocab = w.shape[0]
    steps = 2 * tok_loc // PIECE
    tokens = tok_loc * 2 * CHIPS
    half = width // 2
    n_chunks = -(-vocab // CHUNK)
    last_rows = vocab - (n_chunks - 1) * CHUNK
    inv_tokens = 1.0 / tokens
    dw_acc = dw_out
    zbufs, dzs = (zbuf_a, zbuf_b), (dz_a, dz_b)

    me = lax.axis_index("fsdp")
    core, chip = me % 2, me // 2
    x, y = chip % 2, chip // 2
    partner = chip * 2 + 1 - core
    chip_x, chip_y, chip_d = y * 2 + (1 - x), (1 - y) * 2 + x, (1 - y) * 2 + (1 - x)
    chip_1 = (1 - core) * chip_x + core * chip_y
    chip_2 = (1 - core) * chip_y + core * chip_x

    def remote(src, dst, send, recv, dev):
        return pltpu.make_async_remote_copy(src_ref=src, dst_ref=dst, send_sem=send, recv_sem=recv, device_id={"fsdp": dev},
                                            device_id_type=pl.DeviceIdType.MESH)

    def wait_bytes(ref, sem):
        pltpu.make_async_copy(ref, ref, sem).wait()

    def chunk_rows(c):
        return CHUNK if c < n_chunks - 1 else last_rows

    def piece(s, of_chip, lo=0, n=PIECE):
        return hbuf.at[s, pl.ds(pl.multiple_of(of_chip * PIECE + lo, n), n)]

    def h_sends(q, direct):
        s = 2 * q + core
        peers = (chip_x, chip_y, chip_d)[:3 if direct else 2]
        return [remote(piece(s, chip), piece(s, chip), h_send.at[i, q], h_recv.at[i, q], peer * 2 + core) for i, peer in enumerate(peers)]

    def h_relays(s):
        q = s // 2
        return [remote(piece(s, src, lo, PIECE // 2), piece(s, src, lo, PIECE // 2), h_send.at[3 + i, q], h_recv.at[2, q], dst * 2 + core)
                for i, (src, dst, lo) in enumerate(((chip_x, chip_y, 0), (chip_y, chip_x, PIECE // 2)))]

    def h_forward(s):
        return remote(hbuf.at[s], hbuf.at[s], fw_send.at[s // 2], h_fwd.at[s // 2], partner)

    def stats_sends(s):
        return [remote(st_send.at[s], st_recv.at[s, me], st_ssem.at[s], st_rsem.at[s], (me + i) % (2 * CHIPS)) for i in range(1, 2 * CHIPS)]

    def pair_copy(s):
        rows = pl.ds(pl.multiple_of((1 - core) * half, half), half)
        return remote(dh_acc.at[s % 2, rows], pair_buf.at[s % 2], pair_sem.at[0, s % 2], pair_sem.at[1, s % 2], partner)

    def s1_copies(s):
        sl = s % SLOTS
        return [remote(s1_buf.at[sl, block], r1_buf.at[sl, i], s1_sem.at[0, sl], s1_sem.at[1, sl], chip_1 * 2 + core)
                for i, block in enumerate((chip_1, chip_d))]

    def s2_copy(s):
        return remote(s2_buf.at[s % SLOTS], r2_buf.at[s % SLOTS], s2_sem.at[0, s % SLOTS], s2_sem.at[1, s % SLOTS], chip_2 * 2 + core)

    def out_dst(s):
        return dh_out.at[pl.ds(pl.multiple_of(s // 2 * PIECE, PIECE), PIECE), pl.ds(pl.multiple_of(core * half, half), half)]

    def out_remote(s):
        return remote(out_stage.at[s], out_dst(s), out_send.at[s // 2], out_sem, partner)

    def finish_block(s):
        sl = s % SLOTS
        wait_bytes(r2_buf.at[sl], s2_sem.at[1, sl])
        out_stage[s] = (own_buf[sl] + r2_buf[sl]).T

        @pl.when(s % 2 == core)
        def _():
            pltpu.make_async_copy(out_stage.at[s], out_dst(s), out_sem).start()

        @pl.when(s % 2 != core)
        def _():
            out_remote(s).start()

    def second_stage(s):
        sl = s % SLOTS
        wait_bytes(r1_buf.at[sl], s1_sem.at[1, sl])

        @pl.when(s >= SLOTS)
        def _():
            wait_bytes(s2_buf.at[sl], s2_sem.at[0, sl])

        s2_buf[sl] = s1_buf[sl, chip_2] + r1_buf[sl, 1]
        own_buf[sl] = s1_buf[sl, chip] + r1_buf[sl, 0]
        s2_copy(s).start()

    def first_stage(s):
        sl, sl1 = s % 2, s % SLOTS
        wait_bytes(pair_buf.at[sl], pair_sem.at[1, sl])
        wait_bytes(pair_buf.at[sl], pair_sem.at[0, sl])

        @pl.when(s >= SLOTS)
        def _():
            wait_bytes(r1_buf.at[sl1], s1_sem.at[0, sl1])

        rows = pl.ds(pl.multiple_of(core * half, half), half)
        for j in range(CHIPS):
            cols = pl.ds(j * PIECE, PIECE)
            s1_buf[sl1, j] = dh_acc[sl, rows, cols] + pair_buf[sl, :, cols]
        for copy in s1_copies(s):
            copy.start()

    def reduce_stages(u):
        pl.when(u >= 8)(lambda: finish_block(u - 8))
        pl.when(u >= 6)(lambda: second_stage(u - 6))
        pl.when(u >= 4)(lambda: first_stage(u - 4))
        pl.when(u >= 3)(lambda: pair_copy(u - 3).start())

    def first_set(u):
        return jnp.minimum(DIRECT + u + 2 * jnp.clip(u - 2, 0, 2), steps)

    def h_ready(s, lo):
        for i in range(lo, 3):
            wait_bytes(hbuf.at[s, pl.ds(0, PIECE)], h_recv.at[i, s // 2])

    def h_stages(u):
        for i in range(3):
            @pl.when((first_set(u) + i < first_set(u + 1)) & ((first_set(u) + i) % 2 == core))
            def _():
                for copy in h_sends((first_set(u) + i) // 2, False):
                    copy.start()

        @pl.when((u + 2 >= DIRECT) & (u + 2 < steps) & (u % 2 == core))
        def _():
            for i in range(2):
                wait_bytes(hbuf.at[u + 2, pl.ds(0, PIECE)], h_recv.at[i, (u + 2) // 2])
            for copy in h_relays(u + 2):
                copy.start()

        @pl.when((u + 1 < DIRECT) & ((u + 1) % 2 == core))
        def _():
            h_ready(u + 1, 0)
            h_forward(u + 1).start()

        @pl.when((u + 1 >= DIRECT) & (u + 1 < steps) & ((u + 1) % 2 == core))
        def _():
            h_ready(u + 1, 2)
            h_forward(u + 1).start()

        @pl.when((u > 0) & (u < steps) & (u % 2 != core))
        def _():
            wait_bytes(hbuf.at[u], h_fwd.at[u // 2])

    def row_ids(lo, n):
        return jnp.concatenate([lax.broadcasted_iota(jnp.int32, (n, PIECE), 0) + lo] * CHIPS, axis=1)

    def target_row(s):
        row = jnp.concatenate([tbuf[2 * j + s % 2, pl.ds(s // 2, 1), :] for j in range(CHIPS)], axis=1)
        return row - me * vocab

    def finish_stats(s):
        wait_bytes(st_recv.at[s], st_rsem.at[s])
        stats = st_recv[s]
        m, e = stats[:, :CHIPS], stats[:, CHIPS:]
        top = jnp.max(m, axis=0)
        lse = top + jnp.log(jnp.sum(e * jnp.exp(m - top[None]), axis=0))
        lse_sum[:CHIPS] += lse
        lse_row = jnp.concatenate([lse[j:j + 1] for j in range(CHIPS)], axis=1)
        factor[...] = jnp.exp(runmax[s % 2] - lse_row) * inv_tokens

    def chunks(u, fwd, bwd, late_dw=False):
        par = u % 2
        if fwd:
            h_f = hbuf.at[u]
            t_f = target_row(u)
        if bwd:
            s = u - 2
            h_b = hbuf.at[s]
            t_b = target_row(s)
        run_m = run_s = new_m = m = None
        tacc = jnp.zeros((8, STEP_TOK), F32)
        for c in range(n_chunks + 1):
            m = new_m
            if c < n_chunks and bwd:
                lo, n = c * CHUNK, chunk_rows(c)
                dz_ref, at = dzs[c // GROUP % 2], c % GROUP * CHUNK
                for r in range(0, n, TILE):
                    k = min(TILE, n - r)
                    hot = jnp.where(row_ids(lo + r, k) == t_b, inv_tokens, 0.0)
                    dz = probs[par, lo + r:lo + r + k] * factor[c:c + 1] - hot
                    dz_ref[at + r:at + r + k] = dz.astype(jnp.bfloat16)
                    if late_dw:
                        probs[par, lo + r:lo + r + k] = dz
                if n < CHUNK:
                    dz_ref[at + n:at + CHUNK] = jnp.zeros((CHUNK - n, STEP_TOK), jnp.bfloat16)
            if c < n_chunks and fwd:
                lo, n = c * CHUNK, chunk_rows(c)
                z = lax.dot_general(w[lo:lo + n], h_f[...], (((1,), (1,)), ((), ())), preferred_element_type=F32)
                zbufs[c % 2][:n] = z
                new_m = jnp.max(z, axis=0, keepdims=True)
                if c > 0:
                    new_m = jnp.maximum(new_m, m)
                runmax[par, c:c + 1] = new_m
            if c > 0 and bwd and (c % GROUP == 0 or c == n_chunks):
                g = (c - 1) // GROUP
                lo = g * GROUP * CHUNK
                n = min(GROUP * CHUNK, vocab - lo)
                k = -(-n // CHUNK) * CHUNK
                dz_ref = dzs[g % 2]
                part = jnp.dot(wt[:, lo:lo + k], dz_ref[:k], preferred_element_type=F32)
                if g == 0:
                    dh_acc[par] = part
                else:
                    dh_acc[par] += part
                if not late_dw:
                    dw_acc[lo:lo + n] += jnp.dot(dz_ref[:n], h_b[...], preferred_element_type=F32)
            if c > 0 and fwd:
                p = c - 1
                lo, n = p * CHUNK, chunk_rows(p)
                part = None
                for r in range(0, n, TILE):
                    k = min(TILE, n - r)
                    z = zbufs[p % 2][r:r + k]
                    e = jnp.exp(z - m)
                    probs[par, lo + r:lo + r + k] = e
                    e = jnp.sum(e.reshape(k // 8, 8, STEP_TOK), axis=0)
                    part = e if part is None else part + e
                    for i in range(0, k, 8):
                        tacc = jnp.where(row_ids(lo + r + i, 8) == t_f, z[i:i + 8], tacc)
                if p > 0:
                    part = run_s * jnp.exp(run_m - m) + part
                run_m, run_s = m, part
        if fwd:
            run_s = jnp.sum(run_s, axis=0, keepdims=True)
        if fwd:
            for j in range(CHIPS):
                cols = slice(j * PIECE, (j + 1) * PIECE)
                st_send[u, j:j + 1] = run_m[:, cols]
                st_send[u, CHIPS + j:CHIPS + j + 1] = run_s[:, cols]
            tgt_sum[...] += tacc
            pltpu.make_async_copy(st_send.at[u], st_recv.at[u, me], st_rsem.at[u]).start()
            for copy in stats_sends(u):
                copy.start()

    def late_chunks(s, which):
        for c in which:
            lo, n = c * CHUNK, chunk_rows(c)
            dw_acc[lo:lo + n] += jnp.dot(probs[s % 2, lo:lo + n].astype(jnp.bfloat16), hbuf[s], preferred_element_type=F32)

    def prepare(u):
        reduce_stages(u)
        h_stages(u)

    def own_piece(q):
        return pltpu.make_async_copy(hid.at[pl.ds(pl.multiple_of(q * PIECE, PIECE), PIECE)], piece(2 * q + core, chip), h_own.at[q])

    def start_piece(q, _):
        own_piece(q).start()
        return 0

    def wait_piece(q, _):
        own_piece(q).wait()
        return 0

    lax.fori_loop(0, steps // 2, start_piece, 0)
    w_copy = pltpu.make_async_copy(w_in, w, w_sem)
    w_copy.start()
    barrier = pltpu.get_barrier_semaphore()
    for i in range(1, 2 * CHIPS):
        pl.semaphore_signal(barrier, inc=1, device_id={"fsdp": (me + i) % (2 * CHIPS)}, device_id_type=pl.DeviceIdType.MESH)
    lax.fori_loop(0, steps // 2, wait_piece, 0)
    pl.semaphore_wait(barrier, 2 * CHIPS - 1)

    def send_set(q, of_core):
        @pl.when(core == of_core)
        def _():
            for copy in h_sends(q, True):
                copy.start()

    send_set(0, 0)
    pltpu.make_async_copy(tgt, tbuf.at[me], t_sem).start()
    t_copies = [remote(tgt, tbuf.at[me], t_send, t_sem, (me + i) % (2 * CHIPS)) for i in range(1, 2 * CHIPS)]
    for copy in t_copies:
        copy.start()

    dw_acc[...] = jnp.zeros_like(dw_acc)
    tgt_sum[...] = jnp.zeros_like(tgt_sum)
    lse_sum[...] = jnp.zeros_like(lse_sum)
    w_copy.wait()
    for c in range(n_chunks):
        n = chunk_rows(c)
        wt[:, c * CHUNK:c * CHUNK + n] = w[c * CHUNK:c * CHUNK + n].T
    if last_rows < CHUNK:
        wt[:, vocab:] = jnp.zeros((width, n_chunks * CHUNK - vocab), jnp.bfloat16)

    send_set(0, 1)

    @pl.when(core == 0)
    def _():
        h_ready(0, 0)
        h_forward(0).start()

    @pl.when(core == 1)
    def _():
        wait_bytes(hbuf.at[0], h_fwd.at[0])

    for copy in h_sends(1, True):
        copy.start()

    wait_bytes(tbuf, t_sem)

    def fwd_step(u, _):
        prepare(u)
        chunks(u, True, False)
        return 0

    def both_step(u, _):
        prepare(u)
        finish_stats(u - 2)
        chunks(u, True, True)
        return 0

    def bwd_step(u, _):
        prepare(u)
        finish_stats(u - 2)
        chunks(u, False, True, late_dw=True)
        return 0

    lax.fori_loop(0, 2, fwd_step, 0)
    lax.fori_loop(2, steps, both_step, 0)
    row = jnp.sum(tgt_sum[...], axis=0, keepdims=True)
    tile = jnp.concatenate([row[:, j * PIECE:(j + 1) * PIECE] for j in range(CHIPS)] + [jnp.zeros((8 - CHIPS, PIECE), F32)], axis=0)
    tt_send[:8] = tile
    pltpu.make_async_copy(tt_send.at[:8], tt_recv.at[me], tt_sem.at[1]).start()
    for i in range(1, 2 * CHIPS):
        remote(tt_send.at[:8], tt_recv.at[me], tt_sem.at[0], tt_sem.at[1], (me + i) % (2 * CHIPS)).start()
    lax.fori_loop(steps, steps + 2, bwd_step, 0)
    mid = n_chunks // 2
    reduce_stages(jnp.int32(steps + 2))
    late_chunks(steps - 2, range(mid))
    finish_block(steps - 5)
    second_stage(steps - 3)
    first_stage(steps - 1)
    late_chunks(steps - 2, range(mid, n_chunks))
    late_chunks(steps - 1, range(mid))
    finish_block(steps - 4)
    second_stage(steps - 2)
    late_chunks(steps - 1, range(mid, n_chunks))
    wait_bytes(tt_recv, tt_sem.at[1])
    loss_out[0] = (jnp.sum(lse_sum[...]) - jnp.sum(tt_recv[...])) * inv_tokens
    finish_block(steps - 3)
    second_stage(steps - 1)
    finish_block(steps - 2)
    finish_block(steps - 1)

    wait_bytes(dh_out, out_sem)
    peers = 2 * CHIPS - 1
    wait_bytes(tbuf.at[:peers], t_send)
    wait_bytes(tt_recv.at[:peers], tt_sem.at[0])

    def drain_pieces(q, _):
        for i in range(2):
            wait_bytes(hbuf.at[0, pl.ds(0, PIECE)], h_send.at[i, q])

        @pl.when(2 * q < DIRECT)
        def _():
            wait_bytes(hbuf.at[0, pl.ds(0, PIECE)], h_send.at[2, q])

        @pl.when(2 * q >= DIRECT)
        def _():
            for i in range(2):
                wait_bytes(hbuf.at[0, pl.ds(0, PIECE // 2)], h_send.at[3 + i, q])

        wait_bytes(hbuf.at[0], fw_send.at[q])
        wait_bytes(out_stage.at[2 * q], out_send.at[q])
        return 0

    def drain_stats(s, _):
        wait_bytes(st_recv.at[s, :peers], st_ssem.at[s])
        return 0

    lax.fori_loop(0, steps // 2, drain_pieces, 0)
    lax.fori_loop(0, steps, drain_stats, 0)
    for sl in range(SLOTS):
        wait_bytes(r1_buf.at[sl], s1_sem.at[0, sl])
        wait_bytes(s2_buf.at[sl], s2_sem.at[0, sl])


def solution(mesh):
    groups = mesh.shape["fsdp"]
    tok_spec = P(("dp", "fsdp"), None)

    def local_head(hidden, targets, weight):
        tok_loc, width = hidden.shape
        vocab = weight.shape[0]
        steps = 2 * tok_loc // PIECE
        padded = -(-vocab // CHUNK) * CHUNK
        half = width // 2
        dma, bf16 = pltpu.SemaphoreType.DMA, jnp.bfloat16
        vmem = pl.BlockSpec(memory_space=pltpu.VMEM)
        hbm = pl.BlockSpec(memory_space=pltpu.HBM)
        scratch = [
            pltpu.VMEM((vocab, width), bf16),
            pltpu.VMEM((width, padded), bf16),
            pltpu.VMEM((2, vocab, STEP_TOK), F32),
            pltpu.VMEM((steps, STEP_TOK, width), bf16),
            pltpu.VMEM((groups, tok_loc // PIECE, PIECE), jnp.int32),
            pltpu.VMEM((CHUNK, STEP_TOK), F32), pltpu.VMEM((CHUNK, STEP_TOK), F32),
            pltpu.VMEM((GROUP * CHUNK, STEP_TOK), bf16), pltpu.VMEM((GROUP * CHUNK, STEP_TOK), bf16),
            pltpu.VMEM((2, width, STEP_TOK), F32),
            pltpu.VMEM((2, padded // CHUNK, STEP_TOK), F32),
            pltpu.VMEM((padded // CHUNK, STEP_TOK), F32),
            pltpu.VMEM((8, STEP_TOK), F32),
            pltpu.VMEM((32, PIECE), F32),
            pltpu.VMEM((steps, 8, PIECE), F32),
            pltpu.VMEM((steps, groups, 8, PIECE), F32),
            pltpu.VMEM((32, PIECE), F32),
            pltpu.VMEM((groups, 8, PIECE), F32),
            pltpu.VMEM((2, half, STEP_TOK), F32),
            pltpu.VMEM((SLOTS, CHIPS, half, PIECE), F32),
            pltpu.VMEM((SLOTS, 2, half, PIECE), F32),
            pltpu.VMEM((SLOTS, half, PIECE), F32),
            pltpu.VMEM((SLOTS, half, PIECE), F32),
            pltpu.VMEM((SLOTS, half, PIECE), F32),
            pltpu.VMEM((steps, PIECE, half), F32),
            dma(()), dma((steps // 2,)), dma((3, steps // 2)), dma((steps // 2,)),
            dma((5, steps // 2)), dma((steps // 2,)),
            dma(()), dma(()),
            dma((steps,)), dma((steps,)),
            dma((2,)), dma((2, 2)), dma((2, SLOTS)), dma((2, SLOTS)),
            dma(()), dma((steps // 2,)),
        ]
        flops = 6 * tok_loc * groups * vocab * width
        return pl.pallas_call(
            head_kernel,
            out_shape=(jax.ShapeDtypeStruct((1,), F32), pltpu.VMEM((tok_loc, width), F32), pltpu.VMEM((vocab, width), F32)),
            in_specs=[hbm, hbm, hbm],
            out_specs=(pl.BlockSpec(memory_space=pltpu.SMEM), vmem, vmem),
            scratch_shapes=scratch,
            compiler_params=pltpu.CompilerParams(collective_id=0, has_side_effects=True, vmem_limit_bytes=56_000_000),
            cost_estimate=pl.CostEstimate(flops=flops, bytes_accessed=20_000_000, transcendentals=tok_loc * groups * vocab),
        )(hidden, targets.reshape(tok_loc // PIECE, PIECE), weight)

    return jax.shard_map(local_head, mesh=mesh, in_specs=(tok_spec, P(("dp", "fsdp")), P("fsdp", None)), out_specs=(P("dp"), tok_spec, tok_spec), check_vma=False)
```

```python
import functools

import jax
import jax.numpy as jnp
from jax import lax
from jax.experimental import pallas as pl
from jax.experimental.pallas import tpu as pltpu
from jax.sharding import PartitionSpec as P

PIECE = 128
CHIPS = 4
STEP_TOK = PIECE * CHIPS
GROUP = 1
TILE = 64
SLOTS = 4
DIRECT = 4
CHUNK = 512
F32 = jnp.float32


def head_kernel(hid, tgt, w_in, loss_out, dh_out, dw_out, w, wt, probs, hbuf, tbuf, zbuf_a, zbuf_b, dz_a, dz_b, dh_acc,
                runmax, factor, tgt_sum, lse_sum, st_send, st_recv, tt_send, tt_recv, pair_buf, s1_buf, r1_buf, s2_buf, r2_buf,
                own_buf, out_stage, w_sem, h_own, h_recv, h_fwd, h_send, fw_send, t_sem, t_send, st_rsem, st_ssem, tt_sem, pair_sem,
                s1_sem, s2_sem, out_sem, out_send):
    tok_loc, width = hid.shape
    vocab = w.shape[0]
    steps = 2 * tok_loc // PIECE
    tokens = tok_loc * 2 * CHIPS
    half = width // 2
    n_chunks = -(-vocab // CHUNK)
    last_rows = vocab - (n_chunks - 1) * CHUNK
    inv_tokens = 1.0 / tokens
    dw_acc = dw_out
    zbufs, dzs = (zbuf_a, zbuf_b), (dz_a, dz_b)

    me = lax.axis_index("fsdp")
    core, chip = me % 2, me // 2
    x, y = chip % 2, chip // 2
    partner = chip * 2 + 1 - core
    chip_x, chip_y, chip_d = y * 2 + (1 - x), (1 - y) * 2 + x, (1 - y) * 2 + (1 - x)
    chip_1 = (1 - core) * chip_x + core * chip_y
    chip_2 = (1 - core) * chip_y + core * chip_x

    def remote(src, dst, send, recv, dev):
        return pltpu.make_async_remote_copy(src_ref=src, dst_ref=dst, send_sem=send, recv_sem=recv, device_id={"fsdp": dev},
                                            device_id_type=pl.DeviceIdType.MESH)

    def wait_bytes(ref, sem):
        pltpu.make_async_copy(ref, ref, sem).wait()

    def chunk_rows(c):
        return CHUNK if c < n_chunks - 1 else last_rows

    def piece(s, of_chip, lo=0, n=PIECE):
        return hbuf.at[s, pl.ds(pl.multiple_of(of_chip * PIECE + lo, n), n)]

    def h_sends(q, direct):
        s = 2 * q + core
        peers = (chip_x, chip_y, chip_d)[:3 if direct else 2]
        return [remote(piece(s, chip), piece(s, chip), h_send.at[i, q], h_recv.at[i, q], peer * 2 + core) for i, peer in enumerate(peers)]

    def h_relays(s):
        q = s // 2
        return [remote(piece(s, src, lo, PIECE // 2), piece(s, src, lo, PIECE // 2), h_send.at[3 + i, q], h_recv.at[2, q], dst * 2 + core)
                for i, (src, dst, lo) in enumerate(((chip_x, chip_y, 0), (chip_y, chip_x, PIECE // 2)))]

    def h_forward(s):
        return remote(hbuf.at[s], hbuf.at[s], fw_send.at[s // 2], h_fwd.at[s // 2], partner)

    def stats_sends(s):
        return [remote(st_send.at[s], st_recv.at[s, me], st_ssem.at[s], st_rsem.at[s], (me + i) % (2 * CHIPS)) for i in range(1, 2 * CHIPS)]

    def pair_copy(s):
        rows = pl.ds(pl.multiple_of((1 - core) * half, half), half)
        return remote(dh_acc.at[s % 2, rows], pair_buf.at[s % 2], pair_sem.at[0, s % 2], pair_sem.at[1, s % 2], partner)

    def s1_copies(s):
        sl = s % SLOTS
        return [remote(s1_buf.at[sl, block], r1_buf.at[sl, i], s1_sem.at[0, sl], s1_sem.at[1, sl], chip_1 * 2 + core)
                for i, block in enumerate((chip_1, chip_d))]

    def s2_copy(s):
        return remote(s2_buf.at[s % SLOTS], r2_buf.at[s % SLOTS], s2_sem.at[0, s % SLOTS], s2_sem.at[1, s % SLOTS], chip_2 * 2 + core)

    def out_dst(s):
        return dh_out.at[pl.ds(pl.multiple_of(s // 2 * PIECE, PIECE), PIECE), pl.ds(pl.multiple_of(core * half, half), half)]

    def out_remote(s):
        return remote(out_stage.at[s], out_dst(s), out_send.at[s // 2], out_sem, partner)

    def finish_block(s):
        sl = s % SLOTS
        wait_bytes(r2_buf.at[sl], s2_sem.at[1, sl])
        out_stage[s] = (own_buf[sl] + r2_buf[sl]).T

        @pl.when(s % 2 == core)
        def _():
            pltpu.make_async_copy(out_stage.at[s], out_dst(s), out_sem).start()

        @pl.when(s % 2 != core)
        def _():
            out_remote(s).start()

    def second_stage(s):
        sl = s % SLOTS
        wait_bytes(r1_buf.at[sl], s1_sem.at[1, sl])

        @pl.when(s >= SLOTS)
        def _():
            wait_bytes(s2_buf.at[sl], s2_sem.at[0, sl])

        s2_buf[sl] = s1_buf[sl, chip_2] + r1_buf[sl, 1]
        own_buf[sl] = s1_buf[sl, chip] + r1_buf[sl, 0]
        s2_copy(s).start()

    def first_stage(s):
        sl, sl1 = s % 2, s % SLOTS
        wait_bytes(pair_buf.at[sl], pair_sem.at[1, sl])
        wait_bytes(pair_buf.at[sl], pair_sem.at[0, sl])

        @pl.when(s >= SLOTS)
        def _():
            wait_bytes(r1_buf.at[sl1], s1_sem.at[0, sl1])

        rows = pl.ds(pl.multiple_of(core * half, half), half)
        for j in range(CHIPS):
            cols = pl.ds(j * PIECE, PIECE)
            s1_buf[sl1, j] = dh_acc[sl, rows, cols] + pair_buf[sl, :, cols]
        for copy in s1_copies(s):
            copy.start()

    def reduce_stages(u):
        pl.when(u >= 8)(lambda: finish_block(u - 8))
        pl.when(u >= 6)(lambda: second_stage(u - 6))
        pl.when(u >= 4)(lambda: first_stage(u - 4))
        pl.when(u >= 3)(lambda: pair_copy(u - 3).start())

    def first_set(u):
        return jnp.minimum(DIRECT + u + 2 * jnp.clip(u - 2, 0, 2), steps)

    def h_ready(s, lo):
        for i in range(lo, 3):
            wait_bytes(hbuf.at[s, pl.ds(0, PIECE)], h_recv.at[i, s // 2])

    def h_stages(u):
        for i in range(3):
            @pl.when((first_set(u) + i < first_set(u + 1)) & ((first_set(u) + i) % 2 == core))
            def _():
                for copy in h_sends((first_set(u) + i) // 2, False):
                    copy.start()

        @pl.when((u + 2 >= DIRECT) & (u + 2 < steps) & (u % 2 == core))
        def _():
            for i in range(2):
                wait_bytes(hbuf.at[u + 2, pl.ds(0, PIECE)], h_recv.at[i, (u + 2) // 2])
            for copy in h_relays(u + 2):
                copy.start()

        @pl.when((u + 1 < DIRECT) & ((u + 1) % 2 == core))
        def _():
            h_ready(u + 1, 0)
            h_forward(u + 1).start()

        @pl.when((u + 1 >= DIRECT) & (u + 1 < steps) & ((u + 1) % 2 == core))
        def _():
            h_ready(u + 1, 2)
            h_forward(u + 1).start()

        @pl.when((u < steps) & (u % 2 != core))
        def _():
            wait_bytes(hbuf.at[u], h_fwd.at[u // 2])

    def row_ids(lo, n):
        return jnp.concatenate([lax.broadcasted_iota(jnp.int32, (n, PIECE), 0) + lo] * CHIPS, axis=1)

    def target_row(s):
        row = jnp.concatenate([tbuf[2 * j + s % 2, pl.ds(s // 2, 1), :] for j in range(CHIPS)], axis=1)
        return row - me * vocab

    def finish_stats(s):
        wait_bytes(st_recv.at[s], st_rsem.at[s])
        stats = st_recv[s]
        m, e = stats[:, :CHIPS], stats[:, CHIPS:]
        top = jnp.max(m, axis=0)
        lse = top + jnp.log(jnp.sum(e * jnp.exp(m - top[None]), axis=0))
        lse_sum[:CHIPS] += lse
        lse_row = jnp.concatenate([lse[j:j + 1] for j in range(CHIPS)], axis=1)
        factor[...] = jnp.exp(runmax[s % 2] - lse_row) * inv_tokens

    def chunks(u, fwd, bwd, late_dw=False):
        par = u % 2
        if fwd:
            h_f = hbuf.at[u]
            t_f = target_row(u)
        if bwd:
            s = u - 2
            h_b = hbuf.at[s]
            t_b = target_row(s)
        run_m = run_s = new_m = m = None
        tacc = jnp.zeros((8, STEP_TOK), F32)
        for c in range(n_chunks + 1):
            m = new_m
            if c < n_chunks and bwd:
                lo, n = c * CHUNK, chunk_rows(c)
                dz_ref, at = dzs[c // GROUP % 2], c % GROUP * CHUNK
                for r in range(0, n, TILE):
                    k = min(TILE, n - r)
                    hot = jnp.where(row_ids(lo + r, k) == t_b, inv_tokens, 0.0)
                    dz = probs[par, lo + r:lo + r + k] * factor[c:c + 1] - hot
                    dz_ref[at + r:at + r + k] = dz.astype(jnp.bfloat16)
                    if late_dw:
                        probs[par, lo + r:lo + r + k] = dz
                if n < CHUNK:
                    dz_ref[at + n:at + CHUNK] = jnp.zeros((CHUNK - n, STEP_TOK), jnp.bfloat16)
            if c < n_chunks and fwd:
                lo, n = c * CHUNK, chunk_rows(c)
                z = lax.dot_general(w[lo:lo + n], h_f[...], (((1,), (1,)), ((), ())), preferred_element_type=F32)
                zbufs[c % 2][:n] = z
                new_m = jnp.max(z, axis=0, keepdims=True)
                if c > 0:
                    new_m = jnp.maximum(new_m, m)
                runmax[par, c:c + 1] = new_m
            if c > 0 and bwd and (c % GROUP == 0 or c == n_chunks):
                g = (c - 1) // GROUP
                lo = g * GROUP * CHUNK
                n = min(GROUP * CHUNK, vocab - lo)
                k = -(-n // CHUNK) * CHUNK
                dz_ref = dzs[g % 2]
                part = jnp.dot(wt[:, lo:lo + k], dz_ref[:k], preferred_element_type=F32)
                if g == 0:
                    dh_acc[par] = part
                else:
                    dh_acc[par] += part
                if not late_dw:
                    dw_acc[lo:lo + n] += jnp.dot(dz_ref[:n], h_b[...], preferred_element_type=F32)
            if c > 0 and fwd:
                p = c - 1
                lo, n = p * CHUNK, chunk_rows(p)
                part = None
                for r in range(0, n, TILE):
                    k = min(TILE, n - r)
                    z = zbufs[p % 2][r:r + k]
                    e = jnp.exp(z - m)
                    probs[par, lo + r:lo + r + k] = e
                    e = jnp.sum(e.reshape(k // 8, 8, STEP_TOK), axis=0)
                    part = e if part is None else part + e
                    for i in range(0, k, 8):
                        tacc = jnp.where(row_ids(lo + r + i, 8) == t_f, z[i:i + 8], tacc)
                if p > 0:
                    part = run_s * jnp.exp(run_m - m) + part
                run_m, run_s = m, part
        if fwd:
            run_s = jnp.sum(run_s, axis=0, keepdims=True)
        if fwd:
            for j in range(CHIPS):
                cols = slice(j * PIECE, (j + 1) * PIECE)
                st_send[u, j:j + 1] = run_m[:, cols]
                st_send[u, CHIPS + j:CHIPS + j + 1] = run_s[:, cols]
            tgt_sum[...] += tacc
            pltpu.make_async_copy(st_send.at[u], st_recv.at[u, me], st_rsem.at[u]).start()
            for copy in stats_sends(u):
                copy.start()

    def late_chunks(s, which):
        for c in which:
            lo, n = c * CHUNK, chunk_rows(c)
            dw_acc[lo:lo + n] += jnp.dot(probs[s % 2, lo:lo + n].astype(jnp.bfloat16), hbuf[s], preferred_element_type=F32)

    def prepare(u):
        reduce_stages(u)
        h_stages(u)

    def own_piece(q):
        return pltpu.make_async_copy(hid.at[pl.ds(pl.multiple_of(q * PIECE, PIECE), PIECE)], piece(2 * q + core, chip), h_own.at[q])

    def start_piece(q, _):
        own_piece(q).start()
        return 0

    def wait_piece(q, _):
        own_piece(q).wait()
        return 0

    lax.fori_loop(0, steps // 2, start_piece, 0)
    w_copy = pltpu.make_async_copy(w_in, w, w_sem)
    w_copy.start()
    barrier = pltpu.get_barrier_semaphore()
    for i in range(1, 2 * CHIPS):
        pl.semaphore_signal(barrier, inc=1, device_id={"fsdp": (me + i) % (2 * CHIPS)}, device_id_type=pl.DeviceIdType.MESH)
    lax.fori_loop(0, steps // 2, wait_piece, 0)
    pl.semaphore_wait(barrier, 2 * CHIPS - 1)
    for copy in h_sends(0, True):
        copy.start()
    pltpu.make_async_copy(tgt, tbuf.at[me], t_sem).start()
    t_copies = [remote(tgt, tbuf.at[me], t_send, t_sem, (me + i) % (2 * CHIPS)) for i in range(1, 2 * CHIPS)]
    for copy in t_copies:
        copy.start()
    for copy in h_sends(1, True):
        copy.start()

    dw_acc[...] = jnp.zeros_like(dw_acc)
    tgt_sum[...] = jnp.zeros_like(tgt_sum)
    lse_sum[...] = jnp.zeros_like(lse_sum)
    w_copy.wait()
    for c in range(n_chunks):
        n = chunk_rows(c)
        wt[:, c * CHUNK:c * CHUNK + n] = w[c * CHUNK:c * CHUNK + n].T
    if last_rows < CHUNK:
        wt[:, vocab:] = jnp.zeros((width, n_chunks * CHUNK - vocab), jnp.bfloat16)

    @pl.when(core == 0)
    def _():
        h_ready(0, 0)
        h_forward(0).start()


    wait_bytes(tbuf, t_sem)

    def fwd_step(u, _):
        prepare(u)
        chunks(u, True, False)
        return 0

    def both_step(u, _):
        prepare(u)
        finish_stats(u - 2)
        chunks(u, True, True)
        return 0

    def bwd_step(u, _):
        prepare(u)
        finish_stats(u - 2)
        chunks(u, False, True, late_dw=True)
        return 0

    lax.fori_loop(0, 2, fwd_step, 0)
    lax.fori_loop(2, steps, both_step, 0)
    row = jnp.sum(tgt_sum[...], axis=0, keepdims=True)
    tile = jnp.concatenate([row[:, j * PIECE:(j + 1) * PIECE] for j in range(CHIPS)] + [jnp.zeros((8 - CHIPS, PIECE), F32)], axis=0)
    tt_send[:8] = tile
    pltpu.make_async_copy(tt_send.at[:8], tt_recv.at[me], tt_sem.at[1]).start()
    for i in range(1, 2 * CHIPS):
        remote(tt_send.at[:8], tt_recv.at[me], tt_sem.at[0], tt_sem.at[1], (me + i) % (2 * CHIPS)).start()
    lax.fori_loop(steps, steps + 2, bwd_step, 0)
    mid = n_chunks // 2
    reduce_stages(jnp.int32(steps + 2))
    late_chunks(steps - 2, range(mid))
    finish_block(steps - 5)
    second_stage(steps - 3)
    first_stage(steps - 1)
    late_chunks(steps - 2, range(mid, n_chunks))
    late_chunks(steps - 1, range(mid))
    finish_block(steps - 4)
    second_stage(steps - 2)
    late_chunks(steps - 1, range(mid, n_chunks))
    wait_bytes(tt_recv, tt_sem.at[1])
    loss_out[0] = (jnp.sum(lse_sum[...]) - jnp.sum(tt_recv[...])) * inv_tokens
    finish_block(steps - 3)
    second_stage(steps - 1)
    finish_block(steps - 2)
    finish_block(steps - 1)

    wait_bytes(dh_out, out_sem)
    peers = 2 * CHIPS - 1
    wait_bytes(tbuf.at[:peers], t_send)
    wait_bytes(tt_recv.at[:peers], tt_sem.at[0])

    def drain_pieces(q, _):
        for i in range(2):
            wait_bytes(hbuf.at[0, pl.ds(0, PIECE)], h_send.at[i, q])

        @pl.when(2 * q < DIRECT)
        def _():
            wait_bytes(hbuf.at[0, pl.ds(0, PIECE)], h_send.at[2, q])

        @pl.when(2 * q >= DIRECT)
        def _():
            for i in range(2):
                wait_bytes(hbuf.at[0, pl.ds(0, PIECE // 2)], h_send.at[3 + i, q])

        wait_bytes(hbuf.at[0], fw_send.at[q])
        wait_bytes(out_stage.at[2 * q], out_send.at[q])
        return 0

    def drain_stats(s, _):
        wait_bytes(st_recv.at[s, :peers], st_ssem.at[s])
        return 0

    lax.fori_loop(0, steps // 2, drain_pieces, 0)
    lax.fori_loop(0, steps, drain_stats, 0)
    for sl in range(SLOTS):
        wait_bytes(r1_buf.at[sl], s1_sem.at[0, sl])
        wait_bytes(s2_buf.at[sl], s2_sem.at[0, sl])


def solution(mesh):
    groups = mesh.shape["fsdp"]
    tok_spec = P(("dp", "fsdp"), None)

    def local_head(hidden, targets, weight):
        tok_loc, width = hidden.shape
        vocab = weight.shape[0]
        steps = 2 * tok_loc // PIECE
        padded = -(-vocab // CHUNK) * CHUNK
        half = width // 2
        dma, bf16 = pltpu.SemaphoreType.DMA, jnp.bfloat16
        vmem = pl.BlockSpec(memory_space=pltpu.VMEM)
        hbm = pl.BlockSpec(memory_space=pltpu.HBM)
        scratch = [
            pltpu.VMEM((vocab, width), bf16),
            pltpu.VMEM((width, padded), bf16),
            pltpu.VMEM((2, vocab, STEP_TOK), F32),
            pltpu.VMEM((steps, STEP_TOK, width), bf16),
            pltpu.VMEM((groups, tok_loc // PIECE, PIECE), jnp.int32),
            pltpu.VMEM((CHUNK, STEP_TOK), F32), pltpu.VMEM((CHUNK, STEP_TOK), F32),
            pltpu.VMEM((GROUP * CHUNK, STEP_TOK), bf16), pltpu.VMEM((GROUP * CHUNK, STEP_TOK), bf16),
            pltpu.VMEM((2, width, STEP_TOK), F32),
            pltpu.VMEM((2, padded // CHUNK, STEP_TOK), F32),
            pltpu.VMEM((padded // CHUNK, STEP_TOK), F32),
            pltpu.VMEM((8, STEP_TOK), F32),
            pltpu.VMEM((32, PIECE), F32),
            pltpu.VMEM((steps, 8, PIECE), F32),
            pltpu.VMEM((steps, groups, 8, PIECE), F32),
            pltpu.VMEM((32, PIECE), F32),
            pltpu.VMEM((groups, 8, PIECE), F32),
            pltpu.VMEM((2, half, STEP_TOK), F32),
            pltpu.VMEM((SLOTS, CHIPS, half, PIECE), F32),
            pltpu.VMEM((SLOTS, 2, half, PIECE), F32),
            pltpu.VMEM((SLOTS, half, PIECE), F32),
            pltpu.VMEM((SLOTS, half, PIECE), F32),
            pltpu.VMEM((SLOTS, half, PIECE), F32),
            pltpu.VMEM((steps, PIECE, half), F32),
            dma(()), dma((steps // 2,)), dma((3, steps // 2)), dma((steps // 2,)),
            dma((5, steps // 2)), dma((steps // 2,)),
            dma(()), dma(()),
            dma((steps,)), dma((steps,)),
            dma((2,)), dma((2, 2)), dma((2, SLOTS)), dma((2, SLOTS)),
            dma(()), dma((steps // 2,)),
        ]
        flops = 6 * tok_loc * groups * vocab * width
        return pl.pallas_call(
            head_kernel,
            out_shape=(jax.ShapeDtypeStruct((1,), F32), pltpu.VMEM((tok_loc, width), F32), pltpu.VMEM((vocab, width), F32)),
            in_specs=[hbm, hbm, hbm],
            out_specs=(pl.BlockSpec(memory_space=pltpu.SMEM), vmem, vmem),
            scratch_shapes=scratch,
            compiler_params=pltpu.CompilerParams(collective_id=0, has_side_effects=True, vmem_limit_bytes=56_000_000),
            cost_estimate=pl.CostEstimate(flops=flops, bytes_accessed=20_000_000, transcendentals=tok_loc * groups * vocab),
        )(hidden, targets.reshape(tok_loc // PIECE, PIECE), weight)

    return jax.shard_map(local_head, mesh=mesh, in_specs=(tok_spec, P(("dp", "fsdp")), P("fsdp", None)), out_specs=(P("dp"), tok_spec, tok_spec), check_vma=False)
```

```python
import functools

import jax
import jax.numpy as jnp
from jax import lax
from jax.experimental import pallas as pl
from jax.experimental.pallas import tpu as pltpu
from jax.sharding import PartitionSpec as P

PIECE = 128
CHIPS = 4
STEP_TOK = PIECE * CHIPS
TILE = 64
SLOTS = 4
DIRECT = 4
CHUNK = 512
F32 = jnp.float32


def head_kernel(hid, tgt, w_in, loss_out, dh_out, dw_out, w, wt, probs, hbuf, tbuf, zbuf_a, zbuf_b, dz_a, dz_b, dz_c, dh_acc,
                runmax, factor, tgt_sum, lse_sum, st_send, st_recv, tt_send, tt_recv, pair_buf, s1_buf, r1_buf, s2_buf, r2_buf,
                own_buf, out_stage, w_sem, h_own, h_recv, h_fwd, h_send, fw_send, t_sem, t_send, st_rsem, st_ssem, tt_sem, pair_sem,
                s1_sem, s2_sem, out_sem, out_send):
    tok_loc, width = hid.shape
    vocab = w.shape[0]
    steps = 2 * tok_loc // PIECE
    tokens = tok_loc * 2 * CHIPS
    half = width // 2
    n_chunks = -(-vocab // CHUNK)
    last_rows = vocab - (n_chunks - 1) * CHUNK
    inv_tokens = 1.0 / tokens
    dw_acc = dw_out
    zbufs, dzs = (zbuf_a, zbuf_b), (dz_a, dz_b, dz_c)

    me = lax.axis_index("fsdp")
    core, chip = me % 2, me // 2
    x, y = chip % 2, chip // 2
    partner = chip * 2 + 1 - core
    chip_x, chip_y, chip_d = y * 2 + (1 - x), (1 - y) * 2 + x, (1 - y) * 2 + (1 - x)
    chip_1 = (1 - core) * chip_x + core * chip_y
    chip_2 = (1 - core) * chip_y + core * chip_x

    def remote(src, dst, send, recv, dev):
        return pltpu.make_async_remote_copy(src_ref=src, dst_ref=dst, send_sem=send, recv_sem=recv, device_id={"fsdp": dev},
                                            device_id_type=pl.DeviceIdType.MESH)

    def wait_bytes(ref, sem):
        pltpu.make_async_copy(ref, ref, sem).wait()

    def chunk_rows(c):
        return CHUNK if c < n_chunks - 1 else last_rows

    def piece(s, of_chip, lo=0, n=PIECE):
        return hbuf.at[s, pl.ds(pl.multiple_of(of_chip * PIECE + lo, n), n)]

    def h_sends(q, direct):
        s = 2 * q + core
        peers = (chip_x, chip_y, chip_d)[:3 if direct else 2]
        return [remote(piece(s, chip), piece(s, chip), h_send.at[i, q], h_recv.at[i, q], peer * 2 + core) for i, peer in enumerate(peers)]

    def h_relays(s):
        q = s // 2
        return [remote(piece(s, src, lo, PIECE // 2), piece(s, src, lo, PIECE // 2), h_send.at[3 + i, q], h_recv.at[2, q], dst * 2 + core)
                for i, (src, dst, lo) in enumerate(((chip_x, chip_y, 0), (chip_y, chip_x, PIECE // 2)))]

    def h_forward(s):
        return remote(hbuf.at[s], hbuf.at[s], fw_send.at[s // 2], h_fwd.at[s // 2], partner)

    def stats_sends(s):
        return [remote(st_send.at[s], st_recv.at[s, me], st_ssem.at[s], st_rsem.at[s], (me + i) % (2 * CHIPS)) for i in range(1, 2 * CHIPS)]

    def pair_copy(s):
        rows = pl.ds(pl.multiple_of((1 - core) * half, half), half)
        return remote(dh_acc.at[s % 2, rows], pair_buf.at[s % 2], pair_sem.at[0, s % 2], pair_sem.at[1, s % 2], partner)

    def s1_copies(s):
        sl = s % SLOTS
        return [remote(s1_buf.at[sl, block], r1_buf.at[sl, i], s1_sem.at[0, sl], s1_sem.at[1, sl], chip_1 * 2 + core)
                for i, block in enumerate((chip_1, chip_d))]

    def s2_copy(s):
        return remote(s2_buf.at[s % SLOTS], r2_buf.at[s % SLOTS], s2_sem.at[0, s % SLOTS], s2_sem.at[1, s % SLOTS], chip_2 * 2 + core)

    def out_dst(s):
        return dh_out.at[pl.ds(pl.multiple_of(s // 2 * PIECE, PIECE), PIECE), pl.ds(pl.multiple_of(core * half, half), half)]

    def out_remote(s):
        return remote(out_stage.at[s], out_dst(s), out_send.at[s // 2], out_sem, partner)

    def finish_block(s):
        sl = s % SLOTS
        wait_bytes(r2_buf.at[sl], s2_sem.at[1, sl])
        out_stage[s] = (own_buf[sl] + r2_buf[sl]).T

        @pl.when(s % 2 == core)
        def _():
            pltpu.make_async_copy(out_stage.at[s], out_dst(s), out_sem).start()

        @pl.when(s % 2 != core)
        def _():
            out_remote(s).start()

    def second_stage(s):
        sl = s % SLOTS
        wait_bytes(r1_buf.at[sl], s1_sem.at[1, sl])

        @pl.when(s >= SLOTS)
        def _():
            wait_bytes(s2_buf.at[sl], s2_sem.at[0, sl])

        s2_buf[sl] = s1_buf[sl, chip_2] + r1_buf[sl, 1]
        own_buf[sl] = s1_buf[sl, chip] + r1_buf[sl, 0]
        s2_copy(s).start()

    def first_stage(s):
        sl, sl1 = s % 2, s % SLOTS
        wait_bytes(pair_buf.at[sl], pair_sem.at[1, sl])
        wait_bytes(pair_buf.at[sl], pair_sem.at[0, sl])

        @pl.when(s >= SLOTS)
        def _():
            wait_bytes(r1_buf.at[sl1], s1_sem.at[0, sl1])

        rows = pl.ds(pl.multiple_of(core * half, half), half)
        for j in range(CHIPS):
            cols = pl.ds(j * PIECE, PIECE)
            s1_buf[sl1, j] = dh_acc[sl, rows, cols] + pair_buf[sl, :, cols]
        for copy in s1_copies(s):
            copy.start()

    def reduce_stages(u):
        pl.when(u >= 8)(lambda: finish_block(u - 8))
        pl.when(u >= 6)(lambda: second_stage(u - 6))
        pl.when(u >= 4)(lambda: first_stage(u - 4))
        pl.when(u >= 3)(lambda: pair_copy(u - 3).start())

    def first_set(u):
        return jnp.minimum(DIRECT + u + 2 * jnp.clip(u - 2, 0, 2), steps)

    def h_ready(s, lo):
        for i in range(lo, 3):
            wait_bytes(hbuf.at[s, pl.ds(0, PIECE)], h_recv.at[i, s // 2])

    def h_stages(u):
        for i in range(3):
            @pl.when((first_set(u) + i < first_set(u + 1)) & ((first_set(u) + i) % 2 == core))
            def _():
                for copy in h_sends((first_set(u) + i) // 2, False):
                    copy.start()

        @pl.when((u + 2 >= DIRECT) & (u + 2 < steps) & (u % 2 == core))
        def _():
            for i in range(2):
                wait_bytes(hbuf.at[u + 2, pl.ds(0, PIECE)], h_recv.at[i, (u + 2) // 2])
            for copy in h_relays(u + 2):
                copy.start()

        @pl.when((u + 1 < DIRECT) & ((u + 1) % 2 == core))
        def _():
            h_ready(u + 1, 0)
            h_forward(u + 1).start()

        @pl.when((u + 1 >= DIRECT) & (u + 1 < steps) & ((u + 1) % 2 == core))
        def _():
            h_ready(u + 1, 2)
            h_forward(u + 1).start()

        @pl.when((u < steps) & (u % 2 != core))
        def _():
            wait_bytes(hbuf.at[u], h_fwd.at[u // 2])

    def row_ids(lo, n):
        return jnp.concatenate([lax.broadcasted_iota(jnp.int32, (n, PIECE), 0) + lo] * CHIPS, axis=1)

    def target_row(s):
        row = jnp.concatenate([tbuf[2 * j + s % 2, pl.ds(s // 2, 1), :] for j in range(CHIPS)], axis=1)
        return row - me * vocab

    def finish_stats(s):
        wait_bytes(st_recv.at[s], st_rsem.at[s])
        stats = st_recv[s]
        m, e = stats[:, :CHIPS], stats[:, CHIPS:]
        top = jnp.max(m, axis=0)
        lse = top + jnp.log(jnp.sum(e * jnp.exp(m - top[None]), axis=0))
        lse_sum[:CHIPS] += lse
        lse_row = jnp.concatenate([lse[j:j + 1] for j in range(CHIPS)], axis=1)
        factor[...] = jnp.exp(runmax[s % 2] - lse_row) * inv_tokens

    def chunks(u, fwd, bwd, late_dw=False):
        par = u % 2
        if fwd:
            h_f = hbuf.at[u]
            t_f = target_row(u)
        if bwd:
            s = u - 2
            h_b = hbuf.at[s]
            t_b = target_row(s)
        def dlogits(c):
            lo, n = c * CHUNK, chunk_rows(c)
            dz_ref = dzs[c % len(dzs)]
            for r in range(0, n, TILE):
                k = min(TILE, n - r)
                hot = jnp.where(row_ids(lo + r, k) == t_b, inv_tokens, 0.0)
                dz = probs[par, lo + r:lo + r + k] * factor[c:c + 1] - hot
                dz_ref[r:r + k] = dz.astype(jnp.bfloat16)
                if late_dw:
                    probs[par, lo + r:lo + r + k] = dz
            if n < CHUNK:
                dz_ref[n:] = jnp.zeros((CHUNK - n, STEP_TOK), jnp.bfloat16)

        run_m = run_s = new_m = m = None
        tacc = jnp.zeros((8, STEP_TOK), F32)
        if bwd:
            dlogits(0)
        for c in range(n_chunks + 1):
            m = new_m
            if c < n_chunks and fwd:
                lo, n = c * CHUNK, chunk_rows(c)
                z = lax.dot_general(w[lo:lo + n], h_f[...], (((1,), (1,)), ((), ())), preferred_element_type=F32)
                zbufs[c % 2][:n] = z
                new_m = jnp.max(z, axis=0, keepdims=True)
                if c > 0:
                    new_m = jnp.maximum(new_m, m)
                runmax[par, c:c + 1] = new_m
            if c + 1 < n_chunks and bwd:
                dlogits(c + 1)
            if c < n_chunks and bwd:
                part = jnp.dot(wt[:, c * CHUNK:(c + 1) * CHUNK], dzs[c % len(dzs)][...], preferred_element_type=F32)
                if c == 0:
                    dh_acc[par] = part
                else:
                    dh_acc[par] += part
            if c > 0 and bwd and not late_dw:
                p = c - 1
                lo, n = p * CHUNK, chunk_rows(p)
                dw_acc[lo:lo + n] += jnp.dot(dzs[p % len(dzs)][:n], h_b[...], preferred_element_type=F32)
            if c > 0 and fwd:
                p = c - 1
                lo, n = p * CHUNK, chunk_rows(p)
                part = None
                for r in range(0, n, TILE):
                    k = min(TILE, n - r)
                    z = zbufs[p % 2][r:r + k]
                    e = jnp.exp(z - m)
                    probs[par, lo + r:lo + r + k] = e
                    e = jnp.sum(e.reshape(k // 8, 8, STEP_TOK), axis=0)
                    part = e if part is None else part + e
                    for i in range(0, k, 8):
                        tacc = jnp.where(row_ids(lo + r + i, 8) == t_f, z[i:i + 8], tacc)
                if p > 0:
                    part = run_s * jnp.exp(run_m - m) + part
                run_m, run_s = m, part
        if fwd:
            run_s = jnp.sum(run_s, axis=0, keepdims=True)
        if fwd:
            for j in range(CHIPS):
                cols = slice(j * PIECE, (j + 1) * PIECE)
                st_send[u, j:j + 1] = run_m[:, cols]
                st_send[u, CHIPS + j:CHIPS + j + 1] = run_s[:, cols]
            tgt_sum[...] += tacc
            pltpu.make_async_copy(st_send.at[u], st_recv.at[u, me], st_rsem.at[u]).start()
            for copy in stats_sends(u):
                copy.start()

    def late_chunks(s, which):
        for c in which:
            lo, n = c * CHUNK, chunk_rows(c)
            dw_acc[lo:lo + n] += jnp.dot(probs[s % 2, lo:lo + n].astype(jnp.bfloat16), hbuf[s], preferred_element_type=F32)

    def prepare(u):
        reduce_stages(u)
        h_stages(u)

    def own_piece(q):
        return pltpu.make_async_copy(hid.at[pl.ds(pl.multiple_of(q * PIECE, PIECE), PIECE)], piece(2 * q + core, chip), h_own.at[q])

    def start_piece(q, _):
        own_piece(q).start()
        return 0

    def wait_piece(q, _):
        own_piece(q).wait()
        return 0

    lax.fori_loop(0, steps // 2, start_piece, 0)
    w_copy = pltpu.make_async_copy(w_in, w, w_sem)
    w_copy.start()
    barrier = pltpu.get_barrier_semaphore()
    for i in range(1, 2 * CHIPS):
        pl.semaphore_signal(barrier, inc=1, device_id={"fsdp": (me + i) % (2 * CHIPS)}, device_id_type=pl.DeviceIdType.MESH)
    lax.fori_loop(0, steps // 2, wait_piece, 0)
    pl.semaphore_wait(barrier, 2 * CHIPS - 1)
    for copy in h_sends(0, True):
        copy.start()
    pltpu.make_async_copy(tgt, tbuf.at[me], t_sem).start()
    t_copies = [remote(tgt, tbuf.at[me], t_send, t_sem, (me + i) % (2 * CHIPS)) for i in range(1, 2 * CHIPS)]
    for copy in t_copies:
        copy.start()
    for copy in h_sends(1, True):
        copy.start()

    dw_acc[...] = jnp.zeros_like(dw_acc)
    tgt_sum[...] = jnp.zeros_like(tgt_sum)
    lse_sum[...] = jnp.zeros_like(lse_sum)
    w_copy.wait()
    for c in range(n_chunks):
        n = chunk_rows(c)
        wt[:, c * CHUNK:c * CHUNK + n] = w[c * CHUNK:c * CHUNK + n].T
    if last_rows < CHUNK:
        wt[:, vocab:] = jnp.zeros((width, n_chunks * CHUNK - vocab), jnp.bfloat16)

    @pl.when(core == 0)
    def _():
        h_ready(0, 0)
        h_forward(0).start()


    wait_bytes(tbuf, t_sem)

    def fwd_step(u, _):
        prepare(u)
        chunks(u, True, False)
        return 0

    def both_step(u, _):
        prepare(u)
        finish_stats(u - 2)
        chunks(u, True, True)
        return 0

    def bwd_step(u, _):
        prepare(u)
        finish_stats(u - 2)
        chunks(u, False, True, late_dw=True)
        return 0

    lax.fori_loop(0, 2, fwd_step, 0)
    lax.fori_loop(2, steps, both_step, 0)
    row = jnp.sum(tgt_sum[...], axis=0, keepdims=True)
    tile = jnp.concatenate([row[:, j * PIECE:(j + 1) * PIECE] for j in range(CHIPS)] + [jnp.zeros((8 - CHIPS, PIECE), F32)], axis=0)
    tt_send[:8] = tile
    pltpu.make_async_copy(tt_send.at[:8], tt_recv.at[me], tt_sem.at[1]).start()
    for i in range(1, 2 * CHIPS):
        remote(tt_send.at[:8], tt_recv.at[me], tt_sem.at[0], tt_sem.at[1], (me + i) % (2 * CHIPS)).start()
    lax.fori_loop(steps, steps + 2, bwd_step, 0)
    mid = n_chunks // 2
    reduce_stages(jnp.int32(steps + 2))
    late_chunks(steps - 2, range(mid))
    finish_block(steps - 5)
    second_stage(steps - 3)
    first_stage(steps - 1)
    late_chunks(steps - 2, range(mid, n_chunks))
    late_chunks(steps - 1, range(mid))
    finish_block(steps - 4)
    second_stage(steps - 2)
    late_chunks(steps - 1, range(mid, n_chunks))
    wait_bytes(tt_recv, tt_sem.at[1])
    loss_out[0] = (jnp.sum(lse_sum[...]) - jnp.sum(tt_recv[...])) * inv_tokens
    finish_block(steps - 3)
    second_stage(steps - 1)
    finish_block(steps - 2)
    finish_block(steps - 1)

    wait_bytes(dh_out, out_sem)
    peers = 2 * CHIPS - 1
    wait_bytes(tbuf.at[:peers], t_send)
    wait_bytes(tt_recv.at[:peers], tt_sem.at[0])

    def drain_pieces(q, _):
        for i in range(2):
            wait_bytes(hbuf.at[0, pl.ds(0, PIECE)], h_send.at[i, q])

        @pl.when(2 * q < DIRECT)
        def _():
            wait_bytes(hbuf.at[0, pl.ds(0, PIECE)], h_send.at[2, q])

        @pl.when(2 * q >= DIRECT)
        def _():
            for i in range(2):
                wait_bytes(hbuf.at[0, pl.ds(0, PIECE // 2)], h_send.at[3 + i, q])

        wait_bytes(hbuf.at[0], fw_send.at[q])
        wait_bytes(out_stage.at[2 * q], out_send.at[q])
        return 0

    def drain_stats(s, _):
        wait_bytes(st_recv.at[s, :peers], st_ssem.at[s])
        return 0

    lax.fori_loop(0, steps // 2, drain_pieces, 0)
    lax.fori_loop(0, steps, drain_stats, 0)
    for sl in range(SLOTS):
        wait_bytes(r1_buf.at[sl], s1_sem.at[0, sl])
        wait_bytes(s2_buf.at[sl], s2_sem.at[0, sl])


def solution(mesh):
    groups = mesh.shape["fsdp"]
    tok_spec = P(("dp", "fsdp"), None)

    def local_head(hidden, targets, weight):
        tok_loc, width = hidden.shape
        vocab = weight.shape[0]
        steps = 2 * tok_loc // PIECE
        padded = -(-vocab // CHUNK) * CHUNK
        half = width // 2
        dma, bf16 = pltpu.SemaphoreType.DMA, jnp.bfloat16
        vmem = pl.BlockSpec(memory_space=pltpu.VMEM)
        hbm = pl.BlockSpec(memory_space=pltpu.HBM)
        scratch = [
            pltpu.VMEM((vocab, width), bf16),
            pltpu.VMEM((width, padded), bf16),
            pltpu.VMEM((2, vocab, STEP_TOK), F32),
            pltpu.VMEM((steps, STEP_TOK, width), bf16),
            pltpu.VMEM((groups, tok_loc // PIECE, PIECE), jnp.int32),
            pltpu.VMEM((CHUNK, STEP_TOK), F32), pltpu.VMEM((CHUNK, STEP_TOK), F32),
            pltpu.VMEM((CHUNK, STEP_TOK), bf16), pltpu.VMEM((CHUNK, STEP_TOK), bf16), pltpu.VMEM((CHUNK, STEP_TOK), bf16),
            pltpu.VMEM((2, width, STEP_TOK), F32),
            pltpu.VMEM((2, padded // CHUNK, STEP_TOK), F32),
            pltpu.VMEM((padded // CHUNK, STEP_TOK), F32),
            pltpu.VMEM((8, STEP_TOK), F32),
            pltpu.VMEM((32, PIECE), F32),
            pltpu.VMEM((steps, 8, PIECE), F32),
            pltpu.VMEM((steps, groups, 8, PIECE), F32),
            pltpu.VMEM((32, PIECE), F32),
            pltpu.VMEM((groups, 8, PIECE), F32),
            pltpu.VMEM((2, half, STEP_TOK), F32),
            pltpu.VMEM((SLOTS, CHIPS, half, PIECE), F32),
            pltpu.VMEM((SLOTS, 2, half, PIECE), F32),
            pltpu.VMEM((SLOTS, half, PIECE), F32),
            pltpu.VMEM((SLOTS, half, PIECE), F32),
            pltpu.VMEM((SLOTS, half, PIECE), F32),
            pltpu.VMEM((steps, PIECE, half), F32),
            dma(()), dma((steps // 2,)), dma((3, steps // 2)), dma((steps // 2,)),
            dma((5, steps // 2)), dma((steps // 2,)),
            dma(()), dma(()),
            dma((steps,)), dma((steps,)),
            dma((2,)), dma((2, 2)), dma((2, SLOTS)), dma((2, SLOTS)),
            dma(()), dma((steps // 2,)),
        ]
        flops = 6 * tok_loc * groups * vocab * width
        return pl.pallas_call(
            head_kernel,
            out_shape=(jax.ShapeDtypeStruct((1,), F32), pltpu.VMEM((tok_loc, width), F32), pltpu.VMEM((vocab, width), F32)),
            in_specs=[hbm, hbm, hbm],
            out_specs=(pl.BlockSpec(memory_space=pltpu.SMEM), vmem, vmem),
            scratch_shapes=scratch,
            compiler_params=pltpu.CompilerParams(collective_id=0, has_side_effects=True, vmem_limit_bytes=56_000_000),
            cost_estimate=pl.CostEstimate(flops=flops, bytes_accessed=20_000_000, transcendentals=tok_loc * groups * vocab),
        )(hidden, targets.reshape(tok_loc // PIECE, PIECE), weight)

    return jax.shard_map(local_head, mesh=mesh, in_specs=(tok_spec, P(("dp", "fsdp")), P("fsdp", None)), out_specs=(P("dp"), tok_spec, tok_spec), check_vma=False)
```

```python
import functools

import jax
import jax.numpy as jnp
from jax import lax
from jax.experimental import pallas as pl
from jax.experimental.pallas import tpu as pltpu
from jax.sharding import PartitionSpec as P

PIECE = 128
CHIPS = 4
STEP_TOK = PIECE * CHIPS
TILE = 64
SLOTS = 4
DIRECT = 4
CHUNK = 512
F32 = jnp.float32


def head_kernel(hid, tgt, w_in, loss_out, dh_out, dw_out, w, wt, probs, hbuf, tbuf, zbuf_a, zbuf_b, dz_a, dz_b, dz_c, dh_acc,
                runmax, factor, tgt_sum, lse_sum, st_send, st_recv, tt_send, tt_recv, pair_buf, s1_buf, r1_buf, s2_buf, r2_buf,
                own_buf, out_stage, w_sem, h_own, h_recv, h_fwd, h_send, fw_send, t_sem, t_send, st_rsem, st_ssem, tt_sem, pair_sem,
                s1_sem, s2_sem, out_sem, out_send):
    tok_loc, width = hid.shape
    vocab = w.shape[0]
    steps = 2 * tok_loc // PIECE
    tokens = tok_loc * 2 * CHIPS
    half = width // 2
    n_chunks = -(-vocab // CHUNK)
    last_rows = vocab - (n_chunks - 1) * CHUNK
    inv_tokens = 1.0 / tokens
    dw_acc = dw_out
    zbufs, dzs = (zbuf_a, zbuf_b), (dz_a, dz_b, dz_c)

    me = lax.axis_index("fsdp")
    core, chip = me % 2, me // 2
    x, y = chip % 2, chip // 2
    partner = chip * 2 + 1 - core
    chip_x, chip_y, chip_d = y * 2 + (1 - x), (1 - y) * 2 + x, (1 - y) * 2 + (1 - x)
    chip_1 = (1 - core) * chip_x + core * chip_y
    chip_2 = (1 - core) * chip_y + core * chip_x

    def remote(src, dst, send, recv, dev):
        return pltpu.make_async_remote_copy(src_ref=src, dst_ref=dst, send_sem=send, recv_sem=recv, device_id={"fsdp": dev},
                                            device_id_type=pl.DeviceIdType.MESH)

    def wait_bytes(ref, sem):
        pltpu.make_async_copy(ref, ref, sem).wait()

    def chunk_rows(c):
        return CHUNK if c < n_chunks - 1 else last_rows

    def piece(s, of_chip, lo=0, n=PIECE):
        return hbuf.at[s, pl.ds(pl.multiple_of(of_chip * PIECE + lo, n), n)]

    def h_sends(q, direct):
        s = 2 * q + core
        peers = (chip_x, chip_y, chip_d)[:3 if direct else 2]
        return [remote(piece(s, chip), piece(s, chip), h_send.at[i, q], h_recv.at[i, q], peer * 2 + core) for i, peer in enumerate(peers)]

    def h_relays(s):
        q = s // 2
        return [remote(piece(s, src, lo, PIECE // 2), piece(s, src, lo, PIECE // 2), h_send.at[3 + i, q], h_recv.at[2, q], dst * 2 + core)
                for i, (src, dst, lo) in enumerate(((chip_x, chip_y, 0), (chip_y, chip_x, PIECE // 2)))]

    def h_forward(s):
        return remote(hbuf.at[s], hbuf.at[s], fw_send.at[s // 2], h_fwd.at[s // 2], partner)

    def stats_sends(s):
        return [remote(st_send.at[s], st_recv.at[s, me], st_ssem.at[s], st_rsem.at[s], (me + i) % (2 * CHIPS)) for i in range(1, 2 * CHIPS)]

    def pair_copy(s):
        rows = pl.ds(pl.multiple_of((1 - core) * half, half), half)
        return remote(dh_acc.at[s % 2, rows], pair_buf.at[s % 2], pair_sem.at[0, s % 2], pair_sem.at[1, s % 2], partner)

    def s1_copies(s):
        sl = s % SLOTS
        return [remote(s1_buf.at[sl, block], r1_buf.at[sl, i], s1_sem.at[0, sl], s1_sem.at[1, sl], chip_1 * 2 + core)
                for i, block in enumerate((chip_1, chip_d))]

    def s2_copy(s):
        return remote(s2_buf.at[s % SLOTS], r2_buf.at[s % SLOTS], s2_sem.at[0, s % SLOTS], s2_sem.at[1, s % SLOTS], chip_2 * 2 + core)

    def out_dst(s):
        return dh_out.at[pl.ds(pl.multiple_of(s // 2 * PIECE, PIECE), PIECE), pl.ds(pl.multiple_of(core * half, half), half)]

    def out_remote(s):
        return remote(out_stage.at[s], out_dst(s), out_send.at[s // 2], out_sem, partner)

    def finish_block(s):
        sl = s % SLOTS
        wait_bytes(r2_buf.at[sl], s2_sem.at[1, sl])
        out_stage[s] = (own_buf[sl] + r2_buf[sl]).T

        @pl.when(s % 2 == core)
        def _():
            pltpu.make_async_copy(out_stage.at[s], out_dst(s), out_sem).start()

        @pl.when(s % 2 != core)
        def _():
            out_remote(s).start()

    def second_stage(s):
        sl = s % SLOTS
        wait_bytes(r1_buf.at[sl], s1_sem.at[1, sl])

        @pl.when(s >= SLOTS)
        def _():
            wait_bytes(s2_buf.at[sl], s2_sem.at[0, sl])

        s2_buf[sl] = s1_buf[sl, chip_2] + r1_buf[sl, 1]
        own_buf[sl] = s1_buf[sl, chip] + r1_buf[sl, 0]
        s2_copy(s).start()

    def first_stage(s):
        sl, sl1 = s % 2, s % SLOTS
        wait_bytes(pair_buf.at[sl], pair_sem.at[1, sl])
        wait_bytes(pair_buf.at[sl], pair_sem.at[0, sl])

        @pl.when(s >= SLOTS)
        def _():
            wait_bytes(r1_buf.at[sl1], s1_sem.at[0, sl1])

        rows = pl.ds(pl.multiple_of(core * half, half), half)
        for j in range(CHIPS):
            cols = pl.ds(j * PIECE, PIECE)
            s1_buf[sl1, j] = dh_acc[sl, rows, cols] + pair_buf[sl, :, cols]
        for copy in s1_copies(s):
            copy.start()

    def reduce_stages(u):
        pl.when(u >= 8)(lambda: finish_block(u - 8))
        pl.when(u >= 6)(lambda: second_stage(u - 6))
        pl.when(u >= 4)(lambda: first_stage(u - 4))
        pl.when(u >= 3)(lambda: pair_copy(u - 3).start())

    def first_set(u):
        return jnp.minimum(DIRECT + u + 3 * jnp.clip(u - 2, 0, 2), steps)

    def h_ready(s, lo):
        for i in range(lo, 3):
            wait_bytes(hbuf.at[s, pl.ds(0, PIECE)], h_recv.at[i, s // 2])

    def h_stages(u):
        for i in range(4):
            @pl.when((first_set(u) + i < first_set(u + 1)) & ((first_set(u) + i) % 2 == core))
            def _():
                for copy in h_sends((first_set(u) + i) // 2, False):
                    copy.start()

        @pl.when((u + 2 >= DIRECT) & (u + 2 < steps) & (u % 2 == core))
        def _():
            for i in range(2):
                wait_bytes(hbuf.at[u + 2, pl.ds(0, PIECE)], h_recv.at[i, (u + 2) // 2])
            for copy in h_relays(u + 2):
                copy.start()

        @pl.when((u + 1 < DIRECT) & ((u + 1) % 2 == core))
        def _():
            h_ready(u + 1, 0)
            h_forward(u + 1).start()

        @pl.when((u + 1 >= DIRECT) & (u + 1 < steps) & ((u + 1) % 2 == core))
        def _():
            h_ready(u + 1, 2)
            h_forward(u + 1).start()

        @pl.when((u < steps) & (u % 2 != core))
        def _():
            wait_bytes(hbuf.at[u], h_fwd.at[u // 2])

    def row_ids(lo, n):
        return jnp.concatenate([lax.broadcasted_iota(jnp.int32, (n, PIECE), 0) + lo] * CHIPS, axis=1)

    def target_row(s):
        row = jnp.concatenate([tbuf[2 * j + s % 2, pl.ds(s // 2, 1), :] for j in range(CHIPS)], axis=1)
        return row - me * vocab

    def finish_stats(s):
        wait_bytes(st_recv.at[s], st_rsem.at[s])
        stats = st_recv[s]
        m, e = stats[:, :CHIPS], stats[:, CHIPS:]
        top = jnp.max(m, axis=0)
        lse = top + jnp.log(jnp.sum(e * jnp.exp(m - top[None]), axis=0))
        lse_sum[:CHIPS] += lse
        lse_row = jnp.concatenate([lse[j:j + 1] for j in range(CHIPS)], axis=1)
        factor[...] = jnp.exp(runmax[s % 2] - lse_row) * inv_tokens

    def chunks(u, fwd, bwd, late_dw=False):
        par = u % 2
        if fwd:
            h_f = hbuf.at[u]
            t_f = target_row(u)
        if bwd:
            s = u - 2
            h_b = hbuf.at[s]
            t_b = target_row(s)
        def dlogits(c):
            lo, n = c * CHUNK, chunk_rows(c)
            dz_ref = dzs[c % len(dzs)]
            for r in range(0, n, TILE):
                k = min(TILE, n - r)
                hot = jnp.where(row_ids(lo + r, k) == t_b, inv_tokens, 0.0)
                dz = probs[par, lo + r:lo + r + k] * factor[c:c + 1] - hot
                dz_ref[r:r + k] = dz.astype(jnp.bfloat16)
                if late_dw:
                    probs[par, lo + r:lo + r + k] = dz
            if n < CHUNK:
                dz_ref[n:] = jnp.zeros((CHUNK - n, STEP_TOK), jnp.bfloat16)

        run_m = run_s = new_m = m = None
        tacc = jnp.zeros((8, STEP_TOK), F32)
        if bwd:
            dlogits(0)
        for c in range(n_chunks + 1):
            m = new_m
            if c < n_chunks and fwd:
                lo, n = c * CHUNK, chunk_rows(c)
                z = lax.dot_general(w[lo:lo + n], h_f[...], (((1,), (1,)), ((), ())), preferred_element_type=F32)
                zbufs[c % 2][:n] = z
                new_m = jnp.max(z, axis=0, keepdims=True)
                if c > 0:
                    new_m = jnp.maximum(new_m, m)
                runmax[par, c:c + 1] = new_m
            if c + 1 < n_chunks and bwd:
                dlogits(c + 1)
            if c < n_chunks and bwd:
                part = jnp.dot(wt[:, c * CHUNK:(c + 1) * CHUNK], dzs[c % len(dzs)][...], preferred_element_type=F32)
                if c == 0:
                    dh_acc[par] = part
                else:
                    dh_acc[par] += part
            if c > 0 and bwd and not late_dw:
                p = c - 1
                lo, n = p * CHUNK, chunk_rows(p)
                dw_acc[lo:lo + n] += jnp.dot(dzs[p % len(dzs)][:n], h_b[...], preferred_element_type=F32)
            if c > 0 and fwd:
                p = c - 1
                lo, n = p * CHUNK, chunk_rows(p)
                part = None
                for r in range(0, n, TILE):
                    k = min(TILE, n - r)
                    z = zbufs[p % 2][r:r + k]
                    e = jnp.exp(z - m)
                    probs[par, lo + r:lo + r + k] = e
                    e = jnp.sum(e.reshape(k // 8, 8, STEP_TOK), axis=0)
                    part = e if part is None else part + e
                    for i in range(0, k, 8):
                        tacc = jnp.where(row_ids(lo + r + i, 8) == t_f, z[i:i + 8], tacc)
                if p > 0:
                    part = run_s * jnp.exp(run_m - m) + part
                run_m, run_s = m, part
        if fwd:
            run_s = jnp.sum(run_s, axis=0, keepdims=True)
        if fwd:
            for j in range(CHIPS):
                cols = slice(j * PIECE, (j + 1) * PIECE)
                st_send[u, j:j + 1] = run_m[:, cols]
                st_send[u, CHIPS + j:CHIPS + j + 1] = run_s[:, cols]
            tgt_sum[...] += tacc
            pltpu.make_async_copy(st_send.at[u], st_recv.at[u, me], st_rsem.at[u]).start()
            for copy in stats_sends(u):
                copy.start()

    def late_chunks(s, which):
        for c in which:
            lo, n = c * CHUNK, chunk_rows(c)
            dw_acc[lo:lo + n] += jnp.dot(probs[s % 2, lo:lo + n].astype(jnp.bfloat16), hbuf[s], preferred_element_type=F32)

    def prepare(u):
        reduce_stages(u)
        h_stages(u)

    def own_piece(q):
        return pltpu.make_async_copy(hid.at[pl.ds(pl.multiple_of(q * PIECE, PIECE), PIECE)], piece(2 * q + core, chip), h_own.at[q])

    def start_piece(q, _):
        own_piece(q).start()
        return 0

    def wait_piece(q, _):
        own_piece(q).wait()
        return 0

    lax.fori_loop(0, steps // 2, start_piece, 0)
    w_copy = pltpu.make_async_copy(w_in, w, w_sem)
    w_copy.start()
    barrier = pltpu.get_barrier_semaphore()
    for i in range(1, 2 * CHIPS):
        pl.semaphore_signal(barrier, inc=1, device_id={"fsdp": (me + i) % (2 * CHIPS)}, device_id_type=pl.DeviceIdType.MESH)
    lax.fori_loop(0, steps // 2, wait_piece, 0)
    pl.semaphore_wait(barrier, 2 * CHIPS - 1)
    for copy in h_sends(0, True):
        copy.start()
    pltpu.make_async_copy(tgt, tbuf.at[me], t_sem).start()
    t_copies = [remote(tgt, tbuf.at[me], t_send, t_sem, (me + i) % (2 * CHIPS)) for i in range(1, 2 * CHIPS)]
    for copy in t_copies:
        copy.start()
    for copy in h_sends(1, True):
        copy.start()

    dw_acc[...] = jnp.zeros_like(dw_acc)
    tgt_sum[...] = jnp.zeros_like(tgt_sum)
    lse_sum[...] = jnp.zeros_like(lse_sum)
    w_copy.wait()
    for c in range(n_chunks):
        n = chunk_rows(c)
        wt[:, c * CHUNK:c * CHUNK + n] = w[c * CHUNK:c * CHUNK + n].T
    if last_rows < CHUNK:
        wt[:, vocab:] = jnp.zeros((width, n_chunks * CHUNK - vocab), jnp.bfloat16)

    @pl.when(core == 0)
    def _():
        h_ready(0, 0)
        h_forward(0).start()


    wait_bytes(tbuf, t_sem)

    def fwd_step(u, _):
        prepare(u)
        chunks(u, True, False)
        return 0

    def both_step(u, _):
        prepare(u)
        finish_stats(u - 2)
        chunks(u, True, True)
        return 0

    def bwd_step(u, _):
        prepare(u)
        finish_stats(u - 2)
        chunks(u, False, True, late_dw=True)
        return 0

    lax.fori_loop(0, 2, fwd_step, 0)
    lax.fori_loop(2, steps, both_step, 0)
    row = jnp.sum(tgt_sum[...], axis=0, keepdims=True)
    tile = jnp.concatenate([row[:, j * PIECE:(j + 1) * PIECE] for j in range(CHIPS)] + [jnp.zeros((8 - CHIPS, PIECE), F32)], axis=0)
    tt_send[:8] = tile
    pltpu.make_async_copy(tt_send.at[:8], tt_recv.at[me], tt_sem.at[1]).start()
    for i in range(1, 2 * CHIPS):
        remote(tt_send.at[:8], tt_recv.at[me], tt_sem.at[0], tt_sem.at[1], (me + i) % (2 * CHIPS)).start()
    lax.fori_loop(steps, steps + 2, bwd_step, 0)
    mid = n_chunks // 2
    reduce_stages(jnp.int32(steps + 2))
    late_chunks(steps - 2, range(mid))
    finish_block(steps - 5)
    second_stage(steps - 3)
    first_stage(steps - 1)
    late_chunks(steps - 2, range(mid, n_chunks))
    late_chunks(steps - 1, range(mid))
    finish_block(steps - 4)
    second_stage(steps - 2)
    late_chunks(steps - 1, range(mid, n_chunks))
    wait_bytes(tt_recv, tt_sem.at[1])
    loss_out[0] = (jnp.sum(lse_sum[...]) - jnp.sum(tt_recv[...])) * inv_tokens
    finish_block(steps - 3)
    second_stage(steps - 1)
    finish_block(steps - 2)
    finish_block(steps - 1)

    wait_bytes(dh_out, out_sem)
    peers = 2 * CHIPS - 1
    wait_bytes(tbuf.at[:peers], t_send)
    wait_bytes(tt_recv.at[:peers], tt_sem.at[0])

    def drain_pieces(q, _):
        for i in range(2):
            wait_bytes(hbuf.at[0, pl.ds(0, PIECE)], h_send.at[i, q])

        @pl.when(2 * q < DIRECT)
        def _():
            wait_bytes(hbuf.at[0, pl.ds(0, PIECE)], h_send.at[2, q])

        @pl.when(2 * q >= DIRECT)
        def _():
            for i in range(2):
                wait_bytes(hbuf.at[0, pl.ds(0, PIECE // 2)], h_send.at[3 + i, q])

        wait_bytes(hbuf.at[0], fw_send.at[q])
        wait_bytes(out_stage.at[2 * q], out_send.at[q])
        return 0

    def drain_stats(s, _):
        wait_bytes(st_recv.at[s, :peers], st_ssem.at[s])
        return 0

    lax.fori_loop(0, steps // 2, drain_pieces, 0)
    lax.fori_loop(0, steps, drain_stats, 0)
    for sl in range(SLOTS):
        wait_bytes(r1_buf.at[sl], s1_sem.at[0, sl])
        wait_bytes(s2_buf.at[sl], s2_sem.at[0, sl])


def solution(mesh):
    groups = mesh.shape["fsdp"]
    tok_spec = P(("dp", "fsdp"), None)

    def local_head(hidden, targets, weight):
        tok_loc, width = hidden.shape
        vocab = weight.shape[0]
        steps = 2 * tok_loc // PIECE
        padded = -(-vocab // CHUNK) * CHUNK
        half = width // 2
        dma, bf16 = pltpu.SemaphoreType.DMA, jnp.bfloat16
        vmem = pl.BlockSpec(memory_space=pltpu.VMEM)
        hbm = pl.BlockSpec(memory_space=pltpu.HBM)
        scratch = [
            pltpu.VMEM((vocab, width), bf16),
            pltpu.VMEM((width, padded), bf16),
            pltpu.VMEM((2, vocab, STEP_TOK), F32),
            pltpu.VMEM((steps, STEP_TOK, width), bf16),
            pltpu.VMEM((groups, tok_loc // PIECE, PIECE), jnp.int32),
            pltpu.VMEM((CHUNK, STEP_TOK), F32), pltpu.VMEM((CHUNK, STEP_TOK), F32),
            pltpu.VMEM((CHUNK, STEP_TOK), bf16), pltpu.VMEM((CHUNK, STEP_TOK), bf16), pltpu.VMEM((CHUNK, STEP_TOK), bf16),
            pltpu.VMEM((2, width, STEP_TOK), F32),
            pltpu.VMEM((2, padded // CHUNK, STEP_TOK), F32),
            pltpu.VMEM((padded // CHUNK, STEP_TOK), F32),
            pltpu.VMEM((8, STEP_TOK), F32),
            pltpu.VMEM((32, PIECE), F32),
            pltpu.VMEM((steps, 8, PIECE), F32),
            pltpu.VMEM((steps, groups, 8, PIECE), F32),
            pltpu.VMEM((32, PIECE), F32),
            pltpu.VMEM((groups, 8, PIECE), F32),
            pltpu.VMEM((2, half, STEP_TOK), F32),
            pltpu.VMEM((SLOTS, CHIPS, half, PIECE), F32),
            pltpu.VMEM((SLOTS, 2, half, PIECE), F32),
            pltpu.VMEM((SLOTS, half, PIECE), F32),
            pltpu.VMEM((SLOTS, half, PIECE), F32),
            pltpu.VMEM((SLOTS, half, PIECE), F32),
            pltpu.VMEM((steps, PIECE, half), F32),
            dma(()), dma((steps // 2,)), dma((3, steps // 2)), dma((steps // 2,)),
            dma((5, steps // 2)), dma((steps // 2,)),
            dma(()), dma(()),
            dma((steps,)), dma((steps,)),
            dma((2,)), dma((2, 2)), dma((2, SLOTS)), dma((2, SLOTS)),
            dma(()), dma((steps // 2,)),
        ]
        flops = 6 * tok_loc * groups * vocab * width
        return pl.pallas_call(
            head_kernel,
            out_shape=(jax.ShapeDtypeStruct((1,), F32), pltpu.VMEM((tok_loc, width), F32), pltpu.VMEM((vocab, width), F32)),
            in_specs=[hbm, hbm, hbm],
            out_specs=(pl.BlockSpec(memory_space=pltpu.SMEM), vmem, vmem),
            scratch_shapes=scratch,
            compiler_params=pltpu.CompilerParams(collective_id=0, has_side_effects=True, vmem_limit_bytes=56_000_000),
            cost_estimate=pl.CostEstimate(flops=flops, bytes_accessed=20_000_000, transcendentals=tok_loc * groups * vocab),
        )(hidden, targets.reshape(tok_loc // PIECE, PIECE), weight)

    return jax.shard_map(local_head, mesh=mesh, in_specs=(tok_spec, P(("dp", "fsdp")), P("fsdp", None)), out_specs=(P("dp"), tok_spec, tok_spec), check_vma=False)
```

```python
import functools

import jax
import jax.numpy as jnp
from jax import lax
from jax.experimental import pallas as pl
from jax.experimental.pallas import tpu as pltpu
from jax.sharding import PartitionSpec as P

PIECE = 128
CHIPS = 4
STEP_TOK = PIECE * CHIPS
TILE = 32
SLOTS = 4
DIRECT = 4
CHUNK = 512
F32 = jnp.float32


def head_kernel(hid, tgt, w_in, loss_out, dh_out, dw_out, w, wt, probs, hbuf, tbuf, zbuf_a, zbuf_b, dz_a, dz_b, dz_c, dh_acc,
                runmax, factor, tgt_sum, lse_sum, st_send, st_recv, tt_send, tt_recv, pair_buf, s1_buf, r1_buf, s2_buf, r2_buf,
                own_buf, out_stage, w_sem, h_own, h_recv, h_fwd, h_send, fw_send, t_sem, t_send, st_rsem, st_ssem, tt_sem, pair_sem,
                s1_sem, s2_sem, out_sem, out_send):
    tok_loc, width = hid.shape
    vocab = w.shape[0]
    steps = 2 * tok_loc // PIECE
    tokens = tok_loc * 2 * CHIPS
    half = width // 2
    n_chunks = -(-vocab // CHUNK)
    last_rows = vocab - (n_chunks - 1) * CHUNK
    inv_tokens = 1.0 / tokens
    dw_acc = dw_out
    zbufs, dzs = (zbuf_a, zbuf_b), (dz_a, dz_b, dz_c)

    me = lax.axis_index("fsdp")
    core, chip = me % 2, me // 2
    x, y = chip % 2, chip // 2
    partner = chip * 2 + 1 - core
    chip_x, chip_y, chip_d = y * 2 + (1 - x), (1 - y) * 2 + x, (1 - y) * 2 + (1 - x)
    chip_1 = (1 - core) * chip_x + core * chip_y
    chip_2 = (1 - core) * chip_y + core * chip_x

    def remote(src, dst, send, recv, dev):
        return pltpu.make_async_remote_copy(src_ref=src, dst_ref=dst, send_sem=send, recv_sem=recv, device_id={"fsdp": dev},
                                            device_id_type=pl.DeviceIdType.MESH)

    def wait_bytes(ref, sem):
        pltpu.make_async_copy(ref, ref, sem).wait()

    def chunk_rows(c):
        return CHUNK if c < n_chunks - 1 else last_rows

    def piece(s, of_chip, lo=0, n=PIECE):
        return hbuf.at[s, pl.ds(pl.multiple_of(of_chip * PIECE + lo, n), n)]

    def h_sends(q, direct):
        s = 2 * q + core
        peers = (chip_x, chip_y, chip_d)[:3 if direct else 2]
        return [remote(piece(s, chip), piece(s, chip), h_send.at[i, q], h_recv.at[i, q], peer * 2 + core) for i, peer in enumerate(peers)]

    def h_relays(s):
        q = s // 2
        return [remote(piece(s, src, lo, PIECE // 2), piece(s, src, lo, PIECE // 2), h_send.at[3 + i, q], h_recv.at[2, q], dst * 2 + core)
                for i, (src, dst, lo) in enumerate(((chip_x, chip_y, 0), (chip_y, chip_x, PIECE // 2)))]

    def h_forward(s):
        return remote(hbuf.at[s], hbuf.at[s], fw_send.at[s // 2], h_fwd.at[s // 2], partner)

    def stats_sends(s):
        return [remote(st_send.at[s], st_recv.at[s, me], st_ssem.at[s], st_rsem.at[s], (me + i) % (2 * CHIPS)) for i in range(1, 2 * CHIPS)]

    def pair_copy(s):
        rows = pl.ds(pl.multiple_of((1 - core) * half, half), half)
        return remote(dh_acc.at[s % 2, rows], pair_buf.at[s % 2], pair_sem.at[0, s % 2], pair_sem.at[1, s % 2], partner)

    def s1_copies(s):
        sl = s % SLOTS
        return [remote(s1_buf.at[sl, block], r1_buf.at[sl, i], s1_sem.at[0, sl], s1_sem.at[1, sl], chip_1 * 2 + core)
                for i, block in enumerate((chip_1, chip_d))]

    def s2_copy(s):
        return remote(s2_buf.at[s % SLOTS], r2_buf.at[s % SLOTS], s2_sem.at[0, s % SLOTS], s2_sem.at[1, s % SLOTS], chip_2 * 2 + core)

    def out_dst(s):
        return dh_out.at[pl.ds(pl.multiple_of(s // 2 * PIECE, PIECE), PIECE), pl.ds(pl.multiple_of(core * half, half), half)]

    def out_remote(s):
        return remote(out_stage.at[s], out_dst(s), out_send.at[s // 2], out_sem, partner)

    def finish_block(s):
        sl = s % SLOTS
        wait_bytes(r2_buf.at[sl], s2_sem.at[1, sl])
        out_stage[s] = (own_buf[sl] + r2_buf[sl]).T

        @pl.when(s % 2 == core)
        def _():
            pltpu.make_async_copy(out_stage.at[s], out_dst(s), out_sem).start()

        @pl.when(s % 2 != core)
        def _():
            out_remote(s).start()

    def second_stage(s):
        sl = s % SLOTS
        wait_bytes(r1_buf.at[sl], s1_sem.at[1, sl])

        @pl.when(s >= SLOTS)
        def _():
            wait_bytes(s2_buf.at[sl], s2_sem.at[0, sl])

        s2_buf[sl] = s1_buf[sl, chip_2] + r1_buf[sl, 1]
        own_buf[sl] = s1_buf[sl, chip] + r1_buf[sl, 0]
        s2_copy(s).start()

    def first_stage(s):
        sl, sl1 = s % 2, s % SLOTS
        wait_bytes(pair_buf.at[sl], pair_sem.at[1, sl])
        wait_bytes(pair_buf.at[sl], pair_sem.at[0, sl])

        @pl.when(s >= SLOTS)
        def _():
            wait_bytes(r1_buf.at[sl1], s1_sem.at[0, sl1])

        rows = pl.ds(pl.multiple_of(core * half, half), half)
        for j in range(CHIPS):
            cols = pl.ds(j * PIECE, PIECE)
            s1_buf[sl1, j] = dh_acc[sl, rows, cols] + pair_buf[sl, :, cols]
        for copy in s1_copies(s):
            copy.start()

    def reduce_stages(u):
        pl.when(u >= 8)(lambda: finish_block(u - 8))
        pl.when(u >= 6)(lambda: second_stage(u - 6))
        pl.when(u >= 4)(lambda: first_stage(u - 4))
        pl.when(u >= 3)(lambda: pair_copy(u - 3).start())

    def first_set(u):
        return jnp.minimum(DIRECT + u + 2 * jnp.clip(u - 2, 0, 2), steps)

    def h_ready(s, lo):
        for i in range(lo, 3):
            wait_bytes(hbuf.at[s, pl.ds(0, PIECE)], h_recv.at[i, s // 2])

    def h_stages(u):
        for i in range(3):
            @pl.when((first_set(u) + i < first_set(u + 1)) & ((first_set(u) + i) % 2 == core))
            def _():
                for copy in h_sends((first_set(u) + i) // 2, False):
                    copy.start()

        @pl.when((u + 2 >= DIRECT) & (u + 2 < steps) & (u % 2 == core))
        def _():
            for i in range(2):
                wait_bytes(hbuf.at[u + 2, pl.ds(0, PIECE)], h_recv.at[i, (u + 2) // 2])
            for copy in h_relays(u + 2):
                copy.start()

        @pl.when((u + 1 < DIRECT) & ((u + 1) % 2 == core))
        def _():
            h_ready(u + 1, 0)
            h_forward(u + 1).start()

        @pl.when((u + 1 >= DIRECT) & (u + 1 < steps) & ((u + 1) % 2 == core))
        def _():
            h_ready(u + 1, 2)
            h_forward(u + 1).start()

        @pl.when((u < steps) & (u % 2 != core))
        def _():
            wait_bytes(hbuf.at[u], h_fwd.at[u // 2])

    def row_ids(lo, n):
        return jnp.concatenate([lax.broadcasted_iota(jnp.int32, (n, PIECE), 0) + lo] * CHIPS, axis=1)

    def target_row(s):
        row = jnp.concatenate([tbuf[2 * j + s % 2, pl.ds(s // 2, 1), :] for j in range(CHIPS)], axis=1)
        return row - me * vocab

    def finish_stats(s):
        wait_bytes(st_recv.at[s], st_rsem.at[s])
        stats = st_recv[s]
        m, e = stats[:, :CHIPS], stats[:, CHIPS:]
        top = jnp.max(m, axis=0)
        lse = top + jnp.log(jnp.sum(e * jnp.exp(m - top[None]), axis=0))
        lse_sum[:CHIPS] += lse
        lse_row = jnp.concatenate([lse[j:j + 1] for j in range(CHIPS)], axis=1)
        factor[...] = jnp.exp(runmax[s % 2] - lse_row) * inv_tokens

    def chunks(u, fwd, bwd, late_dw=False):
        par = u % 2
        if fwd:
            h_f = hbuf.at[u]
            t_f = target_row(u)
        if bwd:
            s = u - 2
            h_b = hbuf.at[s]
            t_b = target_row(s)
        def dlogits(c):
            lo, n = c * CHUNK, chunk_rows(c)
            dz_ref = dzs[c % len(dzs)]
            for r in range(0, n, TILE):
                k = min(TILE, n - r)
                hot = jnp.where(row_ids(lo + r, k) == t_b, inv_tokens, 0.0)
                dz = probs[par, lo + r:lo + r + k] * factor[c:c + 1] - hot
                dz_ref[r:r + k] = dz.astype(jnp.bfloat16)
                if late_dw:
                    probs[par, lo + r:lo + r + k] = dz
            if n < CHUNK:
                dz_ref[n:] = jnp.zeros((CHUNK - n, STEP_TOK), jnp.bfloat16)

        run_m = run_s = new_m = m = None
        tacc = jnp.zeros((8, STEP_TOK), F32)
        if bwd:
            dlogits(0)
        for c in range(n_chunks + 1):
            m = new_m
            if c < n_chunks and fwd:
                lo, n = c * CHUNK, chunk_rows(c)
                z = lax.dot_general(w[lo:lo + n], h_f[...], (((1,), (1,)), ((), ())), preferred_element_type=F32)
                zbufs[c % 2][:n] = z
                new_m = jnp.max(z, axis=0, keepdims=True)
                if c > 0:
                    new_m = jnp.maximum(new_m, m)
                runmax[par, c:c + 1] = new_m
            if c + 1 < n_chunks and bwd:
                dlogits(c + 1)
            if c < n_chunks and bwd:
                part = jnp.dot(wt[:, c * CHUNK:(c + 1) * CHUNK], dzs[c % len(dzs)][...], preferred_element_type=F32)
                if c == 0:
                    dh_acc[par] = part
                else:
                    dh_acc[par] += part
            if c > 0 and bwd and not late_dw:
                p = c - 1
                lo, n = p * CHUNK, chunk_rows(p)
                dw_acc[lo:lo + n] += jnp.dot(dzs[p % len(dzs)][:n], h_b[...], preferred_element_type=F32)
            if c > 0 and fwd:
                p = c - 1
                lo, n = p * CHUNK, chunk_rows(p)
                part = None
                for r in range(0, n, TILE):
                    k = min(TILE, n - r)
                    z = zbufs[p % 2][r:r + k]
                    e = jnp.exp(z - m)
                    probs[par, lo + r:lo + r + k] = e
                    e = jnp.sum(e.reshape(k // 8, 8, STEP_TOK), axis=0)
                    part = e if part is None else part + e
                    for i in range(0, k, 8):
                        tacc = jnp.where(row_ids(lo + r + i, 8) == t_f, z[i:i + 8], tacc)
                if p > 0:
                    part = run_s * jnp.exp(run_m - m) + part
                run_m, run_s = m, part
        if fwd:
            run_s = jnp.sum(run_s, axis=0, keepdims=True)
        if fwd:
            for j in range(CHIPS):
                cols = slice(j * PIECE, (j + 1) * PIECE)
                st_send[u, j:j + 1] = run_m[:, cols]
                st_send[u, CHIPS + j:CHIPS + j + 1] = run_s[:, cols]
            tgt_sum[...] += tacc
            pltpu.make_async_copy(st_send.at[u], st_recv.at[u, me], st_rsem.at[u]).start()
            for copy in stats_sends(u):
                copy.start()

    def late_chunks(s, which):
        for c in which:
            lo, n = c * CHUNK, chunk_rows(c)
            dw_acc[lo:lo + n] += jnp.dot(probs[s % 2, lo:lo + n].astype(jnp.bfloat16), hbuf[s], preferred_element_type=F32)

    def prepare(u):
        reduce_stages(u)
        h_stages(u)

    def own_piece(q):
        return pltpu.make_async_copy(hid.at[pl.ds(pl.multiple_of(q * PIECE, PIECE), PIECE)], piece(2 * q + core, chip), h_own.at[q])

    def start_piece(q, _):
        own_piece(q).start()
        return 0

    def wait_piece(q, _):
        own_piece(q).wait()
        return 0

    lax.fori_loop(0, steps // 2, start_piece, 0)
    w_copy = pltpu.make_async_copy(w_in, w, w_sem)
    w_copy.start()
    barrier = pltpu.get_barrier_semaphore()
    for i in range(1, 2 * CHIPS):
        pl.semaphore_signal(barrier, inc=1, device_id={"fsdp": (me + i) % (2 * CHIPS)}, device_id_type=pl.DeviceIdType.MESH)
    lax.fori_loop(0, steps // 2, wait_piece, 0)
    pl.semaphore_wait(barrier, 2 * CHIPS - 1)
    for copy in h_sends(0, True):
        copy.start()
    pltpu.make_async_copy(tgt, tbuf.at[me], t_sem).start()
    t_copies = [remote(tgt, tbuf.at[me], t_send, t_sem, (me + i) % (2 * CHIPS)) for i in range(1, 2 * CHIPS)]
    for copy in t_copies:
        copy.start()
    for copy in h_sends(1, True):
        copy.start()

    dw_acc[...] = jnp.zeros_like(dw_acc)
    tgt_sum[...] = jnp.zeros_like(tgt_sum)
    lse_sum[...] = jnp.zeros_like(lse_sum)
    w_copy.wait()
    for c in range(n_chunks):
        n = chunk_rows(c)
        wt[:, c * CHUNK:c * CHUNK + n] = w[c * CHUNK:c * CHUNK + n].T
    if last_rows < CHUNK:
        wt[:, vocab:] = jnp.zeros((width, n_chunks * CHUNK - vocab), jnp.bfloat16)

    @pl.when(core == 0)
    def _():
        h_ready(0, 0)
        h_forward(0).start()


    wait_bytes(tbuf, t_sem)

    def fwd_step(u, _):
        prepare(u)
        chunks(u, True, False)
        return 0

    def both_step(u, _):
        prepare(u)
        finish_stats(u - 2)
        chunks(u, True, True)
        return 0

    def bwd_step(u, _):
        prepare(u)
        finish_stats(u - 2)
        chunks(u, False, True, late_dw=True)
        return 0

    lax.fori_loop(0, 2, fwd_step, 0)
    lax.fori_loop(2, steps, both_step, 0)
    row = jnp.sum(tgt_sum[...], axis=0, keepdims=True)
    tile = jnp.concatenate([row[:, j * PIECE:(j + 1) * PIECE] for j in range(CHIPS)] + [jnp.zeros((8 - CHIPS, PIECE), F32)], axis=0)
    tt_send[:8] = tile
    pltpu.make_async_copy(tt_send.at[:8], tt_recv.at[me], tt_sem.at[1]).start()
    for i in range(1, 2 * CHIPS):
        remote(tt_send.at[:8], tt_recv.at[me], tt_sem.at[0], tt_sem.at[1], (me + i) % (2 * CHIPS)).start()
    lax.fori_loop(steps, steps + 2, bwd_step, 0)
    mid = n_chunks // 2
    reduce_stages(jnp.int32(steps + 2))
    late_chunks(steps - 2, range(mid))
    finish_block(steps - 5)
    second_stage(steps - 3)
    first_stage(steps - 1)
    late_chunks(steps - 2, range(mid, n_chunks))
    late_chunks(steps - 1, range(mid))
    finish_block(steps - 4)
    second_stage(steps - 2)
    late_chunks(steps - 1, range(mid, n_chunks))
    wait_bytes(tt_recv, tt_sem.at[1])
    loss_out[0] = (jnp.sum(lse_sum[...]) - jnp.sum(tt_recv[...])) * inv_tokens
    finish_block(steps - 3)
    second_stage(steps - 1)
    finish_block(steps - 2)
    finish_block(steps - 1)

    wait_bytes(dh_out, out_sem)
    peers = 2 * CHIPS - 1
    wait_bytes(tbuf.at[:peers], t_send)
    wait_bytes(tt_recv.at[:peers], tt_sem.at[0])

    def drain_pieces(q, _):
        for i in range(2):
            wait_bytes(hbuf.at[0, pl.ds(0, PIECE)], h_send.at[i, q])

        @pl.when(2 * q < DIRECT)
        def _():
            wait_bytes(hbuf.at[0, pl.ds(0, PIECE)], h_send.at[2, q])

        @pl.when(2 * q >= DIRECT)
        def _():
            for i in range(2):
                wait_bytes(hbuf.at[0, pl.ds(0, PIECE // 2)], h_send.at[3 + i, q])

        wait_bytes(hbuf.at[0], fw_send.at[q])
        wait_bytes(out_stage.at[2 * q], out_send.at[q])
        return 0

    def drain_stats(s, _):
        wait_bytes(st_recv.at[s, :peers], st_ssem.at[s])
        return 0

    lax.fori_loop(0, steps // 2, drain_pieces, 0)
    lax.fori_loop(0, steps, drain_stats, 0)
    for sl in range(SLOTS):
        wait_bytes(r1_buf.at[sl], s1_sem.at[0, sl])
        wait_bytes(s2_buf.at[sl], s2_sem.at[0, sl])


def solution(mesh):
    groups = mesh.shape["fsdp"]
    tok_spec = P(("dp", "fsdp"), None)

    def local_head(hidden, targets, weight):
        tok_loc, width = hidden.shape
        vocab = weight.shape[0]
        steps = 2 * tok_loc // PIECE
        padded = -(-vocab // CHUNK) * CHUNK
        half = width // 2
        dma, bf16 = pltpu.SemaphoreType.DMA, jnp.bfloat16
        vmem = pl.BlockSpec(memory_space=pltpu.VMEM)
        hbm = pl.BlockSpec(memory_space=pltpu.HBM)
        scratch = [
            pltpu.VMEM((vocab, width), bf16),
            pltpu.VMEM((width, padded), bf16),
            pltpu.VMEM((2, vocab, STEP_TOK), F32),
            pltpu.VMEM((steps, STEP_TOK, width), bf16),
            pltpu.VMEM((groups, tok_loc // PIECE, PIECE), jnp.int32),
            pltpu.VMEM((CHUNK, STEP_TOK), F32), pltpu.VMEM((CHUNK, STEP_TOK), F32),
            pltpu.VMEM((CHUNK, STEP_TOK), bf16), pltpu.VMEM((CHUNK, STEP_TOK), bf16), pltpu.VMEM((CHUNK, STEP_TOK), bf16),
            pltpu.VMEM((2, width, STEP_TOK), F32),
            pltpu.VMEM((2, padded // CHUNK, STEP_TOK), F32),
            pltpu.VMEM((padded // CHUNK, STEP_TOK), F32),
            pltpu.VMEM((8, STEP_TOK), F32),
            pltpu.VMEM((32, PIECE), F32),
            pltpu.VMEM((steps, 8, PIECE), F32),
            pltpu.VMEM((steps, groups, 8, PIECE), F32),
            pltpu.VMEM((32, PIECE), F32),
            pltpu.VMEM((groups, 8, PIECE), F32),
            pltpu.VMEM((2, half, STEP_TOK), F32),
            pltpu.VMEM((SLOTS, CHIPS, half, PIECE), F32),
            pltpu.VMEM((SLOTS, 2, half, PIECE), F32),
            pltpu.VMEM((SLOTS, half, PIECE), F32),
            pltpu.VMEM((SLOTS, half, PIECE), F32),
            pltpu.VMEM((SLOTS, half, PIECE), F32),
            pltpu.VMEM((steps, PIECE, half), F32),
            dma(()), dma((steps // 2,)), dma((3, steps // 2)), dma((steps // 2,)),
            dma((5, steps // 2)), dma((steps // 2,)),
            dma(()), dma(()),
            dma((steps,)), dma((steps,)),
            dma((2,)), dma((2, 2)), dma((2, SLOTS)), dma((2, SLOTS)),
            dma(()), dma((steps // 2,)),
        ]
        flops = 6 * tok_loc * groups * vocab * width
        return pl.pallas_call(
            head_kernel,
            out_shape=(jax.ShapeDtypeStruct((1,), F32), pltpu.VMEM((tok_loc, width), F32), pltpu.VMEM((vocab, width), F32)),
            in_specs=[hbm, hbm, hbm],
            out_specs=(pl.BlockSpec(memory_space=pltpu.SMEM), vmem, vmem),
            scratch_shapes=scratch,
            compiler_params=pltpu.CompilerParams(collective_id=0, has_side_effects=True, vmem_limit_bytes=56_000_000),
            cost_estimate=pl.CostEstimate(flops=flops, bytes_accessed=20_000_000, transcendentals=tok_loc * groups * vocab),
        )(hidden, targets.reshape(tok_loc // PIECE, PIECE), weight)

    return jax.shard_map(local_head, mesh=mesh, in_specs=(tok_spec, P(("dp", "fsdp")), P("fsdp", None)), out_specs=(P("dp"), tok_spec, tok_spec), check_vma=False)
```
